1024 devices in a mesh: gx: 8 (over y_lo, core), gy: 16 (over y_hi, x), gz: 8 (over z).
Axes of the slice: x: 8, y: 8 (y_hi: 2, y_lo: 4; y = y_hi * 4 + y_lo), z: 8, core: 2. Of those that a mesh axis runs over, the one named last changes fastest.
Arguments:
- sources: float32 [1, 128, 256, 1024], P(None, 'gx', 'gy', 'gz'), may hold values from -6 to 6
- stiffness: float32 [128, 256, 1024], P('gx', 'gy', 'gz'), may hold values from 0.5 to 2
- coarse_inverse: float32 [8192, 8192], P(('gx', 'gy', 'gz')), may hold values from -1.25 to 1.25
Outputs:
- pressure: float32 [1, 128, 256, 1024], P(None, 'gx', 'gy', 'gz')
The draws below stay inside these ranges and needn't reach their ends.
All inputs are finite; a program needn't handle non-finite values.
Results may differ from the reference program's by a relative error of at most 0.0001.
Values sent between devices are 32-bit elements; how exact they have to be, the bound alone decides.
A program may use at most 32 MiB of HBM per device.

```python
import math
import jax
import jax.numpy as jnp
from jax import lax

SYSTEMS = 1
CX = 16
CY = 16
CZ = 128
NX = 128
NY = 256
NZ = 1024
NC = 8192
N_GX = 8
N_GY = 16
N_GZ = 8


def level_of(own_key, shape, cuts, smallest, largest):
    loudness = 1.0
    for dim, shards_of in cuts:
        steps = jax.random.uniform(jax.random.fold_in(jax.random.fold_in(own_key, 6), dim), (shards_of,), jnp.float32, smallest / len(cuts), largest / len(cuts))
        loudness = loudness * jnp.repeat(jnp.exp(steps), shape[dim] // shards_of).reshape((-1,) + (1,) * (len(shape) - 1 - dim))
    return loudness


def centred(own_key, extent, deviation, most, pieces=(), kind=jnp.bfloat16):
    loudness = level_of(own_key, extent, pieces, -0.22, 0.18) if pieces else 1.0
    values = jax.random.normal(own_key, extent, jnp.float32) * deviation * loudness
    return jnp.minimum(jnp.maximum(values, -most), most).astype(kind)


def setup_inputs(seed: int = 0) -> dict:
    splits = jax.random.split(jax.random.key(seed), 4)
    sources = centred(splits[0], (SYSTEMS, NX, NY, NZ), 1.0, 6.0, ((1, 8), (2, 16), (3, 8)), jnp.float32)
    stiffness = jnp.clip(jnp.exp(math.log(2.0) - 1.3862944 * jax.random.uniform(splits[1], (NX, NY, NZ), jnp.float32) ** level_of(splits[1], (NX, NY, NZ), ((0, 8), (1, 16), (2, 8)), -0.2, 0.2)), 0.5, 2.0)
    coarse_inverse = centred(splits[2], (NC, NC), (max(NC // 400, 1)) ** -0.5, 1.25, ((0, 1024),), jnp.float32)
    return {"sources": sources, "stiffness": stiffness, "coarse_inverse": coarse_inverse}


damping = 0.8


def loop_sum(padded):
    total = padded[:, 2:, 1:-1, 1:-1] + padded[:, :-2, 1:-1, 1:-1]
    total = total + padded[:, 1:-1, 2:, 1:-1] + padded[:, 1:-1, :-2, 1:-1]
    total = total + padded[:, 1:-1, 1:-1, 2:] + padded[:, 1:-1, 1:-1, :-2]
    return total


def apply_op(answer, weights):
    scaled = weights * answer
    padded = jnp.pad(scaled, ((0, 0), (1, 1), (1, 1), (1, 1)))
    return weights * (6.0 * scaled - loop_sum(padded))


def pre_smooth(source, weights):
    diagonal = 6.0 * weights * weights
    first = damping * source / diagonal
    second = first + damping * (source - apply_op(first, weights)) / diagonal
    return second, source - apply_op(second, weights)


def post_smooth(answer, source, weights):
    return answer + damping * (source - apply_op(answer, weights)) / (6.0 * weights * weights)


def coarsen(values):
    leading = values.shape[0]
    size_x, size_y, size_z = values.shape[1], values.shape[2], values.shape[3]
    blocks = values.reshape((leading, size_x // 2, 2, size_y // 2, 2, size_z // 2, 2))
    return jnp.mean(blocks, axis=(2, 4, 6))


def refine(values):
    return jnp.repeat(jnp.repeat(jnp.repeat(values, 2, axis=1), 2, axis=2), 2, axis=3)


def reference(sources, stiffness, coarse_inverse):
    weight_list = [stiffness[None]]
    for level in range(3):
        weight_list.append(0.5 * coarsen(weight_list[-1]))
    source_list = []
    answer_list = []
    current = sources
    for level in range(4):
        source_list.append(current)
        answer, resid = pre_smooth(current, weight_list[level])
        answer_list.append(answer)
        current = coarsen(resid)
    coarse_source = current
    block_x = CX // 16
    block_y = CY // 16
    block_z = CZ // 16
    ordered = coarse_source.reshape((SYSTEMS, N_GX, block_x, N_GY, block_y, N_GZ, block_z))
    ordered = ordered.transpose((0, 1, 3, 5, 2, 4, 6)).reshape((SYSTEMS, NC))
    solved = jnp.dot(ordered, coarse_inverse.T, precision=lax.Precision.HIGHEST, preferred_element_type=jnp.float32)
    solved = solved.reshape((SYSTEMS, N_GX, N_GY, N_GZ, block_x, block_y, block_z))
    correction = solved.transpose((0, 1, 4, 2, 5, 3, 6)).reshape(coarse_source.shape)
    for level in range(3, -1, -1):
        correction = post_smooth(answer_list[level] + refine(correction), source_list[level], weight_list[level])
    return correction
```

```python
import functools
import itertools

import jax
import jax.numpy as jnp
from jax import lax
from jax.experimental import pallas as pl
from jax.experimental.pallas import tpu as pltpu
from jax.sharding import PartitionSpec as P

MESH = pl.DeviceIdType.MESH
F32 = jnp.float32
S = 0.8 / 6.0
OFFS = [o for o in itertools.product((-1, 0, 1), repeat=3) if o != (0, 0, 0)]
SLOT = {o: i for i, o in enumerate(OFFS)}
ZOFFS = [o for o in OFFS if o[2] != 0]
ZSLOT = {o: i for i, o in enumerate(ZOFFS)}
XY = [(-1, -1), (-1, 1), (1, -1), (1, 1)]
XZ = [(0, -1), (0, 1)] + XY


def neg(o):
    return tuple(-v for v in o)


def roll(v, shift):
    shift = shift % 128
    return v if shift == 0 else pltpu.roll(v, shift, v.ndim - 1)


def split2(v):
    hi = v.astype(jnp.bfloat16)
    lo = (v - hi.astype(F32)).astype(jnp.bfloat16)
    return jnp.concatenate([hi, lo], axis=1)


def select_dot(v, sel):
    return jnp.dot(split2(v), sel, preferred_element_type=F32)


def kernel(dims, refs):
    nx, ny, nz = dims
    xn = ny // 2
    n_y = nx * 2
    r = refs
    ix, iy, iz = lax.axis_index("gx"), lax.axis_index("gy"), lax.axis_index("gz")
    ih, ixx = iy // xn, iy % xn

    def dev(dx, dy, dz):
        return {
            "gx": lax.rem(ix + dx + nx, nx),
            "gy": lax.rem(iy + dy + ny, ny),
            "gz": lax.rem(iz + dz + nz, nz),
        }

    def copy(src, dst, key, device):
        c = pltpu.make_async_remote_copy(
            src_ref=src,
            dst_ref=dst,
            send_sem=r["ssem"].at[key],
            recv_sem=r["rsem"].at[key],
            device_id=device,
            device_id_type=MESH,
        )
        return c

    def send(src, dst, key, device):
        copy(src, dst, key, device).start()

    me = {"gx": ix, "gy": iy, "gz": iz}
    right = {"gx": lax.rem(ix + 1, nx), "gy": iy, "gz": iz}

    group_y = []
    for k in range(1, n_y):
        t = lax.rem(ih * nx + ix + k, n_y)
        group_y.append({"gx": t % nx, "gy": (t // nx) * xn + ixx, "gz": iz})
    group_x = [{"gx": ix, "gy": ih * xn + lax.rem(ixx + k, xn), "gz": iz} for k in range(1, xn)]
    group_z = [{"gx": ix, "gy": iy, "gz": lax.rem(iz + k, nz)} for k in range(1, nz)]

    barrier = pltpu.get_barrier_semaphore()
    partners = [dev(*o) for o in OFFS] + group_y + group_x + group_z
    for d in partners:
        pl.semaphore_signal(barrier, inc=1, device_id=d, device_id_type=MESH)

    lane = lax.broadcasted_iota(jnp.int32, (8, 128), 1)
    row = lax.broadcasted_iota(jnp.int32, (8, 128), 0)
    zero = jnp.zeros((8, 128), F32)

    def flag(c):
        return jnp.where(c, jnp.float32(1), jnp.float32(0))

    mx = {-1: flag(ix > 0), 0: jnp.float32(1), 1: flag(ix < nx - 1)}
    my = {-1: flag(iy > 0), 0: jnp.float32(1), 1: flag(iy < ny - 1)}
    mz = {-1: flag(iz > 0), 0: jnp.float32(1), 1: flag(iz < nz - 1)}
    zmask = jnp.where(lane < 32, mz[-1], jnp.where(lane >= 96, mz[1], 1.0))

    b_ref, w_ref, c_ref, out_ref = r["b"], r["w"], r["c"], r["out"]
    for name in ("G0", "W0", "V0"):
        a = r[name]
        a[:, 0:8, :] = jnp.zeros((20, 8, 128), F32)
        a[:, 24:32, :] = jnp.zeros((20, 8, 128), F32)
    for name in ("GQ", "WQ", "VQ", "UQ", "G1", "W1", "V1", "U1", "G2", "W2", "V2", "U2", "P2", "Q2", "G3", "W3", "V3", "U3", "P3", "T4"):
        r[name][...] = jnp.zeros(r[name].shape, F32)

    G0, W0, V0 = r["G0"], r["W0"], r["V0"]
    w0 = w_ref[...]
    g0 = b_ref[0] / w0
    W0[2:18, 8:24, :] = w0
    G0[2:18, 8:24, :] = g0

    r["YS"][0] = G0[2:18, 8:10, :]
    r["YS"][1] = G0[2:18, 22:24, :]

    def pack_q(src, dst):
        for h in range(2):
            acc = zero
            for x in range(16):
                m = src[x + 2, 8 + 8 * h : 16 + 8 * h, :]
                base = 6 * (x + 2)
                acc = jnp.where((lane >= base) & (lane < base + 3), roll(m, base - 126), acc)
                acc = jnp.where((lane >= base + 3) & (lane < base + 6), roll(m, base + 3 - 127), acc)
            dst[8 * h : 8 * h + 8, :] = acc

    pack_q(G0, r["QS"])
    r["QE"][0] = r["QS"][0:1, :]
    r["QE"][1] = r["QS"][15:16, :]

    pl.semaphore_wait(barrier, len(partners))

    gsl = pl.ds(8, 16)
    send(G0.at[pl.ds(2, 2), gsl], G0.at[pl.ds(18, 2), gsl], 0, dev(-1, 0, 0))
    send(G0.at[pl.ds(16, 2), gsl], G0.at[pl.ds(0, 2), gsl], 1, dev(1, 0, 0))
    for i, d in enumerate((-1, 1)):
        send(r["YS"].at[i], r["RY"].at[1 - i], 2 + i, dev(0, d, 0))
    for dx, dy in XY:
        src = r["YS"].at[(dy + 1) // 2, 0 if dx < 0 else 15]
        send(src, r["RXY"].at[XY.index((-dx, -dy))], 4, dev(dx, dy, 0))
    for dx, dz in XZ:
        send(r["QS"], r["RQ"].at[XZ.index((-dx, -dz))], 5, dev(dx, 0, dz))
    for dy, dz in XY:
        send(r["QE"].at[(dy + 1) // 2], r["RQE"].at[XY.index((-dy, -dz))], 6, dev(0, dy, dz))

    zr = lax.broadcasted_iota(jnp.int32, (256, 128), 0) % 128
    zc = lax.broadcasted_iota(jnp.int32, (256, 128), 1)
    down = jnp.where(zc == 32 + zr // 2, jnp.float32(1), jnp.float32(0)).astype(jnp.bfloat16)
    up = jnp.where(zr == 32 + zc // 2, jnp.float32(1), jnp.float32(0)).astype(jnp.bfloat16)

    C0 = r["C0"]

    def coarsen0(values, scale):
        C0[...] = jnp.sum(values.reshape(8, 2, 16, 128), axis=1)
        t = C0[:, pl.ds(0, 8, stride=2), :] + C0[:, pl.ds(1, 8, stride=2), :]
        return (select_dot(t.reshape(64, 128), down) * scale).reshape(8, 8, 128)

    def pair_z(t, dil):
        ln = lax.broadcasted_iota(jnp.int32, t.shape, t.ndim - 1)
        return t + jnp.where((ln // dil) % 2 == 0, roll(t, -dil), roll(t, dil))

    C1, C2 = r["C1"], r["C2"]

    def coarsen1(values, scale):
        n = values.shape[0] // 2
        C1[...] = jnp.sum(values.reshape(n, 2, 8, 128), axis=1)
        t = C1[:, pl.ds(0, 4, stride=2), :] + C1[:, pl.ds(1, 4, stride=2), :]
        return pair_z(t, 1) * scale

    S1 = r["S1"]
    w1 = coarsen0(w0, 0.0625)
    own1 = (lane >= 32) & (lane < 96)
    w2 = coarsen1(w1, 0.0625)
    C2[0:4, 0:4, :] = w2
    t = C2[0:4, pl.ds(0, 2, stride=2), :] + C2[0:4, pl.ds(1, 2, stride=2), :]
    w3 = pair_z(jnp.sum(t.reshape(2, 2, 2, 128), axis=1), 2) * 0.0625

    lane4 = lane[0:4]

    def pack2(v):
        halves = []
        for h in range(2):
            a = jnp.where(lane4 % 2 == 0, v[2 * h], v[2 * h + 1])
            halves.append(roll(a, -32 if h == 0 else 32))
        return jnp.where(lane4 < 64, halves[0], halves[1])

    def pack3(v):
        return jnp.where(lane[0:2] < 64, roll(v[0], -32), roll(v[1], 32))

    SW = r["SW"]
    SW[0:4, :] = pack2(w2)
    SW[4:6, :] = pack3(w3)
    SW[6:8, :] = jnp.zeros((2, 128), F32)

    def send_all(src, dst, key):
        for o in OFFS:
            send(src, dst.at[SLOT[neg(o)]], key, dev(*o))

    def wait_recv(dst, key):
        copy(dst, dst, key, right).wait_recv()

    def wait_send(like, key):
        copy(like, like, key, right).wait_send()

    send_all(SW, r["RW"], 7)

    def send1(own, n, key):
        s1, ys, zs = r["S1" + n], r["YS1" + n], r["ZS1" + n]
        s1[...] = own
        ys[0] = s1[:, 0:4, :]
        ys[1] = s1[:, 4:8, :]
        acc = zero
        for x in range(8):
            acc = jnp.where((lane >= 16 * x) & (lane < 16 * x + 4), roll(own[x], 16 * x - 32), acc)
            acc = jnp.where((lane >= 16 * x + 4) & (lane < 16 * x + 8), roll(own[x], 16 * x + 4 - 92), acc)
        zs[...] = acc
        send(s1.at[pl.ds(0, 3)], r["RX1" + n].at[1], key, dev(-1, 0, 0))
        send(s1.at[pl.ds(5, 3)], r["RX1" + n].at[0], key, dev(1, 0, 0))
        send(ys.at[0], r["RY1" + n].at[1], key + 1, dev(0, -1, 0))
        send(ys.at[1], r["RY1" + n].at[0], key + 1, dev(0, 1, 0))
        for dx, dy in XY:
            src = ys.at[(dy + 1) // 2, pl.ds(0 if dx < 0 else 5, 3)]
            send(src, r["RXY1" + n].at[XY.index((-dx, -dy))], key + 2, dev(dx, dy, 0))
        for o in ZOFFS:
            send(zs, r["RZ1" + n].at[ZSLOT[neg(o)]], key + 3, dev(*o))

    def recv1(own, n, key, dst):
        for i, name in enumerate(("RX1", "RY1", "RXY1", "RZ1")):
            wait_recv(r[name + n], key + i)
        for x in range(14):
            dx = -1 if x < 3 else (1 if x > 10 else 0)
            for dy in (-1, 0, 1):
                if dx == 0 and dy == 0:
                    base = own[x - 3]
                elif dy == 0:
                    base = r["RX1" + n][(dx + 1) // 2, x if dx < 0 else x - 11]
                elif dx == 0:
                    base = r["RY1" + n][(dy + 1) // 2, x - 3]
                else:
                    base = r["RXY1" + n][XY.index((dx, dy)), x if dx < 0 else x - 11]
                sx = x - 3 if dx == 0 else (x + 5 if dx < 0 else x - 11)
                rows = slice(0, 8) if dy == 0 else (slice(4, 8) if dy < 0 else slice(0, 4))
                lo = r["RZ1" + n][ZSLOT[(dx, dy, -1)], rows, :]
                hi = r["RZ1" + n][ZSLOT[(dx, dy, 1)], rows, :]
                ln = lane[0:8] if dy == 0 else lane4
                v = jnp.where((ln >= 28) & (ln < 32), roll(lo, 28 - 16 * x0(sx) - 4) * mz[-1], base)
                v = jnp.where((ln >= 96) & (ln < 100), roll(hi, 96 - 16 * x0(sx)) * mz[1], v)
                if dx != 0 or dy != 0:
                    v = v * (mx[dx] * my[dy])
                at = 8 if dy == 0 else (4 if dy < 0 else 16)
                dst[x, at : at + (8 if dy == 0 else 4), :] = v

    def x0(v):
        return v

    send1(w1, "w", 8)

    r["YW"][0] = W0[2:18, 8:9, :]
    r["YW"][1] = W0[2:18, 23:24, :]
    pack_q(W0, r["QW"])
    send(W0.at[pl.ds(2, 1), gsl], W0.at[pl.ds(18, 1), gsl], 12, dev(-1, 0, 0))
    send(W0.at[pl.ds(17, 1), gsl], W0.at[pl.ds(1, 1), gsl], 13, dev(1, 0, 0))
    for i, d in enumerate((-1, 1)):
        send(r["YW"].at[i], r["RYW"].at[1 - i], 14, dev(0, d, 0))
        send(r["QW"], r["RQW"].at[1 - i], 15, dev(0, 0, d))

    wi1 = 1.0 / jnp.where(own1, w1, 1.0)
    wi2 = 1.0 / jnp.where(own1[0:4], w2, 1.0)
    wi3 = 1.0 / jnp.where(own1[0:2], w3, 1.0)

    cp = r["CP"]

    @pl.loop(0, nx)
    def _(x):
        for z in range(nz):
            acc = zero
            for p in range(ny // 2):
                tile = c_ref[:, pl.ds(pl.multiple_of((x * (ny // 2) + p) * 128, 128), 128)]
                for q in range(2):
                    y = 2 * p + q
                    at = 8 * y
                    acc = jnp.where((lane >= at) & (lane < at + 8), roll(tile, at - 64 * q - 8 * z), acc)
            cp[x * nz + z] = acc

    GQ, VQ = r["GQ"], r["VQ"]
    for key, dst in ((0, G0.at[pl.ds(18, 2), gsl]), (1, G0.at[pl.ds(0, 2), gsl]), (2, r["RY"].at[1]), (3, r["RY"].at[0])):
        wait_recv(dst, key)
    wait_recv(r["RXY"], 4)
    wait_recv(r["RQ"], 5)
    wait_recv(r["RQE"], 6)
    G0[0:2, 8:24, :] = G0[0:2, 8:24, :] * mx[-1]
    G0[18:20, 8:24, :] = G0[18:20, 8:24, :] * mx[1]
    G0[2:18, 6:8, :] = r["RY"][0] * my[-1]
    G0[2:18, 24:26, :] = r["RY"][1] * my[1]
    for dx, dy in XY:
        v = r["RXY"][XY.index((dx, dy))] * (mx[dx] * my[dy])
        G0[1 if dx < 0 else 18, 7 if dy < 0 else 24, :] = v[1 if dy < 0 else 0, :]

    def qj(ln):
        return ln % 6

    for h in range(2):
        sl = slice(8 * h, 8 * h + 8)
        own = r["QS"][sl, :]
        j = qj(lane)
        v = jnp.where(j < 2, r["RQ"][0, sl, :] * mz[-1], jnp.where(j > 3, r["RQ"][1, sl, :] * mz[1], own))
        lo = jnp.where(j < 2, r["RQ"][2, sl, :] * mz[-1], jnp.where(j > 3, r["RQ"][3, sl, :] * mz[1], 0.0)) * mx[-1]
        hi = jnp.where(j < 2, r["RQ"][4, sl, :] * mz[-1], jnp.where(j > 3, r["RQ"][5, sl, :] * mz[1], 0.0)) * mx[1]
        v = jnp.where((lane >= 6) & (lane < 12), roll(lo, 6 - 102), jnp.where((lane >= 108) & (lane < 114), roll(hi, 108 - 12), v))
        GQ[8 + 8 * h : 16 + 8 * h, :] = jnp.where((lane >= 6) & (lane < 114), v, 0.0)
    for dy, at in ((-1, 7), (1, 24)):
        j = qj(lane[0:1])
        lo = r["RQE"][XY.index((dy, -1))] * (my[dy] * mz[-1])
        hi = r["RQE"][XY.index((dy, 1))] * (my[dy] * mz[1])
        v = jnp.where(j < 2, lo, jnp.where(j > 3, hi, 0.0))
        GQ[at : at + 1, :] = jnp.where((lane[0:1] >= 12) & (lane[0:1] < 108), v, 0.0)

    INJ = r["INJ"]

    def inject(q, xs, tiles):
        for at in tiles:
            m = q[at : at + 8, :]
            for xp in xs:
                a = roll(m, -(6 * xp + 1))
                c = roll(m, 127 - (6 * xp + 4))
                INJ[xp, at : at + 8, :] = jnp.where(lane == 0, a, jnp.where(lane == 127, c, 0.0))

    def sum0(a, x, n, at):
        c = a[x : x + n, at : at + 8, :]
        t = a[x - 1 : x + n - 1, at : at + 8, :] + a[x + 1 : x + n + 1, at : at + 8, :]
        t = t + (a[x : x + n, at - 1 : at + 7, :] + a[x : x + n, at + 1 : at + 9, :])
        z = jnp.where(lane == 0, 0.0, roll(c, 1)) + jnp.where(lane == 127, 0.0, roll(c, -1))
        return c, t + (z + INJ[x : x + n, at : at + 8, :])

    inject(GQ, range(1, 19), (7, 15, 17))
    for at in (7, 15, 17):
        c, t = sum0(G0, 1, 18, at)
        v = S * (1.2 * c + S * t)
        if at == 7:
            v = v * jnp.where(row == 0, my[-1], 1.0)
        if at == 17:
            v = v * jnp.where(row == 7, my[1], 1.0)
        V0[1:19, at : at + 8, :] = v
    V0[1:2, 7:25, :] = V0[1:2, 7:25, :] * mx[-1]
    V0[18:19, 7:25, :] = V0[18:19, 7:25, :] * mx[1]

    for at in (8, 16):
        c = GQ[at : at + 8, :]
        t = roll(c, 1) + roll(c, -1) + roll(c, 6) + roll(c, -6)
        t = t + GQ[at - 1 : at + 7, :] + GQ[at + 1 : at + 9, :]
        j = qj(lane)
        keep = jnp.where(j == 1, mz[-1], jnp.where(j == 4, mz[1], 0.0))
        keep = jnp.where((lane >= 12) & (lane < 108), keep, 0.0)
        VQ[at : at + 8, :] = S * (1.2 * c + S * t) * keep

    inject(VQ, range(2, 18), (8, 16))
    halves = []
    for at in (8, 16):
        c, t = sum0(V0, 2, 16, at)
        halves.append(W0[2:18, at : at + 8, :] * (G0[2:18, at : at + 8, :] - 6.0 * c + t))
    r0 = jnp.concatenate(halves, axis=1)
    g1 = jnp.where(own1, coarsen0(r0, 0.125) * wi1, 0.0)
    send1(g1, "g", 16)

    G1, W1, V1, U1 = r["G1"], r["W1"], r["V1"], r["U1"]
    G2, W2, V2, U2, P2, Q2 = r["G2"], r["W2"], r["V2"], r["U2"], r["P2"], r["Q2"]
    G3, W3, V3, U3, P3 = r["G3"], r["W3"], r["V3"], r["U3"], r["P3"]
    wait_recv(r["RW"], 7)

    def spread(m0, lo, hi, l, m):
        c = jnp.where((l // 32) % 2 == 1, lo * mz[-1], hi * mz[1]) * m
        return m0 * m, c

    def place(m0, c, l, h):
        a = roll(m0, 32 if h == 0 else 96)
        e = roll(c, 96 if h == 0 else 32)
        return jnp.where((l >= 32) & (l < 96), a, e)

    def piece(buf, own, rows, o):
        return own[rows, :] if o == (0, 0, 0) else buf[SLOT[o], rows, :]

    def unpack2(buf, own, dst):
        rows = slice(0, 4)
        for dx in (-1, 0, 1):
            for dy in (-1, 0, 1):
                m0, c = spread(*[piece(buf, own, rows, (dx, dy, dz)) for dz in (0, -1, 1)], lane4, mx[dx] * my[dy])
                for p in range(2):
                    take = lane4 % 2 == p
                    a = jnp.where(take, m0, roll(m0, 1 if p == 0 else -1))
                    e = jnp.where(take, c, roll(c, 1 if p == 0 else -1))
                    for h in range(2):
                        dst[4 + 4 * dx + 2 * h + p, 8 + 4 * dy : 12 + 4 * dy, :] = place(a, e, lane4, h)

    def unpack3(buf, own, rows, dst):
        l = lane[0:2]
        for dx in (-1, 0, 1):
            for dy in (-1, 0, 1):
                m0, c = spread(*[piece(buf, own, rows, (dx, dy, dz)) for dz in (0, -1, 1)], l, mx[dx] * my[dy])
                for h in range(2):
                    dst[4 + 2 * dx + h, 11 + 2 * dy : 13 + 2 * dy, :] = place(m0, c, l, h)

    unpack2(r["RW"], SW, W2)
    unpack3(r["RW"], SW, slice(4, 6), W3)
    r["SX"][0] = W3[6, 8:16, :]
    r["SX"][1] = W3[3, 8:16, :]
    for i in range(8):
        r["SY"][0, i : i + 1, :] = W3[i + 1, 13:14, :]
        r["SY"][1, i : i + 1, :] = W3[i + 1, 10:11, :]
    for i, d in enumerate((-1, 1)):
        send(r["SX"].at[i], r["RSX"].at[1 - i], 20, dev(d, 0, 0))
        send(r["SY"].at[i], r["RSY"].at[1 - i], 21, dev(0, d, 0))

    recv1(w1, "w", 8, W1)
    wait_recv(W0.at[pl.ds(18, 1), gsl], 12)
    wait_recv(W0.at[pl.ds(1, 1), gsl], 13)
    wait_recv(r["RYW"], 14)
    wait_recv(r["RQW"], 15)
    W0[1:2, 8:24, :] = W0[1:2, 8:24, :] * mx[-1]
    W0[18:19, 8:24, :] = W0[18:19, 8:24, :] * mx[1]
    W0[2:18, 7:8, :] = r["RYW"][0] * my[-1]
    W0[2:18, 24:25, :] = r["RYW"][1] * my[1]
    for h in range(2):
        sl = slice(8 * h, 8 * h + 8)
        j = qj(lane)
        v = jnp.where(j == 1, r["RQW"][0, sl, :] * mz[-1], jnp.where(j == 4, r["RQW"][1, sl, :] * mz[1], 0.0))
        r["WQ"][8 + 8 * h : 16 + 8 * h, :] = v

    wait_recv(r["RSX"], 20)
    wait_recv(r["RSY"], 21)
    W3[1, 8:16, :] = r["RSX"][0] * mx[-1]
    W3[8, 8:16, :] = r["RSX"][1] * mx[1]
    for i in range(1, 7):
        W3[i + 1, 8:9, :] = r["RSY"][0, i : i + 1, :] * my[-1]
        W3[i + 1, 15:16, :] = r["RSY"][1, i : i + 1, :] * my[1]

    def inverse(w):
        return jnp.where(w > 0.0, 1.0 / jnp.where(w > 0.0, w, 1.0), 0.0)

    recv1(g1, "g", 16, G1)

    def nsum(a, x, n, at, rows, dil):
        c = a[x : x + n, at : at + rows, :]
        t = a[x - 1 : x + n - 1, at : at + rows, :] + a[x + 1 : x + n + 1, at : at + rows, :]
        t = t + (a[x : x + n, at - 1 : at + rows - 1, :] + a[x : x + n, at + 1 : at + rows + 1, :])
        return c, t + (roll(c, dil) + roll(c, -dil))

    def rowmask(at, rows, low, high):
        y = lax.broadcasted_iota(jnp.int32, (rows, 128), 0) + at
        l = lax.broadcasted_iota(jnp.int32, (rows, 128), 1)
        m = jnp.where(y < low, my[-1], jnp.where(y >= high, my[1], 1.0))
        return m * jnp.where(l < 32, mz[-1], jnp.where(l >= 96, mz[1], 1.0))

    def xmask(a, low, high, x, n, at, rows):
        if low > x:
            a[x:low, at : at + rows, :] = a[x:low, at : at + rows, :] * mx[-1]
        if x + n > high:
            a[high : x + n, at : at + rows, :] = a[high : x + n, at : at + rows, :] * mx[1]

    for at in (4, 12):
        c, t = nsum(G1, 1, 12, at, 8, 1)
        V1[1:13, at : at + 8, :] = S * (1.2 * c + S * t) * rowmask(at, 8, 8, 16)
    xmask(V1, 3, 11, 1, 12, 4, 16)
    c, t = nsum(V1, 3, 8, 8, 8, 1)
    r1 = W1[3:11, 8:16, :] * (G1[3:11, 8:16, :] - 6.0 * c + t)
    g2 = jnp.where(own1[0:4], coarsen1(r1, 0.125) * wi2, 0.0)
    SC = r["SC"]
    SC[...] = pack2(g2)
    send_all(SC, r["RC"], 22)

    P2[4:8, 8:12, :] = g2
    c, t = nsum(P2, 2, 8, 6, 8, 2)
    Q2[2:10, 6:14, :] = S * (1.2 * c + S * t) * rowmask(6, 8, 8, 12)
    xmask(Q2, 4, 8, 2, 8, 6, 8)
    c, t = nsum(Q2, 2, 8, 6, 8, 2)
    res = W2[2:10, 6:14, :] * (P2[2:10, 6:14, :] - 6.0 * c + t)
    C2[...] = jnp.sum(res.reshape(4, 2, 8, 128), axis=1)
    t = C2[:, pl.ds(0, 4, stride=2), :] + C2[:, pl.ds(1, 4, stride=2), :]
    b3 = pair_z(t, 2) * 0.125
    P3[3:7, 10:14, :] = b3 * inverse(W3[3:7, 10:14, :])
    c, t = nsum(P3, 1, 8, 8, 8, 4)
    V3[1:9, 8:16, :] = S * (1.2 * c + S * t) * rowmask(8, 8, 11, 13)
    xmask(V3, 4, 6, 1, 8, 8, 8)
    c, t = nsum(V3, 1, 8, 8, 8, 4)
    res = W3[1:9, 8:16, :] * (P3[1:9, 8:16, :] - 6.0 * c + t)
    T4 = r["T4"]
    T4[0, 8:16, :] = res[0]
    for i in range(3):
        T4[1 + i, 8:16, :] = res[1 + 2 * i] + res[2 + 2 * i]
    T4[4, 8:16, :] = res[7]
    t = T4[:, pl.ds(7, 8, stride=2), :] + T4[:, pl.ds(8, 8, stride=2), :]
    patch = pair_z(t, 4) * 0.125

    msg = zero
    for dx in range(5):
        v = patch[dx]
        main = zero
        for q in range(4):
            lo = 32 + 16 * q + 7
            main = jnp.where((lane >= 2 * q) & (lane < 2 * q + 2), roll(v, 2 * q - lo), main)
        edge = jnp.where(lane < 2, roll(v, 0 - 23), jnp.where(lane < 4, roll(v, 2 - 103), 0.0))
        line = pltpu.roll(main, 0, 1, stride=8, stride_axis=0) + pltpu.roll(edge, 40, 1, stride=4, stride_axis=0)
        line = jnp.sum(line, axis=0, keepdims=True)
        msg = jnp.where(row == ix + (dx - 2), line, msg)
    msg = jnp.where(ih == 1, roll(msg, 64), msg)
    GA, GB, GC = r["GA"], r["GB"], r["GC"]
    SA, SB, SZ = r["SA"], r["SB"], r["SZ"]
    SA[...] = msg
    ga_at = ih * nx + ix
    for d in group_y:
        send(SA, GA.at[ga_at], 23, d)

    wait_recv(GA.at[pl.ds(0, n_y - 1)], 23)
    GA[ga_at] = msg
    SB[...] = jnp.sum(GA[...], axis=0)
    for d in group_x:
        send(SB, GB.at[ixx], 24, d)

    wait_recv(r["RC"], 22)
    unpack2(r["RC"], SC, G2)
    c, t = nsum(G2, 2, 8, 6, 8, 2)
    V2[2:10, 6:14, :] = S * (1.2 * c + S * t) * rowmask(6, 8, 8, 12)
    xmask(V2, 4, 8, 2, 8, 6, 8)
    c, t = nsum(V2, 4, 4, 8, 4, 2)
    res = W2[4:8, 8:12, :] * (G2[4:8, 8:12, :] - 6.0 * c + t)
    C2[0:2, 0:4, :] = jnp.sum(res.reshape(2, 2, 4, 128), axis=1)
    t = C2[0:2, pl.ds(0, 2, stride=2), :] + C2[0:2, pl.ds(1, 2, stride=2), :]
    g3 = jnp.where(own1[0:2], pair_z(t, 2) * 0.125 * wi3, 0.0)
    SD = r["SD"]
    SD[...] = pack3(g3)
    send_all(SD, r["RD"], 25)

    wait_recv(GB.at[pl.ds(0, xn - 1)], 24)
    GB[ixx] = SB[...]
    main = zero
    edges = [zero] * 5
    for k in range(xn):
        v = GB[k]
        for h in range(2):
            if xn == 8 and h == 1:
                continue
            shift = 8 * k - 16 + h * (8 * xn - 64)
            m = roll(v, shift)
            src = (lane - shift + 256) % 128
            if xn != 8:
                m = jnp.where(src // 64 == h, m, 0.0)
            main = main + jnp.where(src % 64 < 40, m, 0.0)
            for dy in range(5):
                a = 40 + 4 * dy
                edges[dy] = edges[dy] + jnp.where((src % 64 >= a) & (src % 64 < a + 4), m, 0.0)
    edge = zero
    for dy in range(5):
        edge = edge + roll(edges[dy], 4 * dy - 40)
    SZ[0] = main
    SZ[1] = edge
    for d in group_z:
        send(SZ, GC.at[iz], 26, d)

    wait_recv(r["RD"], 25)
    unpack3(r["RD"], SD, slice(0, 2), G3)
    c, t = nsum(G3, 4, 2, 11, 2, 4)
    v3 = jnp.where(own1[0:2], S * (1.2 * c + S * t), 0.0)
    SE = r["SE"]
    SE[2:4, :] = pack3(v3)
    SE[1:2, :] = jnp.zeros((1, 128), F32)

    wait_recv(GC.at[pl.ds(0, nz - 1)], 26)
    GC[iz, 0] = SZ[0]
    GC[iz, 1] = SZ[1]
    acc = [zero] * 4
    for z in range(nz):
        v = GC[z, 0]
        if z + 1 < nz:
            v = v + jnp.where(lane % 8 >= 6, roll(GC[z + 1, 1], 6), 0.0)
        if z > 0:
            v = v + jnp.where(lane % 8 < 2, roll(GC[z - 1, 1], -2), 0.0)
        for x in range(nx):
            acc[x % 4] = acc[x % 4] + cp[x * nz + z] * v[x : x + 1, :]
    acc = (acc[0] + acc[1]) + (acc[2] + acc[3])
    tot = jnp.sum(acc, axis=1, keepdims=True)
    e4 = jnp.sum(jnp.where((lane >= 32 + 8 * row) & (lane < 40 + 8 * row), tot, 0.0), axis=0, keepdims=True)
    SE[0:1, :] = e4
    send_all(SE, r["RE"], 27)
    RE = r["RE"]
    wait_recv(RE, 27)

    unpack3(RE, SE, slice(2, 4), V3)
    for x in (1, 8):
        V3[x, 8:16, :] = zero
    for x in range(2, 8):
        V3[x, 8:9, :] = zero[0:1]
        V3[x, 15:16, :] = zero[0:1]
    l1 = lane[0:1]
    par = []
    for dx in (-1, 0, 1):
        v = zero
        for dy in (-1, 0, 1):
            o = (dx, dy, 0)
            own = SE[0:1, :] if o == (0, 0, 0) else RE[SLOT[o], 0:1, :]
            lo, hi = RE[SLOT[(dx, dy, -1)], 0:1, :], RE[SLOT[(dx, dy, 1)], 0:1, :]
            e = jnp.where((l1 >= 32) & (l1 < 96), own, roll(jnp.where(l1 < 64, hi, lo), 64))
            y = 3 + 2 * dy
            v = jnp.where((row == y) | (row == y + 1), e, v)
        par.append(v)
    for i in range(6):
        U3[2 + i, 8:16, :] = V3[2 + i, 8:16, :] + W3[2 + i, 8:16, :] * par[i // 2]
    c, t = nsum(U3, 3, 4, 8, 8, 4)
    E3 = r["E3"]
    E3[...] = (0.2 * c + S * (G3[3:7, 8:16, :] + t)) * inverse(W3[3:7, 8:16, :])
    F2 = r["F2"]
    F2[:, pl.ds(0, 4, stride=2), :] = E3[:, 2:6, :]
    F2[:, pl.ds(1, 4, stride=2), :] = E3[:, 2:6, :]
    for i in range(8):
        U2[2 + i, 6:14, :] = V2[2 + i, 6:14, :] + W2[2 + i, 6:14, :] * F2[i // 2]
    c, t = nsum(U2, 3, 6, 6, 8, 2)
    E2 = r["E2"]
    E2[...] = (0.2 * c + S * (G2[3:9, 6:14, :] + t)) * inverse(W2[3:9, 6:14, :])
    F1 = r["F1"]
    F1[:, pl.ds(2, 6, stride=2), :] = E2[:, 1:7, :]
    F1[:, pl.ds(3, 6, stride=2), :] = E2[:, 1:7, :]
    for i in range(12):
        U1[1 + i, 6:18, :] = V1[1 + i, 6:18, :] + W1[1 + i, 6:18, :] * F1[i // 2, 2:14, :]
    E1 = r["E1"]
    for at in (7, 9):
        c, t = nsum(U1, 2, 10, at, 8, 1)
        E1[:, at - 7 : at + 1, :] = (0.2 * c + S * (G1[2:12, at : at + 8, :] + t)) * inverse(W1[2:12, at : at + 8, :])
    o = select_dot(E1[...].reshape(160, 128), up).reshape(10, 16, 128)
    F0 = r["F0"]
    O1 = r["O1"]
    O1[...] = o
    F0[:, pl.ds(6, 10, stride=2), :] = O1[:, 0:10, :]
    F0[:, pl.ds(7, 10, stride=2), :] = O1[:, 0:10, :]
    acc = zero
    for x in range(8):
        e = E1[x + 1, 1:9, :]
        for p in range(2):
            base = 6 * (2 * x + p + 2)
            acc = jnp.where(lane == base + 1, roll(e, base + 1 - 31), acc)
            acc = jnp.where(lane == base + 4, roll(e, base + 4 - 96), acc)
    UQ = r["UQ"]
    FQ = r["FQ"]
    FQ[...] = acc
    UQ[pl.ds(8, 8, stride=2), :] = FQ[...]
    UQ[pl.ds(9, 8, stride=2), :] = FQ[...]
    UQ[8:24, :] = VQ[8:24, :] + r["WQ"][8:24, :] * UQ[8:24, :]
    for i in range(18):
        V0[1 + i, 7:25, :] = V0[1 + i, 7:25, :] + W0[1 + i, 7:25, :] * F0[(i + 1) // 2, 7:25, :]
    inject(UQ, range(2, 18), (8, 16))
    for at in (8, 16):
        c, t = sum0(V0, 2, 16, at)
        out_ref[:, at - 8 : at, :] = (0.2 * c + S * (G0[2:18, at : at + 8, :] + t)) / w_ref[:, at - 8 : at, :]

    wait_send(G0.at[pl.ds(2, 2), gsl], 0)
    wait_send(G0.at[pl.ds(16, 2), gsl], 1)
    wait_send(r["YS"].at[0], 2)
    wait_send(r["YS"].at[1], 3)
    for name, key in (("RXY", 4), ("RQ", 5), ("RQE", 6), ("RW", 7), ("RYW", 14), ("RQW", 15), ("RSX", 20), ("RSY", 21)):
        wait_send(r[name], key)
    wait_send(W0.at[pl.ds(2, 1), gsl], 12)
    wait_send(W0.at[pl.ds(17, 1), gsl], 13)
    for n, key in (("w", 8), ("g", 16)):
        for i, name in enumerate(("RX1", "RY1", "RXY1", "RZ1")):
            wait_send(r[name + n], key + i)
    wait_send(r["RC"], 22)
    wait_send(GA.at[pl.ds(0, n_y - 1)], 23)
    wait_send(GB.at[pl.ds(0, xn - 1)], 24)
    wait_send(r["RD"], 25)
    wait_send(GC.at[pl.ds(0, nz - 1)], 26)
    wait_send(r["RE"], 27)


def scratch(dims):
    nx, ny, nz = dims
    xn = ny // 2
    v = {
        "G0": (20, 32, 128), "W0": (20, 32, 128), "V0": (20, 32, 128), "INJ": (20, 32, 128),
        "GQ": (32, 128), "VQ": (32, 128), "WQ": (32, 128), "UQ": (32, 128),
        "YS": (2, 16, 2, 128), "RY": (2, 16, 2, 128), "RXY": (4, 2, 128),
        "QS": (16, 128), "QW": (16, 128), "RQ": (6, 16, 128), "QE": (2, 1, 128), "RQE": (4, 1, 128),
        "YW": (2, 16, 1, 128), "RYW": (2, 16, 1, 128), "RQW": (2, 16, 128),
        "C0": (8, 16, 128), "C1": (4, 8, 128), "C2": (4, 8, 128),
        "S1": (8, 8, 128), "SW": (8, 128), "RW": (26, 8, 128),
        "G1": (14, 24, 128), "W1": (14, 24, 128), "V1": (14, 24, 128), "U1": (14, 24, 128),
        "G2": (12, 24, 128), "W2": (12, 24, 128), "V2": (12, 24, 128), "U2": (12, 24, 128),
        "P2": (12, 24, 128), "Q2": (12, 24, 128),
        "G3": (10, 24, 128), "W3": (10, 24, 128), "V3": (10, 24, 128), "U3": (10, 24, 128), "P3": (10, 24, 128),
        "T4": (5, 24, 128), "SX": (2, 8, 128), "SY": (2, 8, 128), "RSX": (2, 8, 128), "RSY": (2, 8, 128),
        "SC": (4, 128), "RC": (26, 4, 128), "SD": (2, 128), "RD": (26, 2, 128), "SE": (4, 128), "RE": (26, 4, 128),
        "SA": (8, 128), "SB": (8, 128), "SZ": (2, 8, 128),
        "GA": (2 * nx, 8, 128), "GB": (xn, 8, 128), "GC": (nz, 2, 8, 128), "CP": (nx * nz, 8, 128),
        "E3": (4, 8, 128), "F2": (4, 8, 128), "E2": (6, 8, 128), "F1": (6, 16, 128),
        "E1": (10, 16, 128), "O1": (10, 16, 128), "F0": (10, 32, 128), "FQ": (8, 128),
    }
    for n in "wg":
        v["S1" + n] = (8, 8, 128)
        v["YS1" + n] = (2, 8, 4, 128)
        v["ZS1" + n] = (8, 128)
        v["RX1" + n] = (2, 3, 8, 128)
        v["RY1" + n] = (2, 8, 4, 128)
        v["RXY1" + n] = (4, 3, 4, 128)
        v["RZ1" + n] = (18, 8, 128)
    return v


def solution(mesh):
    dims = tuple(mesh.shape[a] for a in ("gx", "gy", "gz"))
    sizes = scratch(dims)

    def body(*args):
        names = ["b", "w", "c", "out"] + list(sizes) + ["ssem", "rsem"]
        kernel(dims, dict(zip(names, args)))

    def per_device(sources, stiffness, coarse_inverse):
        vmem = pl.BlockSpec(memory_space=pltpu.VMEM)
        e = pl.pallas_call(
            body,
            out_shape=jax.ShapeDtypeStruct((16, 16, 128), F32),
            in_specs=[vmem] * 3,
            out_specs=vmem,
            scratch_shapes=[pltpu.VMEM(s, F32) for s in sizes.values()] + [pltpu.SemaphoreType.DMA((28,))] * 2,
            compiler_params=pltpu.CompilerParams(collective_id=0, has_side_effects=True),
            name="vcycle",
        )(sources, stiffness, coarse_inverse)
        return e[None]

    return jax.shard_map(
        per_device,
        mesh=mesh,
        in_specs=(P(None, "gx", "gy", "gz"), P("gx", "gy", "gz"), P(("gx", "gy", "gz"), None)),
        out_specs=P(None, "gx", "gy", "gz"),
        check_vma=False,
    )
```

```python
import functools
import itertools

import jax
import jax.numpy as jnp
from jax import lax
from jax.experimental import pallas as pl
from jax.experimental.pallas import tpu as pltpu
from jax.sharding import PartitionSpec as P

MESH = pl.DeviceIdType.MESH
F32 = jnp.float32
S = 0.8 / 6.0
OFFS = [o for o in itertools.product((-1, 0, 1), repeat=3) if o != (0, 0, 0)]
SLOT = {o: i for i, o in enumerate(OFFS)}
ZOFFS = [o for o in OFFS if o[2] != 0]
ZSLOT = {o: i for i, o in enumerate(ZOFFS)}
XY = [(-1, -1), (-1, 1), (1, -1), (1, 1)]
XZ = [(0, -1), (0, 1)] + XY


def neg(o):
    return tuple(-v for v in o)


def roll(v, shift):
    shift = shift % 128
    return v if shift == 0 else pltpu.roll(v, shift, v.ndim - 1)


def split2(v):
    hi = v.astype(jnp.bfloat16)
    lo = (v - hi.astype(F32)).astype(jnp.bfloat16)
    return jnp.concatenate([hi, lo], axis=1)


def select_dot(v, sel):
    return jnp.dot(split2(v), sel, preferred_element_type=F32)


def kernel(dims, refs):
    nx, ny, nz = dims
    xn = ny // 2
    n_y = nx * 2
    r = refs
    ix, iy, iz = lax.axis_index("gx"), lax.axis_index("gy"), lax.axis_index("gz")
    ih, ixx = iy // xn, iy % xn

    def dev(dx, dy, dz):
        return {
            "gx": lax.rem(ix + dx + nx, nx),
            "gy": lax.rem(iy + dy + ny, ny),
            "gz": lax.rem(iz + dz + nz, nz),
        }

    def copy(src, dst, key, slot, device):
        return pltpu.make_async_remote_copy(
            src_ref=src,
            dst_ref=dst,
            send_sem=r["ssem"].at[key, slot],
            recv_sem=r["rsem"].at[key, slot],
            device_id=device,
            device_id_type=MESH,
        )

    cx = {-1: ix > 0, 1: ix < nx - 1}
    cy = {-1: iy > 0, 1: iy < ny - 1}
    cz = {-1: iz > 0, 1: iz < nz - 1}

    def has(o):
        c = [f[v] for f, v in zip((cx, cy, cz), o) if v]
        return functools.reduce(jnp.logical_and, c)

    def keep(v, *o):
        return jnp.where(has(o), v, 0.0) if any(o) else v

    sent = []

    def exchange(key, o, src, dst, back):
        slot = SLOT[o]
        sent.append((o, src, key, slot))

        @pl.when(has(o))
        def _():
            copy(src, dst, key, slot, dev(*o)).start()

        def wait():
            @pl.when(has(neg(o)))
            def _():
                copy(back, back, key, slot, right).wait_recv()

        return wait

    def to_group(key, src, dst, group):
        for k, d in enumerate(group):
            copy(src, dst, key, k, d).start()

    def from_group(key, buf, n):
        for k in range(n):
            copy(buf.at[0], buf.at[0], key, k, right).wait_recv()

    def run(waits):
        for w in waits:
            w()

    me = {"gx": ix, "gy": iy, "gz": iz}
    right = {"gx": lax.rem(ix + 1, nx), "gy": iy, "gz": iz}

    group_y = []
    for k in range(1, n_y):
        t = lax.rem(ih * nx + ix + k, n_y)
        group_y.append({"gx": t % nx, "gy": (t // nx) * xn + ixx, "gz": iz})
    group_x = [{"gx": ix, "gy": ih * xn + lax.rem(ixx + k, xn), "gz": iz} for k in range(1, xn)]
    group_z = [{"gx": ix, "gy": iy, "gz": lax.rem(iz + k, nz)} for k in range(1, nz)]

    barrier = pltpu.get_barrier_semaphore()
    loads = [pltpu.make_async_copy(r[a], r[b], r["lsem"].at[i]) for i, (a, b) in enumerate((("b", "B0"), ("w", "A0"), ("c", "CM")))]
    for c in loads:
        c.start()
    for o in OFFS:

        @pl.when(has(o))
        def _():
            pl.semaphore_signal(barrier, inc=1, device_id=dev(*o), device_id_type=MESH)

    for d in group_y + group_x + group_z:
        pl.semaphore_signal(barrier, inc=1, device_id=d, device_id_type=MESH)
    partners = sum(jnp.where(has(o), 1, 0) for o in OFFS) + len(group_y + group_x + group_z)

    lane = lax.broadcasted_iota(jnp.int32, (8, 128), 1)
    row = lax.broadcasted_iota(jnp.int32, (8, 128), 0)
    zero = jnp.zeros((8, 128), F32)

    def flag(c):
        return jnp.where(c, jnp.float32(1), jnp.float32(0))

    mx = {-1: flag(ix > 0), 0: jnp.float32(1), 1: flag(ix < nx - 1)}
    my = {-1: flag(iy > 0), 0: jnp.float32(1), 1: flag(iy < ny - 1)}
    mz = {-1: flag(iz > 0), 0: jnp.float32(1), 1: flag(iz < nz - 1)}
    zmask = jnp.where(lane < 32, mz[-1], jnp.where(lane >= 96, mz[1], 1.0))

    b_ref, w_ref, c_ref, out_ref = r["B0"], r["A0"], r["CM"], r["out"]

    G0, W0, V0 = r["G0"], r["W0"], r["V0"]
    loads[0].wait()
    loads[1].wait()
    w0 = w_ref[...]
    g0 = b_ref[0] / w0
    W0[2:18, 8:24, :] = w0
    G0[2:18, 8:24, :] = g0

    r["YS"][0] = G0[2:18, 8:10, :]
    r["YS"][1] = G0[2:18, 22:24, :]

    def pack_q(src, dst):
        for h in range(2):
            acc = zero
            for x in range(16):
                m = src[x + 2, 8 + 8 * h : 16 + 8 * h, :]
                base = 6 * (x + 2)
                acc = jnp.where((lane >= base) & (lane < base + 3), roll(m, base - 126), acc)
                acc = jnp.where((lane >= base + 3) & (lane < base + 6), roll(m, base + 3 - 127), acc)
            dst[8 * h : 8 * h + 8, :] = acc

    pack_q(G0, r["QS"])
    r["QE"][0] = r["QS"][0:1, :]
    r["QE"][1] = r["QS"][15:16, :]

    pl.semaphore_wait(barrier, partners)

    gsl = pl.ds(8, 16)
    wait_g0 = [
        exchange(0, (-1, 0, 0), G0.at[pl.ds(2, 2), gsl], G0.at[pl.ds(18, 2), gsl], G0.at[pl.ds(18, 2), gsl]),
        exchange(0, (1, 0, 0), G0.at[pl.ds(16, 2), gsl], G0.at[pl.ds(0, 2), gsl], G0.at[pl.ds(0, 2), gsl]),
    ]
    for i, d in enumerate((-1, 1)):
        wait_g0.append(exchange(0, (0, d, 0), r["YS"].at[i], r["RY"].at[1 - i], r["RY"].at[1 - i]))
    for dx, dy in XY:
        src = r["YS"].at[(dy + 1) // 2, 0 if dx < 0 else 15]
        dst = r["RXY"].at[XY.index((-dx, -dy))]
        wait_g0.append(exchange(0, (dx, dy, 0), src, dst, dst))
    for dx, dz in XZ:
        dst = r["RQ"].at[XZ.index((-dx, -dz))]
        wait_g0.append(exchange(0, (dx, 0, dz), r["QS"], dst, dst))
    for dy, dz in XY:
        dst = r["RQE"].at[XY.index((-dy, -dz))]
        wait_g0.append(exchange(0, (0, dy, dz), r["QE"].at[(dy + 1) // 2], dst, dst))

    for name in ("G0", "W0", "V0"):
        a = r[name]
        a[:, 0:8, :] = jnp.zeros((20, 8, 128), F32)
        a[:, 24:32, :] = jnp.zeros((20, 8, 128), F32)
    for name in ("GQ", "WQ", "VQ", "UQ", "G1", "W1", "V1", "U1", "G2", "W2", "V2", "U2", "P2", "Q2", "G3", "W3", "V3", "U3", "P3", "T4"):
        r[name][...] = jnp.zeros(r[name].shape, F32)

    zr = lax.broadcasted_iota(jnp.int32, (256, 128), 0) % 128
    zc = lax.broadcasted_iota(jnp.int32, (256, 128), 1)
    down = jnp.where(zc == 32 + zr // 2, jnp.float32(1), jnp.float32(0)).astype(jnp.bfloat16)
    up = jnp.where(zr == 32 + zc // 2, jnp.float32(1), jnp.float32(0)).astype(jnp.bfloat16)

    C0 = r["C0"]

    def coarsen0(values, scale):
        C0[...] = jnp.sum(values.reshape(8, 2, 16, 128), axis=1)
        t = C0[:, pl.ds(0, 8, stride=2), :] + C0[:, pl.ds(1, 8, stride=2), :]
        return (select_dot(t.reshape(64, 128), down) * scale).reshape(8, 8, 128)

    def pair_z(t, dil):
        ln = lax.broadcasted_iota(jnp.int32, t.shape, t.ndim - 1)
        return t + jnp.where((ln // dil) % 2 == 0, roll(t, -dil), roll(t, dil))

    C1, C2 = r["C1"], r["C2"]

    def coarsen1(values, scale):
        n = values.shape[0] // 2
        C1[...] = jnp.sum(values.reshape(n, 2, 8, 128), axis=1)
        t = C1[:, pl.ds(0, 4, stride=2), :] + C1[:, pl.ds(1, 4, stride=2), :]
        return pair_z(t, 1) * scale

    S1 = r["S1"]
    w1 = coarsen0(w0, 0.0625)
    own1 = (lane >= 32) & (lane < 96)
    w2 = coarsen1(w1, 0.0625)
    C2[0:4, 0:4, :] = w2
    t = C2[0:4, pl.ds(0, 2, stride=2), :] + C2[0:4, pl.ds(1, 2, stride=2), :]
    w3 = pair_z(jnp.sum(t.reshape(2, 2, 2, 128), axis=1), 2) * 0.0625

    lane4 = lane[0:4]

    def pack2(v):
        halves = []
        for h in range(2):
            a = jnp.where(lane4 % 2 == 0, v[2 * h], v[2 * h + 1])
            halves.append(roll(a, -32 if h == 0 else 32))
        return jnp.where(lane4 < 64, halves[0], halves[1])

    def pack3(v):
        return jnp.where(lane[0:2] < 64, roll(v[0], -32), roll(v[1], 32))

    SW = r["SW"]
    SW[0:4, :] = pack2(w2)
    SW[4:6, :] = pack3(w3)
    SW[6:8, :] = jnp.zeros((2, 128), F32)

    def send_all(src, dst, key):
        return [exchange(key, o, src, dst.at[SLOT[neg(o)]], dst.at[SLOT[neg(o)]]) for o in OFFS]

    wait_w = send_all(SW, r["RW"], 1)

    def send1(own, n, key):
        s1, ys, zs = r["S1" + n], r["YS1" + n], r["ZS1" + n]
        s1[...] = own
        ys[0] = s1[:, 0:4, :]
        ys[1] = s1[:, 4:8, :]
        acc = zero
        for x in range(8):
            acc = jnp.where((lane >= 16 * x) & (lane < 16 * x + 4), roll(own[x], 16 * x - 32), acc)
            acc = jnp.where((lane >= 16 * x + 4) & (lane < 16 * x + 8), roll(own[x], 16 * x + 4 - 92), acc)
        zs[...] = acc
        rx, ry, rxy, rz = (r[name + n] for name in ("RX1", "RY1", "RXY1", "RZ1"))
        waits = [
            exchange(key, (-1, 0, 0), s1.at[pl.ds(0, 3)], rx.at[1], rx.at[1]),
            exchange(key, (1, 0, 0), s1.at[pl.ds(5, 3)], rx.at[0], rx.at[0]),
            exchange(key, (0, -1, 0), ys.at[0], ry.at[1], ry.at[1]),
            exchange(key, (0, 1, 0), ys.at[1], ry.at[0], ry.at[0]),
        ]
        for dx, dy in XY:
            src = ys.at[(dy + 1) // 2, pl.ds(0 if dx < 0 else 5, 3)]
            dst = rxy.at[XY.index((-dx, -dy))]
            waits.append(exchange(key, (dx, dy, 0), src, dst, dst))
        for o in ZOFFS:
            if n == "g" or 0 in o:
                waits.append(exchange(key, o, zs, rz.at[ZSLOT[neg(o)]], rz.at[ZSLOT[neg(o)]]))
        return waits

    def recv1(own, n, key, dst):
        run(key)
        for x in range(14):
            dx = -1 if x < 3 else (1 if x > 10 else 0)
            for dy in (-1, 0, 1):
                if dx == 0 and dy == 0:
                    base = own[x - 3]
                elif dy == 0:
                    base = r["RX1" + n][(dx + 1) // 2, x if dx < 0 else x - 11]
                elif dx == 0:
                    base = r["RY1" + n][(dy + 1) // 2, x - 3]
                else:
                    base = r["RXY1" + n][XY.index((dx, dy)), x if dx < 0 else x - 11]
                sx = x - 3 if dx == 0 else (x + 5 if dx < 0 else x - 11)
                rows = slice(0, 8) if dy == 0 else (slice(4, 8) if dy < 0 else slice(0, 4))
                lo = r["RZ1" + n][ZSLOT[(dx, dy, -1)], rows, :]
                hi = r["RZ1" + n][ZSLOT[(dx, dy, 1)], rows, :]
                ln = lane[0:8] if dy == 0 else lane4
                v = keep(base, dx, dy, 0)
                if n == "g" or dx == 0 or dy == 0:
                    v = jnp.where((ln >= 28) & (ln < 32), keep(roll(lo, 28 - 16 * sx - 4), dx, dy, -1), v)
                    v = jnp.where((ln >= 96) & (ln < 100), keep(roll(hi, 96 - 16 * sx), dx, dy, 1), v)
                at = 8 if dy == 0 else (4 if dy < 0 else 16)
                dst[x, at : at + (8 if dy == 0 else 4), :] = v

    wait_w1 = send1(w1, "w", 2)

    r["YW"][0] = W0[2:18, 8:9, :]
    r["YW"][1] = W0[2:18, 23:24, :]
    pack_q(W0, r["QW"])
    wait_w0 = [
        exchange(3, (-1, 0, 0), W0.at[pl.ds(2, 1), gsl], W0.at[pl.ds(18, 1), gsl], W0.at[pl.ds(18, 1), gsl]),
        exchange(3, (1, 0, 0), W0.at[pl.ds(17, 1), gsl], W0.at[pl.ds(1, 1), gsl], W0.at[pl.ds(1, 1), gsl]),
    ]
    for i, d in enumerate((-1, 1)):
        wait_w0.append(exchange(3, (0, d, 0), r["YW"].at[i], r["RYW"].at[1 - i], r["RYW"].at[1 - i]))
        wait_w0.append(exchange(3, (0, 0, d), r["QW"], r["RQW"].at[1 - i], r["RQW"].at[1 - i]))

    wi1 = 1.0 / jnp.where(own1, w1, 1.0)
    wi2 = 1.0 / jnp.where(own1[0:4], w2, 1.0)

    GQ, VQ = r["GQ"], r["VQ"]
    run(wait_g0)
    G0[0:2, 8:24, :] = keep(G0[0:2, 8:24, :], -1, 0, 0)
    G0[18:20, 8:24, :] = keep(G0[18:20, 8:24, :], 1, 0, 0)
    G0[2:18, 6:8, :] = keep(r["RY"][0], 0, -1, 0)
    G0[2:18, 24:26, :] = keep(r["RY"][1], 0, 1, 0)
    for dx, dy in XY:
        v = keep(r["RXY"][XY.index((dx, dy))], dx, dy, 0)
        G0[1 if dx < 0 else 18, 7 if dy < 0 else 24, :] = v[1 if dy < 0 else 0, :]

    def qj(ln):
        return ln % 6

    for h in range(2):
        sl = slice(8 * h, 8 * h + 8)
        own = r["QS"][sl, :]
        j = qj(lane)
        q = [keep(r["RQ"][i, sl, :], dx, 0, dz) for i, (dx, dz) in enumerate(XZ)]
        v, lo, hi = (jnp.where(j < 2, q[2 * i], jnp.where(j > 3, q[2 * i + 1], own if i == 0 else 0.0)) for i in range(3))
        v = jnp.where((lane >= 6) & (lane < 12), roll(lo, 6 - 102), jnp.where((lane >= 108) & (lane < 114), roll(hi, 108 - 12), v))
        GQ[8 + 8 * h : 16 + 8 * h, :] = jnp.where((lane >= 6) & (lane < 114), v, 0.0)
    for dy, at in ((-1, 7), (1, 24)):
        j = qj(lane[0:1])
        lo = keep(r["RQE"][XY.index((dy, -1))], 0, dy, -1)
        hi = keep(r["RQE"][XY.index((dy, 1))], 0, dy, 1)
        v = jnp.where(j < 2, lo, jnp.where(j > 3, hi, 0.0))
        GQ[at : at + 1, :] = jnp.where((lane[0:1] >= 12) & (lane[0:1] < 108), v, 0.0)

    INJ = r["INJ"]

    def inject(q, xs, tiles):
        for at in tiles:
            m = q[at : at + 8, :]
            for xp in xs:
                a = roll(m, -(6 * xp + 1))
                c = roll(m, 127 - (6 * xp + 4))
                INJ[xp, at : at + 8, :] = jnp.where(lane == 0, a, jnp.where(lane == 127, c, 0.0))

    def sum0(a, x, n, at):
        c = a[x : x + n, at : at + 8, :]
        t = a[x - 1 : x + n - 1, at : at + 8, :] + a[x + 1 : x + n + 1, at : at + 8, :]
        t = t + (a[x : x + n, at - 1 : at + 7, :] + a[x : x + n, at + 1 : at + 9, :])
        z = jnp.where(lane == 0, 0.0, roll(c, 1)) + jnp.where(lane == 127, 0.0, roll(c, -1))
        return c, t + (z + INJ[x : x + n, at : at + 8, :])

    inject(GQ, range(1, 19), (7, 15, 17))
    for at in (7, 15, 17):
        c, t = sum0(G0, 1, 18, at)
        v = S * (1.2 * c + S * t)
        if at == 7:
            v = v * jnp.where(row == 0, my[-1], 1.0)
        if at == 17:
            v = v * jnp.where(row == 7, my[1], 1.0)
        V0[1:19, at : at + 8, :] = v
    V0[1:2, 7:25, :] = V0[1:2, 7:25, :] * mx[-1]
    V0[18:19, 7:25, :] = V0[18:19, 7:25, :] * mx[1]

    for at in (8, 16):
        c = GQ[at : at + 8, :]
        t = roll(c, 1) + roll(c, -1) + roll(c, 6) + roll(c, -6)
        t = t + GQ[at - 1 : at + 7, :] + GQ[at + 1 : at + 9, :]
        j = qj(lane)
        mask = jnp.where(j == 1, mz[-1], jnp.where(j == 4, mz[1], 0.0))
        mask = jnp.where((lane >= 12) & (lane < 108), mask, 0.0)
        VQ[at : at + 8, :] = S * (1.2 * c + S * t) * mask

    inject(VQ, range(2, 18), (8, 16))
    halves = []
    for at in (8, 16):
        c, t = sum0(V0, 2, 16, at)
        halves.append(W0[2:18, at : at + 8, :] * (G0[2:18, at : at + 8, :] - 6.0 * c + t))
    r0 = jnp.concatenate(halves, axis=1)
    g1 = jnp.where(own1, coarsen0(r0, 0.125) * wi1, 0.0)
    wait_g1 = send1(g1, "g", 4)

    G1, W1, V1, U1 = r["G1"], r["W1"], r["V1"], r["U1"]
    G2, W2, V2, U2, P2, Q2 = r["G2"], r["W2"], r["V2"], r["U2"], r["P2"], r["Q2"]
    G3, W3, V3, U3, P3 = r["G3"], r["W3"], r["V3"], r["U3"], r["P3"]
    run(wait_w)

    def spread(m0, lo, hi, l, dx, dy):
        return keep(m0, dx, dy, 0), jnp.where((l // 32) % 2 == 1, keep(lo, dx, dy, -1), keep(hi, dx, dy, 1))

    def place(m0, c, l, h):
        a = roll(m0, 32 if h == 0 else 96)
        e = roll(c, 96 if h == 0 else 32)
        return jnp.where((l >= 32) & (l < 96), a, e)

    def piece(buf, own, rows, o):
        return own[rows, :] if o == (0, 0, 0) else buf[SLOT[o], rows, :]

    def unpack2(buf, own, dst):
        rows = slice(0, 4)
        for dx in (-1, 0, 1):
            for dy in (-1, 0, 1):
                m0, c = spread(*[piece(buf, own, rows, (dx, dy, dz)) for dz in (0, -1, 1)], lane4, dx, dy)
                for p in range(2):
                    take = lane4 % 2 == p
                    a = jnp.where(take, m0, roll(m0, 1 if p == 0 else -1))
                    e = jnp.where(take, c, roll(c, 1 if p == 0 else -1))
                    for h in range(2):
                        dst[4 + 4 * dx + 2 * h + p, 8 + 4 * dy : 12 + 4 * dy, :] = place(a, e, lane4, h)

    def unpack3(buf, own, rows, dst):
        l = lane[0:2]
        for dx in (-1, 0, 1):
            for dy in (-1, 0, 1):
                m0, c = spread(*[piece(buf, own, rows, (dx, dy, dz)) for dz in (0, -1, 1)], l, dx, dy)
                for h in range(2):
                    dst[4 + 2 * dx + h, 11 + 2 * dy : 13 + 2 * dy, :] = place(m0, c, l, h)

    unpack2(r["RW"], SW, W2)
    unpack3(r["RW"], SW, slice(4, 6), W3)
    r["SX"][0] = W3[6, 8:16, :]
    r["SX"][1] = W3[3, 8:16, :]
    for i in range(8):
        r["SY"][0, i : i + 1, :] = W3[i + 1, 13:14, :]
        r["SY"][1, i : i + 1, :] = W3[i + 1, 10:11, :]
    wait_s = []
    for i, d in enumerate((-1, 1)):
        wait_s.append(exchange(5, (d, 0, 0), r["SX"].at[i], r["RSX"].at[1 - i], r["RSX"].at[1 - i]))
        wait_s.append(exchange(5, (0, d, 0), r["SY"].at[i], r["RSY"].at[1 - i], r["RSY"].at[1 - i]))

    recv1(w1, "w", wait_w1, W1)
    run(wait_w0)
    W0[1:2, 8:24, :] = keep(W0[1:2, 8:24, :], -1, 0, 0)
    W0[18:19, 8:24, :] = keep(W0[18:19, 8:24, :], 1, 0, 0)
    W0[2:18, 7:8, :] = keep(r["RYW"][0], 0, -1, 0)
    W0[2:18, 24:25, :] = keep(r["RYW"][1], 0, 1, 0)
    for h in range(2):
        sl = slice(8 * h, 8 * h + 8)
        j = qj(lane)
        v = jnp.where(j == 1, keep(r["RQW"][0, sl, :], 0, 0, -1), jnp.where(j == 4, keep(r["RQW"][1, sl, :], 0, 0, 1), 0.0))
        r["WQ"][8 + 8 * h : 16 + 8 * h, :] = v

    def inverse(w):
        return jnp.where(w > 0.0, 1.0 / jnp.where(w > 0.0, w, 1.0), 0.0)

    recv1(g1, "g", wait_g1, G1)

    def nsum(a, x, n, at, rows, dil):
        c = a[x : x + n, at : at + rows, :]
        t = a[x - 1 : x + n - 1, at : at + rows, :] + a[x + 1 : x + n + 1, at : at + rows, :]
        t = t + (a[x : x + n, at - 1 : at + rows - 1, :] + a[x : x + n, at + 1 : at + rows + 1, :])
        return c, t + (roll(c, dil) + roll(c, -dil))

    def rowmask(at, rows, low, high):
        y = lax.broadcasted_iota(jnp.int32, (rows, 128), 0) + at
        l = lax.broadcasted_iota(jnp.int32, (rows, 128), 1)
        m = jnp.where(y < low, my[-1], jnp.where(y >= high, my[1], 1.0))
        return m * jnp.where(l < 32, mz[-1], jnp.where(l >= 96, mz[1], 1.0))

    def xmask(a, low, high, x, n, at, rows):
        if low > x:
            a[x:low, at : at + rows, :] = a[x:low, at : at + rows, :] * mx[-1]
        if x + n > high:
            a[high : x + n, at : at + rows, :] = a[high : x + n, at : at + rows, :] * mx[1]

    for at in (4, 12):
        c, t = nsum(G1, 1, 12, at, 8, 1)
        V1[1:13, at : at + 8, :] = S * (1.2 * c + S * t) * rowmask(at, 8, 8, 16)
    xmask(V1, 3, 11, 1, 12, 4, 16)
    c, t = nsum(V1, 3, 8, 8, 8, 1)
    r1 = W1[3:11, 8:16, :] * (G1[3:11, 8:16, :] - 6.0 * c + t)
    g2 = jnp.where(own1[0:4], coarsen1(r1, 0.125) * wi2, 0.0)

    P2[4:8, 8:12, :] = g2
    c, t = nsum(P2, 2, 8, 6, 8, 2)
    Q2[2:10, 6:14, :] = S * (1.2 * c + S * t) * rowmask(6, 8, 8, 12)
    xmask(Q2, 4, 8, 2, 8, 6, 8)
    c, t = nsum(Q2, 2, 8, 6, 8, 2)
    res = W2[2:10, 6:14, :] * (P2[2:10, 6:14, :] - 6.0 * c + t)
    C2[...] = jnp.sum(res.reshape(4, 2, 8, 128), axis=1)
    t = C2[:, pl.ds(0, 4, stride=2), :] + C2[:, pl.ds(1, 4, stride=2), :]
    b3 = pair_z(t, 2) * 0.125
    SC = r["SC"]
    SC[0:4, :] = pack2(g2)
    l4 = lane4 % 4
    SC[4:8, :] = jnp.where(l4 < 2, jnp.where(l4 == 0, b3[0], b3[1]), jnp.where(l4 == 2, b3[2], b3[3]))
    wait_c = send_all(SC, r["RC"], 6)
    run(wait_s)
    W3[1, 8:16, :] = keep(r["RSX"][0], -1, 0, 0)
    W3[8, 8:16, :] = keep(r["RSX"][1], 1, 0, 0)
    for i in range(1, 7):
        W3[i + 1, 8:9, :] = keep(r["RSY"][0, i : i + 1, :], 0, -1, 0)
        W3[i + 1, 15:16, :] = keep(r["RSY"][1, i : i + 1, :], 0, 1, 0)
    P3[3:7, 10:14, :] = b3 * inverse(W3[3:7, 10:14, :])
    c, t = nsum(P3, 1, 8, 8, 8, 4)
    V3[1:9, 8:16, :] = S * (1.2 * c + S * t) * rowmask(8, 8, 11, 13)
    xmask(V3, 4, 6, 1, 8, 8, 8)
    c, t = nsum(V3, 1, 8, 8, 8, 4)
    res = W3[1:9, 8:16, :] * (P3[1:9, 8:16, :] - 6.0 * c + t)
    T4 = r["T4"]
    T4[0, 8:16, :] = res[0]
    for i in range(3):
        T4[1 + i, 8:16, :] = res[1 + 2 * i] + res[2 + 2 * i]
    T4[4, 8:16, :] = res[7]
    t = T4[:, pl.ds(7, 8, stride=2), :] + T4[:, pl.ds(8, 8, stride=2), :]
    patch = pair_z(t, 4) * 0.125

    msg = zero
    for dx in range(5):
        v = patch[dx]
        main = zero
        for q in range(4):
            lo = 32 + 16 * q + 7
            main = jnp.where((lane >= 2 * q) & (lane < 2 * q + 2), roll(v, 2 * q - lo), main)
        edge = jnp.where(lane < 2, roll(v, 0 - 23), jnp.where(lane < 4, roll(v, 2 - 103), 0.0))
        line = pltpu.roll(main, 0, 1, stride=8, stride_axis=0) + pltpu.roll(edge, 40, 1, stride=4, stride_axis=0)
        line = jnp.sum(line, axis=0, keepdims=True)
        msg = jnp.where(row == ix + (dx - 2), line, msg)
    msg = jnp.where(ih == 1, roll(msg, 64), msg)
    GA, GB, GC = r["GA"], r["GB"], r["GC"]
    SA, SB, SZ = r["SA"], r["SB"], r["SZ"]
    SA[...] = msg
    ga_at = ih * nx + ix
    to_group(8, SA, GA.at[ga_at], group_y)

    cp = r["CP"]
    loads[2].wait()

    @pl.loop(0, nx)
    def _(x):
        for z in range(nz):
            acc = zero
            for p in range(ny // 2):
                tile = c_ref[:, pl.ds(pl.multiple_of((x * (ny // 2) + p) * 128, 128), 128)]
                for q in range(2):
                    y = 2 * p + q
                    at = 8 * y
                    acc = jnp.where((lane >= at) & (lane < at + 8), roll(tile, at - 64 * q - 8 * z), acc)
            cp[x * nz + z] = acc

    from_group(8, GA, n_y - 1)
    GA[ga_at] = msg
    SB[...] = jnp.sum(GA[...], axis=0)
    to_group(9, SB, GB.at[ixx], group_x)

    from_group(9, GB, xn - 1)
    GB[ixx] = SB[...]
    main = zero
    edges = [zero] * 5
    for k in range(xn):
        v = GB[k]
        for h in range(2):
            if xn == 8 and h == 1:
                continue
            shift = 8 * k - 16 + h * (8 * xn - 64)
            m = roll(v, shift)
            src = (lane - shift + 256) % 128
            if xn != 8:
                m = jnp.where(src // 64 == h, m, 0.0)
            main = main + jnp.where(src % 64 < 40, m, 0.0)
            for dy in range(5):
                a = 40 + 4 * dy
                edges[dy] = edges[dy] + jnp.where((src % 64 >= a) & (src % 64 < a + 4), m, 0.0)
    edge = zero
    for dy in range(5):
        edge = edge + roll(edges[dy], 4 * dy - 40)
    SZ[0] = main
    SZ[1] = edge
    to_group(10, SZ, GC.at[iz], group_z)

    run(wait_c)
    unpack2(r["RC"], SC, G2)
    c, t = nsum(G2, 2, 8, 6, 8, 2)
    V2[2:10, 6:14, :] = S * (1.2 * c + S * t) * rowmask(6, 8, 8, 12)
    xmask(V2, 4, 8, 2, 8, 6, 8)

    TB, TC, RC = r["TB"], r["TC"], r["RC"]
    for dy in (-1, 0, 1):
        acc = jnp.zeros((4, 128), F32)
        for dx in (-1, 0, 1):
            m0, lo, hi = (keep(piece(RC, SC, slice(4, 8), (dx, dy, dz)), dx, dy, dz) for dz in (0, -1, 1))
            e = jnp.where((lane4 >= 92) & (lane4 < 100), lo, jnp.where((lane4 >= 28) & (lane4 < 36), hi, 0.0))
            q = m0 + roll(e, 64)
            if dx < 0:
                q = jnp.where(l4 < 2, roll(q, -2), 0.0)
            if dx > 0:
                q = jnp.where(l4 >= 2, roll(q, 2), 0.0)
            acc = acc + q
        TB[dy + 1] = acc
    TC[0:2, :] = TB[1, 0:2, :] + TB[0, 2:4, :]
    TC[2:4, :] = TB[1, 2:4, :] + TB[2, 0:2, :]
    for i in range(4):
        v = roll(jnp.where(l4 == i, TC[...], 0.0), -i)
        v = v + roll(v, 1)
        v = v + roll(v, 2)
        G3[3 + i, 10:14, :] = v * inverse(W3[3 + i, 10:14, :])
    c, t = nsum(G3, 4, 2, 11, 2, 4)
    v3 = jnp.where(own1[0:2], S * (1.2 * c + S * t), 0.0)
    SE = r["SE"]
    SE[2:4, :] = pack3(v3)
    SE[1:2, :] = jnp.zeros((1, 128), F32)

    from_group(10, GC, nz - 1)
    GC[iz, 0] = SZ[0]
    GC[iz, 1] = SZ[1]
    acc = [zero] * 4
    for z in range(nz):
        v = GC[z, 0]
        if z + 1 < nz:
            v = v + jnp.where(lane % 8 >= 6, roll(GC[z + 1, 1], 6), 0.0)
        if z > 0:
            v = v + jnp.where(lane % 8 < 2, roll(GC[z - 1, 1], -2), 0.0)
        for x in range(nx):
            acc[x % 4] = acc[x % 4] + cp[x * nz + z] * v[x : x + 1, :]
    acc = (acc[0] + acc[1]) + (acc[2] + acc[3])
    tot = jnp.sum(acc, axis=1, keepdims=True)
    e4 = jnp.sum(jnp.where((lane >= 32 + 8 * row) & (lane < 40 + 8 * row), tot, 0.0), axis=0, keepdims=True)
    SE[0:1, :] = e4
    RE = r["RE"]
    run(send_all(SE, RE, 7))

    unpack3(RE, SE, slice(2, 4), V3)
    for x in (1, 8):
        V3[x, 8:16, :] = zero
    for x in range(2, 8):
        V3[x, 8:9, :] = zero[0:1]
        V3[x, 15:16, :] = zero[0:1]
    l1 = lane[0:1]
    par = []
    for dx in (-1, 0, 1):
        v = zero
        for dy in (-1, 0, 1):
            o = (dx, dy, 0)
            own = SE[0:1, :] if o == (0, 0, 0) else keep(RE[SLOT[o], 0:1, :], *o)
            lo, hi = (keep(RE[SLOT[(dx, dy, dz)], 0:1, :], dx, dy, dz) for dz in (-1, 1))
            e = jnp.where((l1 >= 32) & (l1 < 96), own, roll(jnp.where(l1 < 64, hi, lo), 64))
            y = 3 + 2 * dy
            v = jnp.where((row == y) | (row == y + 1), e, v)
        par.append(v)
    for i in range(6):
        U3[2 + i, 8:16, :] = V3[2 + i, 8:16, :] + W3[2 + i, 8:16, :] * par[i // 2]
    c, t = nsum(U3, 3, 4, 8, 8, 4)
    E3 = r["E3"]
    E3[...] = (0.2 * c + S * (G3[3:7, 8:16, :] + t)) * inverse(W3[3:7, 8:16, :])
    F2 = r["F2"]
    F2[:, pl.ds(0, 4, stride=2), :] = E3[:, 2:6, :]
    F2[:, pl.ds(1, 4, stride=2), :] = E3[:, 2:6, :]
    for i in range(8):
        U2[2 + i, 6:14, :] = V2[2 + i, 6:14, :] + W2[2 + i, 6:14, :] * F2[i // 2]
    c, t = nsum(U2, 3, 6, 6, 8, 2)
    E2 = r["E2"]
    E2[...] = (0.2 * c + S * (G2[3:9, 6:14, :] + t)) * inverse(W2[3:9, 6:14, :])
    F1 = r["F1"]
    F1[:, pl.ds(2, 6, stride=2), :] = E2[:, 1:7, :]
    F1[:, pl.ds(3, 6, stride=2), :] = E2[:, 1:7, :]
    for i in range(12):
        U1[1 + i, 6:18, :] = V1[1 + i, 6:18, :] + W1[1 + i, 6:18, :] * F1[i // 2, 2:14, :]
    E1 = r["E1"]
    for at in (7, 9):
        c, t = nsum(U1, 2, 10, at, 8, 1)
        E1[:, at - 7 : at + 1, :] = (0.2 * c + S * (G1[2:12, at : at + 8, :] + t)) * inverse(W1[2:12, at : at + 8, :])
    o = select_dot(E1[...].reshape(160, 128), up).reshape(10, 16, 128)
    F0 = r["F0"]
    O1 = r["O1"]
    O1[...] = o
    F0[:, pl.ds(6, 10, stride=2), :] = O1[:, 0:10, :]
    F0[:, pl.ds(7, 10, stride=2), :] = O1[:, 0:10, :]
    acc = zero
    for x in range(8):
        e = E1[x + 1, 1:9, :]
        for p in range(2):
            base = 6 * (2 * x + p + 2)
            acc = jnp.where(lane == base + 1, roll(e, base + 1 - 31), acc)
            acc = jnp.where(lane == base + 4, roll(e, base + 4 - 96), acc)
    UQ = r["UQ"]
    FQ = r["FQ"]
    FQ[...] = acc
    UQ[pl.ds(8, 8, stride=2), :] = FQ[...]
    UQ[pl.ds(9, 8, stride=2), :] = FQ[...]
    UQ[8:24, :] = VQ[8:24, :] + r["WQ"][8:24, :] * UQ[8:24, :]
    for i in range(18):
        V0[1 + i, 7:25, :] = V0[1 + i, 7:25, :] + W0[1 + i, 7:25, :] * F0[(i + 1) // 2, 7:25, :]
    inject(UQ, range(2, 18), (8, 16))
    for at in (8, 16):
        c, t = sum0(V0, 2, 16, at)
        out_ref[:, at - 8 : at, :] = 0.2 * c + S * (G0[2:18, at : at + 8, :] + t)

    def drain(o, src, key, slot):
        @pl.when(has(o))
        def _():
            copy(src, src, key, slot, right).wait_send()

    for item in sent:
        drain(*item)
    for key, src, n in ((8, SA, n_y - 1), (9, SB, xn - 1), (10, SZ, nz - 1)):
        for k in range(n):
            copy(src, src, key, k, right).wait_send()


def scratch(dims):
    nx, ny, nz = dims
    xn = ny // 2
    v = {
        "B0": (1, 16, 16, 128), "A0": (16, 16, 128), "CM": (8, nx * ny * nz * 8),
        "G0": (20, 32, 128), "W0": (20, 32, 128), "V0": (20, 32, 128), "INJ": (20, 32, 128),
        "GQ": (32, 128), "VQ": (32, 128), "WQ": (32, 128), "UQ": (32, 128),
        "YS": (2, 16, 2, 128), "RY": (2, 16, 2, 128), "RXY": (4, 2, 128),
        "QS": (16, 128), "QW": (16, 128), "RQ": (6, 16, 128), "QE": (2, 1, 128), "RQE": (4, 1, 128),
        "YW": (2, 16, 1, 128), "RYW": (2, 16, 1, 128), "RQW": (2, 16, 128),
        "C0": (8, 16, 128), "C1": (4, 8, 128), "C2": (4, 8, 128),
        "S1": (8, 8, 128), "SW": (8, 128), "RW": (26, 8, 128),
        "G1": (14, 24, 128), "W1": (14, 24, 128), "V1": (14, 24, 128), "U1": (14, 24, 128),
        "G2": (12, 24, 128), "W2": (12, 24, 128), "V2": (12, 24, 128), "U2": (12, 24, 128),
        "P2": (12, 24, 128), "Q2": (12, 24, 128),
        "G3": (10, 24, 128), "W3": (10, 24, 128), "V3": (10, 24, 128), "U3": (10, 24, 128), "P3": (10, 24, 128),
        "T4": (5, 24, 128), "SX": (2, 8, 128), "SY": (2, 8, 128), "RSX": (2, 8, 128), "RSY": (2, 8, 128),
        "SC": (8, 128), "RC": (26, 8, 128), "TB": (3, 4, 128), "TC": (4, 128), "SE": (4, 128), "RE": (26, 4, 128),
        "SA": (8, 128), "SB": (8, 128), "SZ": (2, 8, 128),
        "GA": (2 * nx, 8, 128), "GB": (xn, 8, 128), "GC": (nz, 2, 8, 128), "CP": (nx * nz, 8, 128),
        "E3": (4, 8, 128), "F2": (4, 8, 128), "E2": (6, 8, 128), "F1": (6, 16, 128),
        "E1": (10, 16, 128), "O1": (10, 16, 128), "F0": (10, 32, 128), "FQ": (8, 128),
    }
    for n in "wg":
        v["S1" + n] = (8, 8, 128)
        v["YS1" + n] = (2, 8, 4, 128)
        v["ZS1" + n] = (8, 128)
        v["RX1" + n] = (2, 3, 8, 128)
        v["RY1" + n] = (2, 8, 4, 128)
        v["RXY1" + n] = (4, 3, 4, 128)
        v["RZ1" + n] = (18, 8, 128)
    return v


def solution(mesh):
    dims = tuple(mesh.shape[a] for a in ("gx", "gy", "gz"))
    sizes = scratch(dims)

    def body(*args):
        names = ["b", "w", "c", "out"] + list(sizes) + ["ssem", "rsem", "lsem"]
        kernel(dims, dict(zip(names, args)))

    def per_device(sources, stiffness, coarse_inverse):
        vmem = pl.BlockSpec(memory_space=pltpu.VMEM)
        e = pl.pallas_call(
            body,
            out_shape=jax.ShapeDtypeStruct((16, 16, 128), F32),
            in_specs=[pl.BlockSpec(memory_space=pltpu.HBM)] * 3,
            out_specs=vmem,
            scratch_shapes=[pltpu.VMEM(s, F32) for s in sizes.values()] + [pltpu.SemaphoreType.DMA((11, 26))] * 2 + [pltpu.SemaphoreType.DMA((3,))],
            compiler_params=pltpu.CompilerParams(collective_id=0, has_side_effects=True, vmem_limit_bytes=24 * 2**20),
            name="vcycle",
        )(*[pltpu.with_memory_space_constraint(a, pltpu.HBM) for a in (sources, stiffness, coarse_inverse)])
        return (e / stiffness)[None]

    return jax.shard_map(
        per_device,
        mesh=mesh,
        in_specs=(P(None, "gx", "gy", "gz"), P("gx", "gy", "gz"), P(("gx", "gy", "gz"), None)),
        out_specs=P(None, "gx", "gy", "gz"),
        check_vma=False,
    )
```

```python
import functools
import itertools

import jax
import jax.numpy as jnp
from jax import lax
from jax.experimental import pallas as pl
from jax.experimental.pallas import tpu as pltpu
from jax.sharding import PartitionSpec as P

MESH = pl.DeviceIdType.MESH
F32 = jnp.float32
S = 0.8 / 6.0
OFFS = [o for o in itertools.product((-1, 0, 1), repeat=3) if o != (0, 0, 0)]
SLOT = {o: i for i, o in enumerate(OFFS)}
ZOFFS = [o for o in OFFS if o[2] != 0]
ZSLOT = {o: i for i, o in enumerate(ZOFFS)}
XY = [(-1, -1), (-1, 1), (1, -1), (1, 1)]
XZ = [(0, -1), (0, 1)] + XY


def neg(o):
    return tuple(-v for v in o)


def roll(v, shift):
    shift = shift % 128
    return v if shift == 0 else pltpu.roll(v, shift, v.ndim - 1)


def split2(v):
    hi = v.astype(jnp.bfloat16)
    lo = (v - hi.astype(F32)).astype(jnp.bfloat16)
    return jnp.concatenate([hi, lo], axis=1)


def select_dot(v, sel):
    return jnp.dot(split2(v), sel, preferred_element_type=F32)


def kernel(dims, refs):
    nx, ny, nz = dims
    xn = ny // 2
    n_y = nx * 2
    r = refs
    ix, iy, iz = lax.axis_index("gx"), lax.axis_index("gy"), lax.axis_index("gz")
    ih, ixx = iy // xn, iy % xn

    def dev(dx, dy, dz):
        return {
            "gx": lax.rem(ix + dx + nx, nx),
            "gy": lax.rem(iy + dy + ny, ny),
            "gz": lax.rem(iz + dz + nz, nz),
        }

    def copy(src, dst, key, device):
        return pltpu.make_async_remote_copy(
            src_ref=src,
            dst_ref=dst,
            send_sem=r["ssem"].at[key],
            recv_sem=r["rsem"].at[key],
            device_id=device,
            device_id_type=MESH,
        )

    cx = {-1: ix > 0, 1: ix < nx - 1}
    cy = {-1: iy > 0, 1: iy < ny - 1}
    cz = {-1: iz > 0, 1: iz < nz - 1}

    def has(o):
        c = [f[v] for f, v in zip((cx, cy, cz), o) if v]
        return functools.reduce(jnp.logical_and, c)

    def keep(v, *o):
        return jnp.where(has(o), v, 0.0) if any(o) else v

    sent = []

    def round_of(key, items, slots):
        for o, src, dst in items:

            @pl.when(has(o))
            def _():
                copy(src, dst, key, dev(*o)).start()

        offs = [o for o, _, _ in items]
        count = sum(jnp.where(has(o), 1, 0) for o in offs)
        sizes = set()
        for ends in itertools.product((((-1, 1), (-1,), (1,), ())), repeat=3):
            sizes.add(sum(all(v == 0 or v in e for v, e in zip(o, ends)) for o in offs))
        sizes = sorted(n for n in sizes if n)
        sent.append((key, slots, count, sizes))

        def wait():
            for n in sizes:

                @pl.when(count == n)
                def _():
                    copy(slots(n), slots(n), key, right).wait_recv()

        return wait

    def first(ref):
        return lambda n: ref.at[pl.ds(0, n)]

    def to_group(key, src, dst, group):
        for d in group:
            copy(src, dst, key, d).start()

    def from_group(key, buf, n):
        copy(buf.at[pl.ds(0, n)], buf.at[pl.ds(0, n)], key, right).wait_recv()

    def run(waits):
        for w in waits:
            w()

    me = {"gx": ix, "gy": iy, "gz": iz}
    right = {"gx": lax.rem(ix + 1, nx), "gy": iy, "gz": iz}

    group_y = []
    for k in range(1, n_y):
        t = lax.rem(ih * nx + ix + k, n_y)
        group_y.append({"gx": t % nx, "gy": (t // nx) * xn + ixx, "gz": iz})
    group_x = [{"gx": ix, "gy": ih * xn + lax.rem(ixx + k, xn), "gz": iz} for k in range(1, xn)]
    group_z = [{"gx": ix, "gy": iy, "gz": lax.rem(iz + k, nz)} for k in range(1, nz)]

    barrier = pltpu.get_barrier_semaphore()
    loads = [pltpu.make_async_copy(r[a], r[b], r["lsem"].at[i]) for i, (a, b) in enumerate((("b", "B0"), ("w", "A0"), ("c", "CM")))]
    for c in loads:
        c.start()
    for o in OFFS:

        @pl.when(has(o))
        def _():
            pl.semaphore_signal(barrier, inc=1, device_id=dev(*o), device_id_type=MESH)

    for d in group_y + group_x + group_z:
        pl.semaphore_signal(barrier, inc=1, device_id=d, device_id_type=MESH)
    partners = sum(jnp.where(has(o), 1, 0) for o in OFFS) + len(group_y + group_x + group_z)

    lane = lax.broadcasted_iota(jnp.int32, (8, 128), 1)
    row = lax.broadcasted_iota(jnp.int32, (8, 128), 0)
    zero = jnp.zeros((8, 128), F32)

    def flag(c):
        return jnp.where(c, jnp.float32(1), jnp.float32(0))

    mx = {-1: flag(ix > 0), 0: jnp.float32(1), 1: flag(ix < nx - 1)}
    my = {-1: flag(iy > 0), 0: jnp.float32(1), 1: flag(iy < ny - 1)}
    mz = {-1: flag(iz > 0), 0: jnp.float32(1), 1: flag(iz < nz - 1)}
    zmask = jnp.where(lane < 32, mz[-1], jnp.where(lane >= 96, mz[1], 1.0))

    b_ref, w_ref, c_ref, out_ref = r["B0"], r["A0"], r["CM"], r["out"]

    G0, W0, V0 = r["G0"], r["W0"], r["V0"]
    loads[0].wait()
    loads[1].wait()
    w0 = w_ref[...]
    g0 = b_ref[0] / w0
    W0[2:18, 8:24, :] = w0
    G0[2:18, 8:24, :] = g0

    r["YS"][0] = G0[2:18, 8:10, :]
    r["YS"][1] = G0[2:18, 22:24, :]

    def pack_q(src, dst):
        for h in range(2):
            acc = zero
            for x in range(16):
                m = src[x + 2, 8 + 8 * h : 16 + 8 * h, :]
                base = 6 * (x + 2)
                acc = jnp.where((lane >= base) & (lane < base + 3), roll(m, base - 126), acc)
                acc = jnp.where((lane >= base + 3) & (lane < base + 6), roll(m, base + 3 - 127), acc)
            dst[8 * h : 8 * h + 8, :] = acc

    pack_q(G0, r["QS"])
    r["QE"][0] = r["QS"][0:1, :]
    r["QE"][1] = r["QS"][15:16, :]

    pl.semaphore_wait(barrier, partners)

    gsl = pl.ds(8, 16)
    wait_g0 = [
        round_of(
            0,
            [
                ((-1, 0, 0), G0.at[pl.ds(2, 2), gsl], G0.at[pl.ds(18, 2), gsl]),
                ((1, 0, 0), G0.at[pl.ds(16, 2), gsl], G0.at[pl.ds(0, 2), gsl]),
            ],
            lambda n: G0.at[pl.ds(0, 2 * n), gsl],
        ),
        round_of(1, [((0, d, 0), r["YS"].at[i], r["RY"].at[1 - i]) for i, d in enumerate((-1, 1))], first(r["RY"])),
        round_of(
            2,
            [
                ((dx, dy, 0), r["YS"].at[(dy + 1) // 2, 0 if dx < 0 else 15], r["RXY"].at[XY.index((-dx, -dy))])
                for dx, dy in XY
            ],
            first(r["RXY"]),
        ),
        round_of(3, [((dx, 0, dz), r["QS"], r["RQ"].at[XZ.index((-dx, -dz))]) for dx, dz in XZ], first(r["RQ"])),
        round_of(
            4,
            [((0, dy, dz), r["QE"].at[(dy + 1) // 2], r["RQE"].at[XY.index((-dy, -dz))]) for dy, dz in XY],
            first(r["RQE"]),
        ),
    ]

    for name in ("G0", "W0", "V0"):
        a = r[name]
        a[:, 0:8, :] = jnp.zeros((20, 8, 128), F32)
        a[:, 24:32, :] = jnp.zeros((20, 8, 128), F32)
    for name in ("GQ", "WQ", "VQ", "UQ", "G1", "W1", "V1", "U1", "G2", "W2", "V2", "U2", "P2", "Q2", "G3", "W3", "V3", "U3", "P3", "T4"):
        r[name][...] = jnp.zeros(r[name].shape, F32)

    zr = lax.broadcasted_iota(jnp.int32, (256, 128), 0) % 128
    zc = lax.broadcasted_iota(jnp.int32, (256, 128), 1)
    down = jnp.where(zc == 32 + zr // 2, jnp.float32(1), jnp.float32(0)).astype(jnp.bfloat16)
    up = jnp.where(zr == 32 + zc // 2, jnp.float32(1), jnp.float32(0)).astype(jnp.bfloat16)

    C0 = r["C0"]

    def coarsen0(values, scale):
        C0[...] = jnp.sum(values.reshape(8, 2, 16, 128), axis=1)
        t = C0[:, pl.ds(0, 8, stride=2), :] + C0[:, pl.ds(1, 8, stride=2), :]
        return (select_dot(t.reshape(64, 128), down) * scale).reshape(8, 8, 128)

    def pair_z(t, dil):
        ln = lax.broadcasted_iota(jnp.int32, t.shape, t.ndim - 1)
        return t + jnp.where((ln // dil) % 2 == 0, roll(t, -dil), roll(t, dil))

    C1, C2 = r["C1"], r["C2"]

    def coarsen1(values, scale):
        n = values.shape[0] // 2
        C1[...] = jnp.sum(values.reshape(n, 2, 8, 128), axis=1)
        t = C1[:, pl.ds(0, 4, stride=2), :] + C1[:, pl.ds(1, 4, stride=2), :]
        return pair_z(t, 1) * scale

    S1 = r["S1"]
    w1 = coarsen0(w0, 0.0625)
    own1 = (lane >= 32) & (lane < 96)
    w2 = coarsen1(w1, 0.0625)
    C2[0:4, 0:4, :] = w2
    t = C2[0:4, pl.ds(0, 2, stride=2), :] + C2[0:4, pl.ds(1, 2, stride=2), :]
    w3 = pair_z(jnp.sum(t.reshape(2, 2, 2, 128), axis=1), 2) * 0.0625

    lane4 = lane[0:4]

    def pack2(v):
        halves = []
        for h in range(2):
            a = jnp.where(lane4 % 2 == 0, v[2 * h], v[2 * h + 1])
            halves.append(roll(a, -32 if h == 0 else 32))
        return jnp.where(lane4 < 64, halves[0], halves[1])

    def pack3(v):
        return jnp.where(lane[0:2] < 64, roll(v[0], -32), roll(v[1], 32))

    SW = r["SW"]
    SW[0:4, :] = pack2(w2)
    SW[4:6, :] = pack3(w3)
    SW[6:8, :] = jnp.zeros((2, 128), F32)

    def send_all(src, dst, key):
        return [round_of(key, [(o, src, dst.at[SLOT[neg(o)]]) for o in OFFS], first(dst))]

    wait_w = send_all(SW, r["RW"], 5)

    def send1(own, n, key):
        s1, ys, zs = r["S1" + n], r["YS1" + n], r["ZS1" + n]
        s1[...] = own
        ys[0] = s1[:, 0:4, :]
        ys[1] = s1[:, 4:8, :]
        acc = zero
        for x in range(8):
            acc = jnp.where((lane >= 16 * x) & (lane < 16 * x + 4), roll(own[x], 16 * x - 32), acc)
            acc = jnp.where((lane >= 16 * x + 4) & (lane < 16 * x + 8), roll(own[x], 16 * x + 4 - 92), acc)
        zs[...] = acc
        rx, ry, rxy, rz = (r[name + n] for name in ("RX1", "RY1", "RXY1", "RZ1"))
        zo = [o for o in ZOFFS if n == "g" or 0 in o]
        return [
            round_of(
                key,
                [((-1, 0, 0), s1.at[pl.ds(0, 3)], rx.at[1]), ((1, 0, 0), s1.at[pl.ds(5, 3)], rx.at[0])],
                first(rx),
            ),
            round_of(key + 1, [((0, -1, 0), ys.at[0], ry.at[1]), ((0, 1, 0), ys.at[1], ry.at[0])], first(ry)),
            round_of(
                key + 2,
                [
                    ((dx, dy, 0), ys.at[(dy + 1) // 2, pl.ds(0 if dx < 0 else 5, 3)], rxy.at[XY.index((-dx, -dy))])
                    for dx, dy in XY
                ],
                first(rxy),
            ),
            round_of(key + 3, [(o, zs, rz.at[ZSLOT[neg(o)]]) for o in zo], first(rz)),
        ]

    def recv1(own, n, key, dst):
        run(key)
        for x in range(14):
            dx = -1 if x < 3 else (1 if x > 10 else 0)
            for dy in (-1, 0, 1):
                if dx == 0 and dy == 0:
                    base = own[x - 3]
                elif dy == 0:
                    base = r["RX1" + n][(dx + 1) // 2, x if dx < 0 else x - 11]
                elif dx == 0:
                    base = r["RY1" + n][(dy + 1) // 2, x - 3]
                else:
                    base = r["RXY1" + n][XY.index((dx, dy)), x if dx < 0 else x - 11]
                sx = x - 3 if dx == 0 else (x + 5 if dx < 0 else x - 11)
                rows = slice(0, 8) if dy == 0 else (slice(4, 8) if dy < 0 else slice(0, 4))
                lo = r["RZ1" + n][ZSLOT[(dx, dy, -1)], rows, :]
                hi = r["RZ1" + n][ZSLOT[(dx, dy, 1)], rows, :]
                ln = lane[0:8] if dy == 0 else lane4
                v = keep(base, dx, dy, 0)
                if n == "g" or dx == 0 or dy == 0:
                    v = jnp.where((ln >= 28) & (ln < 32), keep(roll(lo, 28 - 16 * sx - 4), dx, dy, -1), v)
                    v = jnp.where((ln >= 96) & (ln < 100), keep(roll(hi, 96 - 16 * sx), dx, dy, 1), v)
                at = 8 if dy == 0 else (4 if dy < 0 else 16)
                dst[x, at : at + (8 if dy == 0 else 4), :] = v

    wait_w1 = send1(w1, "w", 6)

    r["YW"][0] = W0[2:18, 8:9, :]
    r["YW"][1] = W0[2:18, 23:24, :]
    pack_q(W0, r["QW"])
    wait_w0 = [
        round_of(
            14,
            [
                ((-1, 0, 0), W0.at[pl.ds(2, 1), gsl], W0.at[pl.ds(18, 1), gsl]),
                ((1, 0, 0), W0.at[pl.ds(17, 1), gsl], W0.at[pl.ds(1, 1), gsl]),
            ],
            lambda n: W0.at[pl.ds(0, n), gsl],
        ),
        round_of(15, [((0, d, 0), r["YW"].at[i], r["RYW"].at[1 - i]) for i, d in enumerate((-1, 1))], first(r["RYW"])),
        round_of(16, [((0, 0, d), r["QW"], r["RQW"].at[1 - i]) for i, d in enumerate((-1, 1))], first(r["RQW"])),
    ]

    wi1 = 1.0 / jnp.where(own1, w1, 1.0)
    wi2 = 1.0 / jnp.where(own1[0:4], w2, 1.0)

    GQ, VQ = r["GQ"], r["VQ"]
    run(wait_g0)
    G0[0:2, 8:24, :] = keep(G0[0:2, 8:24, :], -1, 0, 0)
    G0[18:20, 8:24, :] = keep(G0[18:20, 8:24, :], 1, 0, 0)
    G0[2:18, 6:8, :] = keep(r["RY"][0], 0, -1, 0)
    G0[2:18, 24:26, :] = keep(r["RY"][1], 0, 1, 0)
    for dx, dy in XY:
        v = keep(r["RXY"][XY.index((dx, dy))], dx, dy, 0)
        G0[1 if dx < 0 else 18, 7 if dy < 0 else 24, :] = v[1 if dy < 0 else 0, :]

    def qj(ln):
        return ln % 6

    for h in range(2):
        sl = slice(8 * h, 8 * h + 8)
        own = r["QS"][sl, :]
        j = qj(lane)
        q = [keep(r["RQ"][i, sl, :], dx, 0, dz) for i, (dx, dz) in enumerate(XZ)]
        v, lo, hi = (jnp.where(j < 2, q[2 * i], jnp.where(j > 3, q[2 * i + 1], own if i == 0 else 0.0)) for i in range(3))
        v = jnp.where((lane >= 6) & (lane < 12), roll(lo, 6 - 102), jnp.where((lane >= 108) & (lane < 114), roll(hi, 108 - 12), v))
        GQ[8 + 8 * h : 16 + 8 * h, :] = jnp.where((lane >= 6) & (lane < 114), v, 0.0)
    for dy, at in ((-1, 7), (1, 24)):
        j = qj(lane[0:1])
        lo = keep(r["RQE"][XY.index((dy, -1))], 0, dy, -1)
        hi = keep(r["RQE"][XY.index((dy, 1))], 0, dy, 1)
        v = jnp.where(j < 2, lo, jnp.where(j > 3, hi, 0.0))
        GQ[at : at + 1, :] = jnp.where((lane[0:1] >= 12) & (lane[0:1] < 108), v, 0.0)

    INJ = r["INJ"]

    def inject(q, xs, tiles):
        for at in tiles:
            m = q[at : at + 8, :]
            for xp in xs:
                a = roll(m, -(6 * xp + 1))
                c = roll(m, 127 - (6 * xp + 4))
                INJ[xp, at : at + 8, :] = jnp.where(lane == 0, a, jnp.where(lane == 127, c, 0.0))

    def sum0(a, x, n, at):
        c = a[x : x + n, at : at + 8, :]
        t = a[x - 1 : x + n - 1, at : at + 8, :] + a[x + 1 : x + n + 1, at : at + 8, :]
        t = t + (a[x : x + n, at - 1 : at + 7, :] + a[x : x + n, at + 1 : at + 9, :])
        z = jnp.where(lane == 0, 0.0, roll(c, 1)) + jnp.where(lane == 127, 0.0, roll(c, -1))
        return c, t + (z + INJ[x : x + n, at : at + 8, :])

    inject(GQ, range(1, 19), (7, 15, 17))
    for at in (7, 15, 17):
        c, t = sum0(G0, 1, 18, at)
        v = S * (1.2 * c + S * t)
        if at == 7:
            v = v * jnp.where(row == 0, my[-1], 1.0)
        if at == 17:
            v = v * jnp.where(row == 7, my[1], 1.0)
        V0[1:19, at : at + 8, :] = v
    V0[1:2, 7:25, :] = V0[1:2, 7:25, :] * mx[-1]
    V0[18:19, 7:25, :] = V0[18:19, 7:25, :] * mx[1]

    for at in (8, 16):
        c = GQ[at : at + 8, :]
        t = roll(c, 1) + roll(c, -1) + roll(c, 6) + roll(c, -6)
        t = t + GQ[at - 1 : at + 7, :] + GQ[at + 1 : at + 9, :]
        j = qj(lane)
        mask = jnp.where(j == 1, mz[-1], jnp.where(j == 4, mz[1], 0.0))
        mask = jnp.where((lane >= 12) & (lane < 108), mask, 0.0)
        VQ[at : at + 8, :] = S * (1.2 * c + S * t) * mask

    inject(VQ, range(2, 18), (8, 16))
    halves = []
    for at in (8, 16):
        c, t = sum0(V0, 2, 16, at)
        halves.append(W0[2:18, at : at + 8, :] * (G0[2:18, at : at + 8, :] - 6.0 * c + t))
    r0 = jnp.concatenate(halves, axis=1)
    g1 = jnp.where(own1, coarsen0(r0, 0.125) * wi1, 0.0)
    wait_g1 = send1(g1, "g", 10)

    G1, W1, V1, U1 = r["G1"], r["W1"], r["V1"], r["U1"]
    G2, W2, V2, U2, P2, Q2 = r["G2"], r["W2"], r["V2"], r["U2"], r["P2"], r["Q2"]
    G3, W3, V3, U3, P3 = r["G3"], r["W3"], r["V3"], r["U3"], r["P3"]
    run(wait_w)

    def spread(m0, lo, hi, l, dx, dy):
        return keep(m0, dx, dy, 0), jnp.where((l // 32) % 2 == 1, keep(lo, dx, dy, -1), keep(hi, dx, dy, 1))

    def place(m0, c, l, h):
        a = roll(m0, 32 if h == 0 else 96)
        e = roll(c, 96 if h == 0 else 32)
        return jnp.where((l >= 32) & (l < 96), a, e)

    def piece(buf, own, rows, o):
        return own[rows, :] if o == (0, 0, 0) else buf[SLOT[o], rows, :]

    def unpack2(buf, own, dst):
        rows = slice(0, 4)
        for dx in (-1, 0, 1):
            for dy in (-1, 0, 1):
                m0, c = spread(*[piece(buf, own, rows, (dx, dy, dz)) for dz in (0, -1, 1)], lane4, dx, dy)
                for p in range(2):
                    take = lane4 % 2 == p
                    a = jnp.where(take, m0, roll(m0, 1 if p == 0 else -1))
                    e = jnp.where(take, c, roll(c, 1 if p == 0 else -1))
                    for h in range(2):
                        dst[4 + 4 * dx + 2 * h + p, 8 + 4 * dy : 12 + 4 * dy, :] = place(a, e, lane4, h)

    def unpack3(buf, own, rows, dst):
        l = lane[0:2]
        for dx in (-1, 0, 1):
            for dy in (-1, 0, 1):
                m0, c = spread(*[piece(buf, own, rows, (dx, dy, dz)) for dz in (0, -1, 1)], l, dx, dy)
                for h in range(2):
                    dst[4 + 2 * dx + h, 11 + 2 * dy : 13 + 2 * dy, :] = place(m0, c, l, h)

    unpack2(r["RW"], SW, W2)
    unpack3(r["RW"], SW, slice(4, 6), W3)
    r["SX"][0] = W3[6, 8:16, :]
    r["SX"][1] = W3[3, 8:16, :]
    for i in range(8):
        r["SY"][0, i : i + 1, :] = W3[i + 1, 13:14, :]
        r["SY"][1, i : i + 1, :] = W3[i + 1, 10:11, :]
    wait_s = [
        round_of(17, [((d, 0, 0), r["SX"].at[i], r["RSX"].at[1 - i]) for i, d in enumerate((-1, 1))], first(r["RSX"])),
        round_of(18, [((0, d, 0), r["SY"].at[i], r["RSY"].at[1 - i]) for i, d in enumerate((-1, 1))], first(r["RSY"])),
    ]

    recv1(w1, "w", wait_w1, W1)
    run(wait_w0)
    W0[1:2, 8:24, :] = keep(W0[1:2, 8:24, :], -1, 0, 0)
    W0[18:19, 8:24, :] = keep(W0[18:19, 8:24, :], 1, 0, 0)
    W0[2:18, 7:8, :] = keep(r["RYW"][0], 0, -1, 0)
    W0[2:18, 24:25, :] = keep(r["RYW"][1], 0, 1, 0)
    for h in range(2):
        sl = slice(8 * h, 8 * h + 8)
        j = qj(lane)
        v = jnp.where(j == 1, keep(r["RQW"][0, sl, :], 0, 0, -1), jnp.where(j == 4, keep(r["RQW"][1, sl, :], 0, 0, 1), 0.0))
        r["WQ"][8 + 8 * h : 16 + 8 * h, :] = v

    def inverse(w):
        return jnp.where(w > 0.0, 1.0 / jnp.where(w > 0.0, w, 1.0), 0.0)

    recv1(g1, "g", wait_g1, G1)

    def nsum(a, x, n, at, rows, dil):
        c = a[x : x + n, at : at + rows, :]
        t = a[x - 1 : x + n - 1, at : at + rows, :] + a[x + 1 : x + n + 1, at : at + rows, :]
        t = t + (a[x : x + n, at - 1 : at + rows - 1, :] + a[x : x + n, at + 1 : at + rows + 1, :])
        return c, t + (roll(c, dil) + roll(c, -dil))

    def rowmask(at, rows, low, high):
        y = lax.broadcasted_iota(jnp.int32, (rows, 128), 0) + at
        l = lax.broadcasted_iota(jnp.int32, (rows, 128), 1)
        m = jnp.where(y < low, my[-1], jnp.where(y >= high, my[1], 1.0))
        return m * jnp.where(l < 32, mz[-1], jnp.where(l >= 96, mz[1], 1.0))

    def xmask(a, low, high, x, n, at, rows):
        if low > x:
            a[x:low, at : at + rows, :] = a[x:low, at : at + rows, :] * mx[-1]
        if x + n > high:
            a[high : x + n, at : at + rows, :] = a[high : x + n, at : at + rows, :] * mx[1]

    for at in (4, 12):
        c, t = nsum(G1, 1, 12, at, 8, 1)
        V1[1:13, at : at + 8, :] = S * (1.2 * c + S * t) * rowmask(at, 8, 8, 16)
    xmask(V1, 3, 11, 1, 12, 4, 16)
    c, t = nsum(V1, 3, 8, 8, 8, 1)
    r1 = W1[3:11, 8:16, :] * (G1[3:11, 8:16, :] - 6.0 * c + t)
    g2 = jnp.where(own1[0:4], coarsen1(r1, 0.125) * wi2, 0.0)

    P2[4:8, 8:12, :] = g2
    c, t = nsum(P2, 2, 8, 6, 8, 2)
    Q2[2:10, 6:14, :] = S * (1.2 * c + S * t) * rowmask(6, 8, 8, 12)
    xmask(Q2, 4, 8, 2, 8, 6, 8)
    c, t = nsum(Q2, 2, 8, 6, 8, 2)
    res = W2[2:10, 6:14, :] * (P2[2:10, 6:14, :] - 6.0 * c + t)
    C2[...] = jnp.sum(res.reshape(4, 2, 8, 128), axis=1)
    t = C2[:, pl.ds(0, 4, stride=2), :] + C2[:, pl.ds(1, 4, stride=2), :]
    b3 = pair_z(t, 2) * 0.125
    SC = r["SC"]
    SC[0:4, :] = pack2(g2)
    l4 = lane4 % 4
    SC[4:8, :] = jnp.where(l4 < 2, jnp.where(l4 == 0, b3[0], b3[1]), jnp.where(l4 == 2, b3[2], b3[3]))
    wait_c = send_all(SC, r["RC"], 19)
    run(wait_s)
    W3[1, 8:16, :] = keep(r["RSX"][0], -1, 0, 0)
    W3[8, 8:16, :] = keep(r["RSX"][1], 1, 0, 0)
    for i in range(1, 7):
        W3[i + 1, 8:9, :] = keep(r["RSY"][0, i : i + 1, :], 0, -1, 0)
        W3[i + 1, 15:16, :] = keep(r["RSY"][1, i : i + 1, :], 0, 1, 0)
    P3[3:7, 10:14, :] = b3 * inverse(W3[3:7, 10:14, :])
    c, t = nsum(P3, 1, 8, 8, 8, 4)
    V3[1:9, 8:16, :] = S * (1.2 * c + S * t) * rowmask(8, 8, 11, 13)
    xmask(V3, 4, 6, 1, 8, 8, 8)
    c, t = nsum(V3, 1, 8, 8, 8, 4)
    res = W3[1:9, 8:16, :] * (P3[1:9, 8:16, :] - 6.0 * c + t)
    T4 = r["T4"]
    T4[0, 8:16, :] = res[0]
    for i in range(3):
        T4[1 + i, 8:16, :] = res[1 + 2 * i] + res[2 + 2 * i]
    T4[4, 8:16, :] = res[7]
    t = T4[:, pl.ds(7, 8, stride=2), :] + T4[:, pl.ds(8, 8, stride=2), :]
    patch = pair_z(t, 4) * 0.125

    msg = zero
    for dx in range(5):
        v = patch[dx]
        main = zero
        for q in range(4):
            lo = 32 + 16 * q + 7
            main = jnp.where((lane >= 2 * q) & (lane < 2 * q + 2), roll(v, 2 * q - lo), main)
        edge = jnp.where(lane < 2, roll(v, 0 - 23), jnp.where(lane < 4, roll(v, 2 - 103), 0.0))
        line = pltpu.roll(main, 0, 1, stride=8, stride_axis=0) + pltpu.roll(edge, 40, 1, stride=4, stride_axis=0)
        line = jnp.sum(line, axis=0, keepdims=True)
        msg = jnp.where(row == ix + (dx - 2), line, msg)
    msg = jnp.where(ih == 1, roll(msg, 64), msg)
    GA, GB, GC = r["GA"], r["GB"], r["GC"]
    SA, SB, SZ = r["SA"], r["SB"], r["SZ"]
    SA[...] = msg
    ga_at = ih * nx + ix
    to_group(21, SA, GA.at[ga_at], group_y)

    cp = r["CP"]
    loads[2].wait()

    @pl.loop(0, nx)
    def _(x):
        for z in range(nz):
            acc = zero
            for p in range(ny // 2):
                tile = c_ref[:, pl.ds(pl.multiple_of((x * (ny // 2) + p) * 128, 128), 128)]
                for q in range(2):
                    y = 2 * p + q
                    at = 8 * y
                    acc = jnp.where((lane >= at) & (lane < at + 8), roll(tile, at - 64 * q - 8 * z), acc)
            cp[x * nz + z] = acc

    from_group(21, GA, n_y - 1)
    GA[ga_at] = msg
    SB[...] = jnp.sum(GA[...], axis=0)
    to_group(22, SB, GB.at[ixx], group_x)

    from_group(22, GB, xn - 1)
    GB[ixx] = SB[...]
    main = zero
    edges = [zero] * 5
    for k in range(xn):
        v = GB[k]
        for h in range(2):
            if xn == 8 and h == 1:
                continue
            shift = 8 * k - 16 + h * (8 * xn - 64)
            m = roll(v, shift)
            src = (lane - shift + 256) % 128
            if xn != 8:
                m = jnp.where(src // 64 == h, m, 0.0)
            main = main + jnp.where(src % 64 < 40, m, 0.0)
            for dy in range(5):
                a = 40 + 4 * dy
                edges[dy] = edges[dy] + jnp.where((src % 64 >= a) & (src % 64 < a + 4), m, 0.0)
    edge = zero
    for dy in range(5):
        edge = edge + roll(edges[dy], 4 * dy - 40)
    SZ[0] = main
    SZ[1] = edge
    to_group(23, SZ, GC.at[iz], group_z)

    run(wait_c)
    unpack2(r["RC"], SC, G2)
    c, t = nsum(G2, 2, 8, 6, 8, 2)
    V2[2:10, 6:14, :] = S * (1.2 * c + S * t) * rowmask(6, 8, 8, 12)
    xmask(V2, 4, 8, 2, 8, 6, 8)

    TB, TC, RC = r["TB"], r["TC"], r["RC"]
    for dy in (-1, 0, 1):
        acc = jnp.zeros((4, 128), F32)
        for dx in (-1, 0, 1):
            m0, lo, hi = (keep(piece(RC, SC, slice(4, 8), (dx, dy, dz)), dx, dy, dz) for dz in (0, -1, 1))
            e = jnp.where((lane4 >= 92) & (lane4 < 100), lo, jnp.where((lane4 >= 28) & (lane4 < 36), hi, 0.0))
            q = m0 + roll(e, 64)
            if dx < 0:
                q = jnp.where(l4 < 2, roll(q, -2), 0.0)
            if dx > 0:
                q = jnp.where(l4 >= 2, roll(q, 2), 0.0)
            acc = acc + q
        TB[dy + 1] = acc
    TC[0:2, :] = TB[1, 0:2, :] + TB[0, 2:4, :]
    TC[2:4, :] = TB[1, 2:4, :] + TB[2, 0:2, :]
    for i in range(4):
        v = roll(jnp.where(l4 == i, TC[...], 0.0), -i)
        v = v + roll(v, 1)
        v = v + roll(v, 2)
        G3[3 + i, 10:14, :] = v * inverse(W3[3 + i, 10:14, :])
    c, t = nsum(G3, 4, 2, 11, 2, 4)
    v3 = jnp.where(own1[0:2], S * (1.2 * c + S * t), 0.0)
    SE = r["SE"]
    SE[2:4, :] = pack3(v3)
    SE[1:2, :] = jnp.zeros((1, 128), F32)

    from_group(23, GC, nz - 1)
    GC[iz, 0] = SZ[0]
    GC[iz, 1] = SZ[1]
    acc = [zero] * 4
    for z in range(nz):
        v = GC[z, 0]
        if z + 1 < nz:
            v = v + jnp.where(lane % 8 >= 6, roll(GC[z + 1, 1], 6), 0.0)
        if z > 0:
            v = v + jnp.where(lane % 8 < 2, roll(GC[z - 1, 1], -2), 0.0)
        for x in range(nx):
            acc[x % 4] = acc[x % 4] + cp[x * nz + z] * v[x : x + 1, :]
    acc = (acc[0] + acc[1]) + (acc[2] + acc[3])
    tot = jnp.sum(acc, axis=1, keepdims=True)
    e4 = jnp.sum(jnp.where((lane >= 32 + 8 * row) & (lane < 40 + 8 * row), tot, 0.0), axis=0, keepdims=True)
    SE[0:1, :] = e4
    RE = r["RE"]
    run(send_all(SE, RE, 20))

    unpack3(RE, SE, slice(2, 4), V3)
    for x in (1, 8):
        V3[x, 8:16, :] = zero
    for x in range(2, 8):
        V3[x, 8:9, :] = zero[0:1]
        V3[x, 15:16, :] = zero[0:1]
    l1 = lane[0:1]
    par = []
    for dx in (-1, 0, 1):
        v = zero
        for dy in (-1, 0, 1):
            o = (dx, dy, 0)
            own = SE[0:1, :] if o == (0, 0, 0) else keep(RE[SLOT[o], 0:1, :], *o)
            lo, hi = (keep(RE[SLOT[(dx, dy, dz)], 0:1, :], dx, dy, dz) for dz in (-1, 1))
            e = jnp.where((l1 >= 32) & (l1 < 96), own, roll(jnp.where(l1 < 64, hi, lo), 64))
            y = 3 + 2 * dy
            v = jnp.where((row == y) | (row == y + 1), e, v)
        par.append(v)
    for i in range(6):
        U3[2 + i, 8:16, :] = V3[2 + i, 8:16, :] + W3[2 + i, 8:16, :] * par[i // 2]
    c, t = nsum(U3, 3, 4, 8, 8, 4)
    E3 = r["E3"]
    E3[...] = (0.2 * c + S * (G3[3:7, 8:16, :] + t)) * inverse(W3[3:7, 8:16, :])
    F2 = r["F2"]
    F2[:, pl.ds(0, 4, stride=2), :] = E3[:, 2:6, :]
    F2[:, pl.ds(1, 4, stride=2), :] = E3[:, 2:6, :]
    for i in range(8):
        U2[2 + i, 6:14, :] = V2[2 + i, 6:14, :] + W2[2 + i, 6:14, :] * F2[i // 2]
    c, t = nsum(U2, 3, 6, 6, 8, 2)
    E2 = r["E2"]
    E2[...] = (0.2 * c + S * (G2[3:9, 6:14, :] + t)) * inverse(W2[3:9, 6:14, :])
    F1 = r["F1"]
    F1[:, pl.ds(2, 6, stride=2), :] = E2[:, 1:7, :]
    F1[:, pl.ds(3, 6, stride=2), :] = E2[:, 1:7, :]
    for i in range(12):
        U1[1 + i, 6:18, :] = V1[1 + i, 6:18, :] + W1[1 + i, 6:18, :] * F1[i // 2, 2:14, :]
    E1 = r["E1"]
    for at in (7, 9):
        c, t = nsum(U1, 2, 10, at, 8, 1)
        E1[:, at - 7 : at + 1, :] = (0.2 * c + S * (G1[2:12, at : at + 8, :] + t)) * inverse(W1[2:12, at : at + 8, :])
    o = select_dot(E1[...].reshape(160, 128), up).reshape(10, 16, 128)
    F0 = r["F0"]
    O1 = r["O1"]
    O1[...] = o
    F0[:, pl.ds(6, 10, stride=2), :] = O1[:, 0:10, :]
    F0[:, pl.ds(7, 10, stride=2), :] = O1[:, 0:10, :]
    acc = zero
    for x in range(8):
        e = E1[x + 1, 1:9, :]
        for p in range(2):
            base = 6 * (2 * x + p + 2)
            acc = jnp.where(lane == base + 1, roll(e, base + 1 - 31), acc)
            acc = jnp.where(lane == base + 4, roll(e, base + 4 - 96), acc)
    UQ = r["UQ"]
    FQ = r["FQ"]
    FQ[...] = acc
    UQ[pl.ds(8, 8, stride=2), :] = FQ[...]
    UQ[pl.ds(9, 8, stride=2), :] = FQ[...]
    UQ[8:24, :] = VQ[8:24, :] + r["WQ"][8:24, :] * UQ[8:24, :]
    for i in range(18):
        V0[1 + i, 7:25, :] = V0[1 + i, 7:25, :] + W0[1 + i, 7:25, :] * F0[(i + 1) // 2, 7:25, :]
    inject(UQ, range(2, 18), (8, 16))
    for at in (8, 16):
        c, t = sum0(V0, 2, 16, at)
        out_ref[:, at - 8 : at, :] = 0.2 * c + S * (G0[2:18, at : at + 8, :] + t)

    def drain(key, slots, count, sizes):
        for n in sizes:

            @pl.when(count == n)
            def _():
                copy(slots(n), slots(n), key, right).wait_send()

    for item in sent:
        drain(*item)
    for key, buf, n in ((21, GA, n_y - 1), (22, GB, xn - 1), (23, GC, nz - 1)):
        copy(buf.at[pl.ds(0, n)], buf.at[pl.ds(0, n)], key, right).wait_send()


def scratch(dims):
    nx, ny, nz = dims
    xn = ny // 2
    v = {
        "B0": (1, 16, 16, 128), "A0": (16, 16, 128), "CM": (8, nx * ny * nz * 8),
        "G0": (20, 32, 128), "W0": (20, 32, 128), "V0": (20, 32, 128), "INJ": (20, 32, 128),
        "GQ": (32, 128), "VQ": (32, 128), "WQ": (32, 128), "UQ": (32, 128),
        "YS": (2, 16, 2, 128), "RY": (2, 16, 2, 128), "RXY": (4, 2, 128),
        "QS": (16, 128), "QW": (16, 128), "RQ": (6, 16, 128), "QE": (2, 1, 128), "RQE": (4, 1, 128),
        "YW": (2, 16, 1, 128), "RYW": (2, 16, 1, 128), "RQW": (2, 16, 128),
        "C0": (8, 16, 128), "C1": (4, 8, 128), "C2": (4, 8, 128),
        "S1": (8, 8, 128), "SW": (8, 128), "RW": (26, 8, 128),
        "G1": (14, 24, 128), "W1": (14, 24, 128), "V1": (14, 24, 128), "U1": (14, 24, 128),
        "G2": (12, 24, 128), "W2": (12, 24, 128), "V2": (12, 24, 128), "U2": (12, 24, 128),
        "P2": (12, 24, 128), "Q2": (12, 24, 128),
        "G3": (10, 24, 128), "W3": (10, 24, 128), "V3": (10, 24, 128), "U3": (10, 24, 128), "P3": (10, 24, 128),
        "T4": (5, 24, 128), "SX": (2, 8, 128), "SY": (2, 8, 128), "RSX": (2, 8, 128), "RSY": (2, 8, 128),
        "SC": (8, 128), "RC": (26, 8, 128), "TB": (3, 4, 128), "TC": (4, 128), "SE": (4, 128), "RE": (26, 4, 128),
        "SA": (8, 128), "SB": (8, 128), "SZ": (2, 8, 128),
        "GA": (2 * nx, 8, 128), "GB": (xn, 8, 128), "GC": (nz, 2, 8, 128), "CP": (nx * nz, 8, 128),
        "E3": (4, 8, 128), "F2": (4, 8, 128), "E2": (6, 8, 128), "F1": (6, 16, 128),
        "E1": (10, 16, 128), "O1": (10, 16, 128), "F0": (10, 32, 128), "FQ": (8, 128),
    }
    for n in "wg":
        v["S1" + n] = (8, 8, 128)
        v["YS1" + n] = (2, 8, 4, 128)
        v["ZS1" + n] = (8, 128)
        v["RX1" + n] = (2, 3, 8, 128)
        v["RY1" + n] = (2, 8, 4, 128)
        v["RXY1" + n] = (4, 3, 4, 128)
        v["RZ1" + n] = (18, 8, 128)
    return v


def solution(mesh):
    dims = tuple(mesh.shape[a] for a in ("gx", "gy", "gz"))
    sizes = scratch(dims)

    def body(*args):
        names = ["b", "w", "c", "out"] + list(sizes) + ["ssem", "rsem", "lsem"]
        kernel(dims, dict(zip(names, args)))

    def per_device(sources, stiffness, coarse_inverse):
        vmem = pl.BlockSpec(memory_space=pltpu.VMEM)
        e = pl.pallas_call(
            body,
            out_shape=jax.ShapeDtypeStruct((16, 16, 128), F32),
            in_specs=[pl.BlockSpec(memory_space=pltpu.HBM)] * 3,
            out_specs=vmem,
            scratch_shapes=[pltpu.VMEM(s, F32) for s in sizes.values()] + [pltpu.SemaphoreType.DMA((24,))] * 2 + [pltpu.SemaphoreType.DMA((3,))],
            compiler_params=pltpu.CompilerParams(collective_id=0, has_side_effects=True, vmem_limit_bytes=24 * 2**20),
            name="vcycle",
        )(*[pltpu.with_memory_space_constraint(a, pltpu.HBM) for a in (sources, stiffness, coarse_inverse)])
        return (e / stiffness)[None]

    return jax.shard_map(
        per_device,
        mesh=mesh,
        in_specs=(P(None, "gx", "gy", "gz"), P("gx", "gy", "gz"), P(("gx", "gy", "gz"), None)),
        out_specs=P(None, "gx", "gy", "gz"),
        check_vma=False,
    )
```

```python
import functools
import itertools

import jax
import jax.numpy as jnp
from jax import lax
from jax.experimental import pallas as pl
from jax.experimental.pallas import tpu as pltpu
from jax.sharding import PartitionSpec as P

MESH = pl.DeviceIdType.MESH
F32 = jnp.float32
S = 0.8 / 6.0
OFFS = [o for o in itertools.product((-1, 0, 1), repeat=3) if o != (0, 0, 0)]
OFFS.sort(key=lambda o: (-abs(o[1]), -abs(o[2]), -abs(o[0])))
OFF2X = [(2 * a, b, c) for a in (-1, 1) for b in (-1, 0, 1) for c in (-1, 0, 1)]
OFF2Y = [(b, 2 * a, c) for a in (-1, 1) for b in (-1, 0, 1) for c in (-1, 0, 1)]
FLAT = [o for o in OFFS if o[2] == 0]
SLOT = {o: i for i, o in enumerate(OFFS)}
ZOFFS = [o for o in OFFS if o[2] != 0]
ZSLOT = {o: i for i, o in enumerate(ZOFFS)}
XY = [(-1, -1), (-1, 1), (1, -1), (1, 1)]
XZ = [(0, -1), (0, 1)] + XY


def neg(o):
    return tuple(-v for v in o)


def roll(v, shift):
    shift = shift % 128
    return v if shift == 0 else pltpu.roll(v, shift, v.ndim - 1)


def split2(v):
    hi = v.astype(jnp.bfloat16)
    lo = (v - hi.astype(F32)).astype(jnp.bfloat16)
    return jnp.concatenate([hi, lo], axis=1)


def select_dot(v, sel):
    return jnp.dot(split2(v), sel, preferred_element_type=F32)


def kernel(dims, refs):
    nx, ny, nz = dims
    xn = ny // 2
    n_y = nx * 2
    r = refs
    ix, iy, iz = lax.axis_index("gx"), lax.axis_index("gy"), lax.axis_index("gz")
    ih, ixx = iy // xn, iy % xn

    def dev(dx, dy, dz):
        return {
            "gx": lax.rem(ix + dx + nx, nx),
            "gy": lax.rem(iy + dy + ny, ny),
            "gz": lax.rem(iz + dz + nz, nz),
        }

    def copy(src, dst, key, device):
        return pltpu.make_async_remote_copy(
            src_ref=src,
            dst_ref=dst,
            send_sem=r["ssem"].at[key],
            recv_sem=r["rsem"].at[key],
            device_id=device,
            device_id_type=MESH,
        )

    cx = {-2: ix > 1, -1: ix > 0, 1: ix < nx - 1, 2: ix < nx - 2}
    cy = {-2: iy > 1, -1: iy > 0, 1: iy < ny - 1, 2: iy < ny - 2}
    cz = {-1: iz > 0, 1: iz < nz - 1}

    def has(o):
        c = [f[v] for f, v in zip((cx, cy, cz), o) if v]
        return functools.reduce(jnp.logical_and, c)

    def keep(v, *o):
        return jnp.where(has(o), v, 0.0) if any(o) else v

    sent = []

    def round_of(key, items, slots):
        for o, src, dst in items:

            @pl.when(has(o))
            def _():
                copy(src, dst, key, dev(*o)).start()

        offs = [o for o, _, _ in items]
        count = sum(jnp.where(has(o), 1, 0) for o in offs)
        spots = [sorted({0, 1, 2, n - 3, n - 2, n - 1} & set(range(n))) for n in dims]
        sizes = {sum(all(0 <= v + p < n for v, p, n in zip(o, at, dims)) for o in offs) for at in itertools.product(*spots)}
        sizes = sorted(n for n in sizes if n)
        sent.append((key, slots, count, sizes))

        def wait():
            for n in sizes:

                @pl.when(count == n)
                def _():
                    copy(slots(n), slots(n), key, right).wait_recv()

        return wait

    def first(ref):
        return lambda n: ref.at[pl.ds(0, n)]

    def to_group(key, src, dst, group):
        for d in group:
            copy(src, dst, key, d).start()

    def from_group(key, buf, n):
        copy(buf.at[pl.ds(0, n)], buf.at[pl.ds(0, n)], key, right).wait_recv()

    def run(waits):
        for w in waits:
            w()

    me = {"gx": ix, "gy": iy, "gz": iz}
    right = {"gx": lax.rem(ix + 1, nx), "gy": iy, "gz": iz}

    group_y = []
    for k in range(1, n_y):
        t = lax.rem(ih * nx + ix + k, n_y)
        group_y.append({"gx": t % nx, "gy": (t // nx) * xn + ixx, "gz": iz})
    group_x = [{"gx": ix, "gy": ih * xn + lax.rem(ixx + k, xn), "gz": iz} for k in range(1, xn)]
    group_z = [{"gx": ix, "gy": iy, "gz": lax.rem(iz + k, nz)} for k in range(1, nz)]

    barrier = pltpu.get_barrier_semaphore()
    loads = [pltpu.make_async_copy(r[a], r[b], r["lsem"].at[i]) for i, (a, b) in enumerate((("b", "B0"), ("w", "A0"), ("c", "CM")))]
    for c in loads:
        c.start()
    for o in OFFS + OFF2X + OFF2Y:

        @pl.when(has(o))
        def _():
            pl.semaphore_signal(barrier, inc=1, device_id=dev(*o), device_id_type=MESH)

    for d in group_y + group_x + group_z:
        pl.semaphore_signal(barrier, inc=1, device_id=d, device_id_type=MESH)
    partners = sum(jnp.where(has(o), 1, 0) for o in OFFS + OFF2X + OFF2Y) + len(group_y + group_x + group_z)

    lane = lax.broadcasted_iota(jnp.int32, (8, 128), 1)
    row = lax.broadcasted_iota(jnp.int32, (8, 128), 0)
    zero = jnp.zeros((8, 128), F32)

    def flag(c):
        return jnp.where(c, jnp.float32(1), jnp.float32(0))

    mx = {-1: flag(ix > 0), 0: jnp.float32(1), 1: flag(ix < nx - 1)}
    my = {-1: flag(iy > 0), 0: jnp.float32(1), 1: flag(iy < ny - 1)}
    mz = {-1: flag(iz > 0), 0: jnp.float32(1), 1: flag(iz < nz - 1)}

    b_ref, w_ref, c_ref, out_ref = r["B0"], r["A0"], r["CM"], r["out"]

    G0, W0, V0 = r["G0"], r["W0"], r["V0"]
    loads[0].wait()
    loads[1].wait()
    w0 = w_ref[...]
    g0 = b_ref[0] / w0
    W0[2:18, 8:24, :] = w0
    G0[2:18, 8:24, :] = g0

    r["YS"][0] = G0[2:18, 8:10, :]
    r["YS"][1] = G0[2:18, 22:24, :]

    def pack_q(src, dst):
        for h in range(2):
            acc = zero
            for x in range(16):
                m = src[x + 2, 8 + 8 * h : 16 + 8 * h, :]
                base = 6 * (x + 2)
                acc = jnp.where((lane >= base) & (lane < base + 3), roll(m, base - 126), acc)
                acc = jnp.where((lane >= base + 3) & (lane < base + 6), roll(m, base + 3 - 127), acc)
            dst[8 * h : 8 * h + 8, :] = acc

    pack_q(G0, r["QS"])
    r["QE"][0] = r["QS"][0:1, :]
    r["QE"][1] = r["QS"][15:16, :]

    pl.semaphore_wait(barrier, partners)

    gsl = pl.ds(8, 16)
    wait_g0 = [
        round_of(
            0,
            [
                ((-1, 0, 0), G0.at[pl.ds(2, 2), gsl], G0.at[pl.ds(18, 2), gsl]),
                ((1, 0, 0), G0.at[pl.ds(16, 2), gsl], G0.at[pl.ds(0, 2), gsl]),
            ],
            lambda n: G0.at[pl.ds(0, 2 * n), gsl],
        ),
        round_of(1, [((0, d, 0), r["YS"].at[i], r["RY"].at[1 - i]) for i, d in enumerate((-1, 1))], first(r["RY"])),
        round_of(
            2,
            [
                ((dx, dy, 0), r["YS"].at[(dy + 1) // 2, 0 if dx < 0 else 15], r["RXY"].at[XY.index((-dx, -dy))])
                for dx, dy in XY
            ],
            first(r["RXY"]),
        ),
        round_of(3, [((dx, 0, dz), r["QS"], r["RQ"].at[XZ.index((-dx, -dz))]) for dx, dz in XZ], first(r["RQ"])),
        round_of(
            4,
            [((0, dy, dz), r["QE"].at[(dy + 1) // 2], r["RQE"].at[XY.index((-dy, -dz))]) for dy, dz in XY],
            first(r["RQE"]),
        ),
    ]

    for name in ("G0", "W0", "V0"):
        a = r[name]
        a[:, 0:8, :] = jnp.zeros((20, 8, 128), F32)
        a[:, 24:32, :] = jnp.zeros((20, 8, 128), F32)
    for name in ("GQ", "WQ", "VQ", "UQ", "G1", "W1", "V1", "U1", "G2", "W2", "V2", "U2", "P2", "Q2", "G3", "W3", "V3", "U3", "P3", "T4", "A1", "Q1", "R2", "PT", "QT", "Q3"):
        r[name][...] = jnp.zeros(r[name].shape, F32)

    zr = lax.broadcasted_iota(jnp.int32, (256, 128), 0) % 128
    zc = lax.broadcasted_iota(jnp.int32, (256, 128), 1)
    down = jnp.where(zc == 32 + zr // 2, jnp.float32(1), jnp.float32(0)).astype(jnp.bfloat16)
    up = jnp.where(zr == 32 + zc // 2, jnp.float32(1), jnp.float32(0)).astype(jnp.bfloat16)

    C0 = r["C0"]

    def coarsen0(values, scale):
        C0[...] = jnp.sum(values.reshape(8, 2, 16, 128), axis=1)
        t = C0[:, pl.ds(0, 8, stride=2), :] + C0[:, pl.ds(1, 8, stride=2), :]
        return (select_dot(t.reshape(64, 128), down) * scale).reshape(8, 8, 128)

    def pair_z(t, dil):
        ln = lax.broadcasted_iota(jnp.int32, t.shape, t.ndim - 1)
        return t + jnp.where((ln // dil) % 2 == 0, roll(t, -dil), roll(t, dil))

    C1, C2 = r["C1"], r["C2"]

    def coarsen1(values, scale):
        n = values.shape[0] // 2
        C1[...] = jnp.sum(values.reshape(n, 2, 8, 128), axis=1)
        t = C1[:, pl.ds(0, 4, stride=2), :] + C1[:, pl.ds(1, 4, stride=2), :]
        return pair_z(t, 1) * scale

    w1 = coarsen0(w0, 0.0625)
    own1 = (lane >= 32) & (lane < 96)
    w2 = coarsen1(w1, 0.0625)
    C2[0:4, 0:4, :] = w2
    t = C2[0:4, pl.ds(0, 2, stride=2), :] + C2[0:4, pl.ds(1, 2, stride=2), :]
    w3 = pair_z(jnp.sum(t.reshape(2, 2, 2, 128), axis=1), 2) * 0.0625

    lane4 = lane[0:4]

    def pack2(v):
        halves = []
        for h in range(2):
            a = jnp.where(lane4 % 2 == 0, v[2 * h], v[2 * h + 1])
            halves.append(roll(a, -32 if h == 0 else 32))
        return jnp.where(lane4 < 64, halves[0], halves[1])

    def pack3(v):
        return jnp.where(lane[0:2] < 64, roll(v[0], -32), roll(v[1], 32))

    SW2, SW3, SWZ = r["SW2"], r["SW3"], r["SWZ"]
    p2 = pack2(w2)
    SW2[...] = p2
    SW3[...] = pack3(w3)
    zp = jnp.zeros((4, 128), F32)
    for h in range(2):
        zp = jnp.where((lane4 >= 16 * h) & (lane4 < 16 * h + 8), roll(p2, -48 * h), zp)
        zp = jnp.where((lane4 >= 16 * h + 8) & (lane4 < 16 * h + 16), roll(p2, -48 * h - 48), zp)
    row4 = row[0:4]
    SWZ[...] = sum(roll(jnp.sum(jnp.where(row4 == y, zp, 0.0), axis=0, keepdims=True), 32 * y) for y in range(4))

    def send_all(src, dst, key):
        return [round_of(key, [(o, src, dst.at[SLOT[neg(o)]]) for o in OFFS], first(dst))]

    def pack_z1(own, zs):
        acc = zero
        for x in range(8):
            acc = jnp.where((lane >= 16 * x) & (lane < 16 * x + 4), roll(own[x], 16 * x - 32), acc)
            acc = jnp.where((lane >= 16 * x + 4) & (lane < 16 * x + 8), roll(own[x], 16 * x + 4 - 92), acc)
        zs[...] = acc

    s1w, ysw, zsw, yzw = r["S1w"], r["YS1w"], r["ZS1w"], r["YZ1w"]
    s1w[...] = w1
    ysw[0] = s1w[:, 0:2, :]
    ysw[1] = s1w[:, 6:8, :]
    pack_z1(w1, zsw)
    yzw[0] = zsw[0:2, :]
    yzw[1] = zsw[6:8, :]
    RX, RY, RXY, RZ, RYZ = (r[name + "w"] for name in ("RX1", "RY1", "RXY1", "RZ1", "RYZ1"))
    wait_w = [
        round_of(7, [((0, -1, 0), ysw.at[0], RY.at[1]), ((0, 1, 0), ysw.at[1], RY.at[0])], first(RY)),
        round_of(
            8,
            [
                ((dx, dy, 0), ysw.at[(dy + 1) // 2, 0 if dx < 0 else 7], RXY.at[XY.index((-dx, -dy))])
                for dx, dy in XY
            ],
            first(RXY),
        ),
        round_of(
            27,
            [((0, dy, dz), yzw.at[(dy + 1) // 2], RYZ.at[XY.index((-dy, -dz))]) for dy, dz in XY],
            first(RYZ),
        ),
        round_of(5, [(o, SW2, r["RW2"].at[FLAT.index(neg(o))]) for o in FLAT], first(r["RW2"])),
        round_of(17, [(o, SWZ, r["RWZ"].at[ZSLOT[neg(o)]]) for o in ZOFFS], first(r["RWZ"])),
        round_of(18, [(o, SW3, r["RW3"].at[SLOT[neg(o)]]) for o in OFFS], first(r["RW3"])),
        round_of(25, [(o, SW3, r["RW3Y"].at[OFF2Y.index(neg(o))]) for o in OFF2Y], first(r["RW3Y"])),
        round_of(24, [(o, SW3, r["RW3X"].at[OFF2X.index(neg(o))]) for o in OFF2X], first(r["RW3X"])),
        round_of(6, [((-1, 0, 0), s1w.at[pl.ds(0, 2)], RX.at[1]), ((1, 0, 0), s1w.at[pl.ds(6, 2)], RX.at[0])], first(RX)),
        round_of(9, [((dx, 0, dz), zsw, RZ.at[XZ.index((-dx, -dz))]) for dx, dz in XZ], first(RZ)),
    ]

    def recv1w(dst):
        for x in range(1, 13):
            dx = -1 if x < 3 else (1 if x > 10 else 0)
            sx = x - 3 if dx == 0 else (x + 5 if dx < 0 else x - 11)

            def ends(v, ln, lo, hi, dx, dy):
                v = jnp.where((ln >= 28) & (ln < 32), keep(roll(lo, 28 - 16 * sx - 4), dx, dy, -1), v)
                return jnp.where((ln >= 96) & (ln < 100), keep(roll(hi, 96 - 16 * sx), dx, dy, 1), v)

            base = w1[x - 3] if dx == 0 else keep(RX[(dx + 1) // 2, x - 1 if dx < 0 else x - 11], dx, 0, 0)
            lo, hi = (RZ[XZ.index((dx, dz))] for dz in (-1, 1))
            dst[x, 8:16, :] = ends(base, lane, lo, hi, dx, 0)
            for dy, at in ((-1, 6), (1, 16)):
                if dx == 0:
                    lo, hi = (RYZ[XY.index((dy, dz))] for dz in (-1, 1))
                    v = keep(RY[(dy + 1) // 2, x - 3], 0, dy, 0)
                    dst[x, at : at + 2, :] = ends(v, lane[0:2], lo, hi, 0, dy)
                elif x in (2, 11):
                    dst[x, at : at + 2, :] = keep(RXY[XY.index((dx, dy))], dx, dy, 0)

    def send1(own, n, key):
        s1, ys, zs = r["S1" + n], r["YS1" + n], r["ZS1" + n]
        s1[...] = own
        ys[0] = s1[:, 0:4, :]
        ys[1] = s1[:, 4:8, :]
        pack_z1(own, zs)
        rx, ry, rxy, rz = (r[name + n] for name in ("RX1", "RY1", "RXY1", "RZ1"))
        return [
            round_of(
                key,
                [((-1, 0, 0), s1.at[pl.ds(0, 3)], rx.at[1]), ((1, 0, 0), s1.at[pl.ds(5, 3)], rx.at[0])],
                first(rx),
            ),
            round_of(key + 1, [((0, -1, 0), ys.at[0], ry.at[1]), ((0, 1, 0), ys.at[1], ry.at[0])], first(ry)),
            round_of(
                key + 2,
                [
                    ((dx, dy, 0), ys.at[(dy + 1) // 2, pl.ds(0 if dx < 0 else 5, 3)], rxy.at[XY.index((-dx, -dy))])
                    for dx, dy in XY
                ],
                first(rxy),
            ),
            round_of(key + 3, [(o, zs, rz.at[ZSLOT[neg(o)]]) for o in ZOFFS], first(rz)),
        ]

    def recv1(own, n, key, dst):
        run(key)
        for x in range(14):
            dx = -1 if x < 3 else (1 if x > 10 else 0)
            for dy in (-1, 0, 1):
                if dx == 0 and dy == 0:
                    base = own[x - 3]
                elif dy == 0:
                    base = r["RX1" + n][(dx + 1) // 2, x if dx < 0 else x - 11]
                elif dx == 0:
                    base = r["RY1" + n][(dy + 1) // 2, x - 3]
                else:
                    base = r["RXY1" + n][XY.index((dx, dy)), x if dx < 0 else x - 11]
                sx = x - 3 if dx == 0 else (x + 5 if dx < 0 else x - 11)
                rows = slice(0, 8) if dy == 0 else (slice(4, 8) if dy < 0 else slice(0, 4))
                lo = r["RZ1" + n][ZSLOT[(dx, dy, -1)], rows, :]
                hi = r["RZ1" + n][ZSLOT[(dx, dy, 1)], rows, :]
                ln = lane[0:8] if dy == 0 else lane4
                v = keep(base, dx, dy, 0)
                v = jnp.where((ln >= 28) & (ln < 32), keep(roll(lo, 28 - 16 * sx - 4), dx, dy, -1), v)
                v = jnp.where((ln >= 96) & (ln < 100), keep(roll(hi, 96 - 16 * sx), dx, dy, 1), v)
                at = 8 if dy == 0 else (4 if dy < 0 else 16)
                dst[x, at : at + (8 if dy == 0 else 4), :] = v

    r["YW"][0] = W0[2:18, 8:9, :]
    r["YW"][1] = W0[2:18, 23:24, :]
    pack_q(W0, r["QW"])
    wait_w0 = [
        round_of(
            14,
            [
                ((-1, 0, 0), W0.at[pl.ds(2, 1), gsl], W0.at[pl.ds(18, 1), gsl]),
                ((1, 0, 0), W0.at[pl.ds(17, 1), gsl], W0.at[pl.ds(1, 1), gsl]),
            ],
            lambda n: W0.at[pl.ds(0, n), gsl],
        ),
        round_of(15, [((0, d, 0), r["YW"].at[i], r["RYW"].at[1 - i]) for i, d in enumerate((-1, 1))], first(r["RYW"])),
        round_of(16, [((0, 0, d), r["QW"], r["RQW"].at[1 - i]) for i, d in enumerate((-1, 1))], first(r["RQW"])),
    ]

    wi1 = 1.0 / jnp.where(own1, w1, 1.0)
    wi2 = 1.0 / jnp.where(own1[0:4], w2, 1.0)

    GQ, VQ = r["GQ"], r["VQ"]
    run(wait_g0)
    G0[0:2, 8:24, :] = keep(G0[0:2, 8:24, :], -1, 0, 0)
    G0[18:20, 8:24, :] = keep(G0[18:20, 8:24, :], 1, 0, 0)
    G0[2:18, 6:8, :] = keep(r["RY"][0], 0, -1, 0)
    G0[2:18, 24:26, :] = keep(r["RY"][1], 0, 1, 0)
    for dx, dy in XY:
        v = keep(r["RXY"][XY.index((dx, dy))], dx, dy, 0)
        G0[1 if dx < 0 else 18, 7 if dy < 0 else 24, :] = v[1 if dy < 0 else 0, :]

    def qj(ln):
        return ln % 6

    for h in range(2):
        sl = slice(8 * h, 8 * h + 8)
        own = r["QS"][sl, :]
        j = qj(lane)
        q = [keep(r["RQ"][i, sl, :], dx, 0, dz) for i, (dx, dz) in enumerate(XZ)]
        v, lo, hi = (jnp.where(j < 2, q[2 * i], jnp.where(j > 3, q[2 * i + 1], own if i == 0 else 0.0)) for i in range(3))
        v = jnp.where((lane >= 6) & (lane < 12), roll(lo, 6 - 102), jnp.where((lane >= 108) & (lane < 114), roll(hi, 108 - 12), v))
        GQ[8 + 8 * h : 16 + 8 * h, :] = jnp.where((lane >= 6) & (lane < 114), v, 0.0)
    for dy, at in ((-1, 7), (1, 24)):
        j = qj(lane[0:1])
        lo = keep(r["RQE"][XY.index((dy, -1))], 0, dy, -1)
        hi = keep(r["RQE"][XY.index((dy, 1))], 0, dy, 1)
        v = jnp.where(j < 2, lo, jnp.where(j > 3, hi, 0.0))
        GQ[at : at + 1, :] = jnp.where((lane[0:1] >= 12) & (lane[0:1] < 108), v, 0.0)

    INJ = r["INJ"]

    def inject(q, xs, tiles):
        for at in tiles:
            m = q[at : at + 8, :]
            for xp in xs:
                a = roll(m, -(6 * xp + 1))
                c = roll(m, 127 - (6 * xp + 4))
                INJ[xp, at : at + 8, :] = jnp.where(lane == 0, a, jnp.where(lane == 127, c, 0.0))

    def sum0(a, x, n, at):
        c = a[x : x + n, at : at + 8, :]
        t = a[x - 1 : x + n - 1, at : at + 8, :] + a[x + 1 : x + n + 1, at : at + 8, :]
        t = t + (a[x : x + n, at - 1 : at + 7, :] + a[x : x + n, at + 1 : at + 9, :])
        z = jnp.where(lane == 0, 0.0, roll(c, 1)) + jnp.where(lane == 127, 0.0, roll(c, -1))
        return c, t + (z + INJ[x : x + n, at : at + 8, :])

    inject(GQ, range(1, 19), (7, 15, 17))
    for at in (7, 15, 17):
        c, t = sum0(G0, 1, 18, at)
        v = S * (1.2 * c + S * t)
        if at == 7:
            v = v * jnp.where(row == 0, my[-1], 1.0)
        if at == 17:
            v = v * jnp.where(row == 7, my[1], 1.0)
        V0[1:19, at : at + 8, :] = v
    V0[1:2, 7:25, :] = V0[1:2, 7:25, :] * mx[-1]
    V0[18:19, 7:25, :] = V0[18:19, 7:25, :] * mx[1]

    for at in (8, 16):
        c = GQ[at : at + 8, :]
        t = roll(c, 1) + roll(c, -1) + roll(c, 6) + roll(c, -6)
        t = t + GQ[at - 1 : at + 7, :] + GQ[at + 1 : at + 9, :]
        j = qj(lane)
        mask = jnp.where(j == 1, mz[-1], jnp.where(j == 4, mz[1], 0.0))
        mask = jnp.where((lane >= 12) & (lane < 108), mask, 0.0)
        VQ[at : at + 8, :] = S * (1.2 * c + S * t) * mask

    inject(VQ, range(2, 18), (8, 16))
    halves = []
    for at in (8, 16):
        c, t = sum0(V0, 2, 16, at)
        halves.append(W0[2:18, at : at + 8, :] * (G0[2:18, at : at + 8, :] - 6.0 * c + t))
    r0 = jnp.concatenate(halves, axis=1)
    g1 = jnp.where(own1, coarsen0(r0, 0.125) * wi1, 0.0)
    wait_g1 = send1(g1, "g", 10)

    G1, W1, V1, U1 = r["G1"], r["W1"], r["V1"], r["U1"]
    G2, W2, V2, U2, P2, Q2 = r["G2"], r["W2"], r["V2"], r["U2"], r["P2"], r["Q2"]
    G3, W3, V3, U3, P3 = r["G3"], r["W3"], r["V3"], r["U3"], r["P3"]
    run(wait_w)
    recv1w(W1)

    def spread(m0, lo, hi, l, dx, dy):
        return keep(m0, dx, dy, 0), jnp.where((l // 32) % 2 == 1, keep(lo, dx, dy, -1), keep(hi, dx, dy, 1))

    def place(m0, c, l, h):
        a = roll(m0, 32 if h == 0 else 96)
        e = roll(c, 96 if h == 0 else 32)
        return jnp.where((l >= 32) & (l < 96), a, e)

    def piece(buf, own, rows, o):
        return own[rows, :] if o == (0, 0, 0) else buf[SLOT[o], rows, :]

    def unpack2(buf, own, dst):
        rows = slice(0, 4)
        for dx in (-1, 0, 1):
            for dy in (-1, 0, 1):
                m0, c = spread(*[piece(buf, own, rows, (dx, dy, dz)) for dz in (0, -1, 1)], lane4, dx, dy)
                spread2(m0, c, dst, dx, dy)

    def spread2(m0, c, dst, dx, dy):
        for p in range(2):
            take = lane4 % 2 == p
            a = jnp.where(take, m0, roll(m0, 1 if p == 0 else -1))
            e = jnp.where(take, c, roll(c, 1 if p == 0 else -1))
            for h in range(2):
                dst[4 + 4 * dx + 2 * h + p, 8 + 4 * dy : 12 + 4 * dy, :] = place(a, e, lane4, h)

    def unpack3(get, spots, dst):
        l = lane[0:2]
        for dx, dy in spots:
            m0, c = spread(*[get((dx, dy, dz)) for dz in (0, -1, 1)], l, dx, dy)
            for h in range(2):
                dst[5 + 2 * dx + h, 12 + 2 * dy : 14 + 2 * dy, :] = place(m0, c, l, h)

    for dx in (-1, 0, 1):
        for dy in (-1, 0, 1):
            m0 = keep(SW2[...] if dx == dy == 0 else r["RW2"][FLAT.index((dx, dy, 0))], dx, dy, 0)
            lo, hi = (keep(r["RWZ"][ZSLOT[(dx, dy, dz)]], dx, dy, dz) for dz in (-1, 1))
            line = jnp.where(lane[0:1] % 16 >= 8, lo, hi)
            e = jnp.zeros((4, 128), F32)
            for y in range(4):
                e = jnp.where(row4 == y, roll(line, -32 * y), e)
            c = jnp.zeros((4, 128), F32)
            for h in range(2):
                c = jnp.where((lane4 >= 64 * h) & (lane4 < 64 * h + 8), roll(e, 48 * h), c)
                c = jnp.where((lane4 >= 64 * h + 56) & (lane4 < 64 * h + 64), roll(e, 48 * h + 48), c)
            spread2(m0, c, W2, dx, dy)

    def piece3(o):
        if o == (0, 0, 0):
            return SW3[...]
        if abs(o[0]) == 2:
            return r["RW3X"][OFF2X.index(o)]
        if abs(o[1]) == 2:
            return r["RW3Y"][OFF2Y.index(o)]
        return r["RW3"][SLOT[o]]

    unpack3(piece3, [(a, b) for a in range(-2, 3) for b in range(-2, 3) if abs(a) < 2 or abs(b) < 2], W3)

    def inverse(w):
        return jnp.where(w > 0.0, 1.0 / jnp.where(w > 0.0, w, 1.0), 0.0)

    def nsum(a, x, n, at, rows, dil):
        c = a[x : x + n, at : at + rows, :]
        t = a[x - 1 : x + n - 1, at : at + rows, :] + a[x + 1 : x + n + 1, at : at + rows, :]
        t = t + (a[x : x + n, at - 1 : at + rows - 1, :] + a[x : x + n, at + 1 : at + rows + 1, :])
        return c, t + (roll(c, dil) + roll(c, -dil))

    def rowmask(at, rows, low, high):
        y = lax.broadcasted_iota(jnp.int32, (rows, 128), 0) + at
        l = lax.broadcasted_iota(jnp.int32, (rows, 128), 1)
        m = jnp.where(y < low, my[-1], jnp.where(y >= high, my[1], 1.0))
        return m * jnp.where(l < 32, mz[-1], jnp.where(l >= 96, mz[1], 1.0))

    def xmask(a, low, high, x, n, at, rows):
        if low > x:
            a[x:low, at : at + rows, :] = a[x:low, at : at + rows, :] * mx[-1]
        if x + n > high:
            a[high : x + n, at : at + rows, :] = a[high : x + n, at : at + rows, :] * mx[1]

    A1, Q1, R2, PT, QT, Q3 = r["A1"], r["Q1"], r["R2"], r["PT"], r["QT"], r["Q3"]
    A1[3:11, 8:16, :] = g1
    for at in (4, 12):
        c, t = nsum(A1, 1, 12, at, 8, 1)
        Q1[1:13, at : at + 8, :] = S * (1.2 * c + S * t) * rowmask(at, 8, 8, 16)
    xmask(Q1, 3, 11, 1, 12, 4, 16)
    C3 = r["C3"]
    for at in (6, 10):
        c, t = nsum(Q1, 1, 12, at, 8, 1)
        res = W1[1:13, at : at + 8, :] * (A1[1:13, at : at + 8, :] - 6.0 * c + t)
        C3[:, at - 6 : at + 2, :] = jnp.sum(res.reshape(6, 2, 8, 128), axis=1)
    t = C3[:, pl.ds(0, 6, stride=2), :] + C3[:, pl.ds(1, 6, stride=2), :]
    P2[3:9, 7:13, :] = pair_z(t, 1) * 0.125 * inverse(W2[3:9, 7:13, :])
    c, t = nsum(P2, 2, 8, 6, 8, 2)
    Q2[2:10, 6:14, :] = S * (1.2 * c + S * t) * rowmask(6, 8, 8, 12)
    xmask(Q2, 4, 8, 2, 8, 6, 8)
    for at in (5, 7):
        c, t = nsum(Q2, 1, 10, at, 8, 2)
        R2[1:11, at : at + 8, :] = W2[1:11, at : at + 8, :] * (P2[1:11, at : at + 8, :] - 6.0 * c + t)
    C3[...] = jnp.sum(R2[:, 4:20, :].reshape(6, 2, 16, 128), axis=1)
    t = C3[:, pl.ds(0, 6, stride=2), :] + C3[:, pl.ds(1, 6, stride=2), :]
    b3 = pair_z(t, 2) * 0.125
    P3[3:9, 10:16, :] = b3 * inverse(W3[3:9, 10:16, :])
    c, t = nsum(P3, 2, 8, 9, 8, 4)
    Q3[2:10, 9:17, :] = S * (1.2 * c + S * t) * rowmask(9, 8, 12, 14)
    xmask(Q3, 5, 7, 2, 8, 9, 8)
    T4 = r["T4"]
    for at in (8, 10):
        c, t = nsum(Q3, 1, 10, at, 8, 4)
        res = W3[1:11, at : at + 8, :] * (P3[1:11, at : at + 8, :] - 6.0 * c + t)
        T4[:, at : at + 8, :] = jnp.sum(res.reshape(5, 2, 8, 128), axis=1)
    t = T4[:, pl.ds(8, 8, stride=2), :] + T4[:, pl.ds(9, 8, stride=2), :]
    patch = pair_z(t, 4) * 0.125

    lines = []
    for dx in range(5):
        v = patch[dx]
        main = zero
        for q in range(4):
            lo = 32 + 16 * q + 7
            main = jnp.where((lane >= 2 * q) & (lane < 2 * q + 2), roll(v, 2 * q - lo), main)
        edge = jnp.where(lane < 2, roll(v, 0 - 23), jnp.where(lane < 4, roll(v, 2 - 103), 0.0))
        line = pltpu.roll(main, 0, 1, stride=8, stride_axis=0) + pltpu.roll(edge, 40, 1, stride=4, stride_axis=0)
        lines.append(jnp.sum(line, axis=0, keepdims=True))
    GA, GB, GC = r["GA"], r["GB"], r["GC"]
    SA, SB, SZ = r["SA"], r["SB"], r["SZ"]
    for p in range(2):
        SA[p : p + 1, :] = lines[2 * p] + roll(lines[2 * p + 1], 64)
    SA[2:3, :] = lines[4]
    SA[3:4, :] = jnp.zeros((1, 128), F32)
    ga_at = ih * nx + ix
    to_group(21, SA, GA.at[ga_at], group_y)

    cp = r["CP"]
    loads[2].wait()

    @pl.loop(0, nx)
    def _(x):
        for z in range(nz):
            acc = zero
            for p in range(ny // 2):
                tile = c_ref[:, pl.ds(pl.multiple_of((x * (ny // 2) + p) * 128, 128), 128)]
                for q in range(2):
                    y = 2 * p + q
                    at = 8 * y
                    acc = jnp.where((lane >= at) & (lane < at + 8), roll(tile, at - 64 * q - 8 * z), acc)
            cp[x * nz + z] = acc

    run(wait_w0)
    W0[1:2, 8:24, :] = keep(W0[1:2, 8:24, :], -1, 0, 0)
    W0[18:19, 8:24, :] = keep(W0[18:19, 8:24, :], 1, 0, 0)
    W0[2:18, 7:8, :] = keep(r["RYW"][0], 0, -1, 0)
    W0[2:18, 24:25, :] = keep(r["RYW"][1], 0, 1, 0)
    for h in range(2):
        sl = slice(8 * h, 8 * h + 8)
        j = qj(lane)
        v = jnp.where(j == 1, keep(r["RQW"][0, sl, :], 0, 0, -1), jnp.where(j == 4, keep(r["RQW"][1, sl, :], 0, 0, 1), 0.0))
        r["WQ"][8 + 8 * h : 16 + 8 * h, :] = v

    from_group(21, GA, n_y - 1)
    GA[ga_at] = SA[...]
    sums = []
    for h in range(2):
        even, odd = zero, zero
        for p in range(3):
            m = zero
            for g in range(nx):
                m = jnp.where(row == g, GA[h * nx + g, p : p + 1, :], m)
            even = even + (m if p == 1 else pltpu.roll(m, (2 * p - 2) % 8, 0))
            if p < 2:
                odd = odd + pltpu.roll(m, (2 * p - 1) % 8, 0)
        sums.append(jnp.where(lane < 64, even, 0.0) + roll(jnp.where(lane < 64, 0.0, odd), 64))
    SB[...] = sums[0] + roll(sums[1], 64)
    to_group(22, SB, GB.at[ixx], group_x)

    recv1(g1, "g", wait_g1, G1)
    for at in (4, 12):
        c, t = nsum(G1, 1, 12, at, 8, 1)
        V1[1:13, at : at + 8, :] = S * (1.2 * c + S * t) * rowmask(at, 8, 8, 16)
    xmask(V1, 3, 11, 1, 12, 4, 16)
    c, t = nsum(V1, 3, 8, 8, 8, 1)
    r1 = W1[3:11, 8:16, :] * (G1[3:11, 8:16, :] - 6.0 * c + t)
    g2 = jnp.where(own1[0:4], coarsen1(r1, 0.125) * wi2, 0.0)

    PT[4:8, 8:12, :] = g2
    c, t = nsum(PT, 2, 8, 6, 8, 2)
    QT[2:10, 6:14, :] = S * (1.2 * c + S * t) * rowmask(6, 8, 8, 12)
    xmask(QT, 4, 8, 2, 8, 6, 8)
    c, t = nsum(QT, 2, 8, 6, 8, 2)
    res = W2[2:10, 6:14, :] * (PT[2:10, 6:14, :] - 6.0 * c + t)
    C2[...] = jnp.sum(res.reshape(4, 2, 8, 128), axis=1)
    t = C2[:, pl.ds(0, 4, stride=2), :] + C2[:, pl.ds(1, 4, stride=2), :]
    b3 = pair_z(t, 2) * 0.125
    SC = r["SC"]
    SC[0:4, :] = pack2(g2)
    l4 = lane4 % 4
    SC[4:8, :] = jnp.where(l4 < 2, jnp.where(l4 == 0, b3[0], b3[1]), jnp.where(l4 == 2, b3[2], b3[3]))
    wait_c = send_all(SC, r["RC"], 19)

    from_group(22, GB, xn - 1)
    GB[ixx] = SB[...]
    main = zero
    edges = [zero] * 5
    for k in range(xn):
        v = GB[k]
        for h in range(2):
            if xn == 8 and h == 1:
                continue
            shift = 8 * k - 16 + h * (8 * xn - 64)
            m = roll(v, shift)
            src = (lane - shift + 256) % 128
            if xn != 8:
                m = jnp.where(src // 64 == h, m, 0.0)
            main = main + jnp.where(src % 64 < 40, m, 0.0)
            for dy in range(5):
                a = 40 + 4 * dy
                edges[dy] = edges[dy] + jnp.where((src % 64 >= a) & (src % 64 < a + 4), m, 0.0)
    edge = zero
    for dy in range(5):
        edge = edge + roll(edges[dy], 4 * dy - 40)
    SZ[0] = main
    SZ[1] = edge
    to_group(23, SZ, GC.at[iz], group_z)

    run(wait_c)
    unpack2(r["RC"], SC, G2)
    c, t = nsum(G2, 2, 8, 6, 8, 2)
    V2[2:10, 6:14, :] = S * (1.2 * c + S * t) * rowmask(6, 8, 8, 12)
    xmask(V2, 4, 8, 2, 8, 6, 8)

    TB, TC, RC = r["TB"], r["TC"], r["RC"]
    for dy in (-1, 0, 1):
        acc = jnp.zeros((4, 128), F32)
        for dx in (-1, 0, 1):
            m0, lo, hi = (keep(piece(RC, SC, slice(4, 8), (dx, dy, dz)), dx, dy, dz) for dz in (0, -1, 1))
            e = jnp.where((lane4 >= 92) & (lane4 < 100), lo, jnp.where((lane4 >= 28) & (lane4 < 36), hi, 0.0))
            q = m0 + roll(e, 64)
            if dx < 0:
                q = jnp.where(l4 < 2, roll(q, -2), 0.0)
            if dx > 0:
                q = jnp.where(l4 >= 2, roll(q, 2), 0.0)
            acc = acc + q
        TB[dy + 1] = acc
    TC[0:2, :] = TB[1, 0:2, :] + TB[0, 2:4, :]
    TC[2:4, :] = TB[1, 2:4, :] + TB[2, 0:2, :]
    for i in range(4):
        v = roll(jnp.where(l4 == i, TC[...], 0.0), -i)
        v = v + roll(v, 1)
        v = v + roll(v, 2)
        G3[4 + i, 11:15, :] = v * inverse(W3[4 + i, 11:15, :])
    c, t = nsum(G3, 5, 2, 12, 2, 4)
    v3 = jnp.where(own1[0:2], S * (1.2 * c + S * t), 0.0)
    SE, SV, RE, RV = r["SE"], r["SV"], r["RE"], r["RV"]
    SV[...] = pack3(v3)
    wait_v = send_all(SV, RV, 26)

    from_group(23, GC, nz - 1)
    GC[iz, 0] = SZ[0]
    GC[iz, 1] = SZ[1]
    acc = [zero] * 4
    for z in range(nz):
        v = GC[z, 0]
        if z + 1 < nz:
            v = v + jnp.where(lane % 8 >= 6, roll(GC[z + 1, 1], 6), 0.0)
        if z > 0:
            v = v + jnp.where(lane % 8 < 2, roll(GC[z - 1, 1], -2), 0.0)
        for x in range(nx):
            acc[x % 4] = acc[x % 4] + cp[x * nz + z] * v[x : x + 1, :]
    acc = (acc[0] + acc[1]) + (acc[2] + acc[3])
    tot = jnp.sum(acc, axis=1, keepdims=True)
    e4 = jnp.sum(jnp.where((lane >= 32 + 8 * row) & (lane < 40 + 8 * row), tot, 0.0), axis=0, keepdims=True)
    SE[...] = e4
    wait_e = send_all(SE, RE, 20)
    run(wait_v)

    near = [(a, b) for a in (-1, 0, 1) for b in (-1, 0, 1)]
    unpack3(lambda o: SV[...] if o == (0, 0, 0) else RV[SLOT[o]], near, V3)
    run(wait_e)
    l1 = lane[0:1]
    par = []
    for dx in (-1, 0, 1):
        v = zero
        for dy in (-1, 0, 1):
            o = (dx, dy, 0)
            own = SE[...] if o == (0, 0, 0) else keep(RE[SLOT[o], 0:1, :], *o)
            lo, hi = (keep(RE[SLOT[(dx, dy, dz)], 0:1, :], dx, dy, dz) for dz in (-1, 1))
            e = jnp.where((l1 >= 32) & (l1 < 96), own, roll(jnp.where(l1 < 64, hi, lo), 64))
            y = 4 + 2 * dy
            v = jnp.where((row == y) | (row == y + 1), e, v)
        par.append(v)
    for i in range(6):
        U3[3 + i, 8:16, :] = V3[3 + i, 8:16, :] + W3[3 + i, 8:16, :] * par[i // 2]
    c, t = nsum(U3, 4, 4, 8, 8, 4)
    E3 = r["E3"]
    E3[...] = (0.2 * c + S * (G3[4:8, 8:16, :] + t)) * inverse(W3[4:8, 8:16, :])
    F2 = r["F2"]
    F2[:, pl.ds(0, 4, stride=2), :] = E3[:, 3:7, :]
    F2[:, pl.ds(1, 4, stride=2), :] = E3[:, 3:7, :]
    for i in range(8):
        U2[2 + i, 6:14, :] = V2[2 + i, 6:14, :] + W2[2 + i, 6:14, :] * F2[i // 2]
    c, t = nsum(U2, 3, 6, 6, 8, 2)
    E2 = r["E2"]
    E2[...] = (0.2 * c + S * (G2[3:9, 6:14, :] + t)) * inverse(W2[3:9, 6:14, :])
    F1 = r["F1"]
    F1[:, pl.ds(2, 6, stride=2), :] = E2[:, 1:7, :]
    F1[:, pl.ds(3, 6, stride=2), :] = E2[:, 1:7, :]
    for i in range(12):
        U1[1 + i, 6:18, :] = V1[1 + i, 6:18, :] + W1[1 + i, 6:18, :] * F1[i // 2, 2:14, :]
    E1 = r["E1"]
    for at in (7, 9):
        c, t = nsum(U1, 2, 10, at, 8, 1)
        E1[:, at - 7 : at + 1, :] = (0.2 * c + S * (G1[2:12, at : at + 8, :] + t)) * inverse(W1[2:12, at : at + 8, :])
    o = select_dot(E1[...].reshape(160, 128), up).reshape(10, 16, 128)
    F0 = r["F0"]
    O1 = r["O1"]
    O1[...] = o
    F0[:, pl.ds(6, 10, stride=2), :] = O1[:, 0:10, :]
    F0[:, pl.ds(7, 10, stride=2), :] = O1[:, 0:10, :]
    acc = zero
    for x in range(8):
        e = E1[x + 1, 1:9, :]
        for p in range(2):
            base = 6 * (2 * x + p + 2)
            acc = jnp.where(lane == base + 1, roll(e, base + 1 - 31), acc)
            acc = jnp.where(lane == base + 4, roll(e, base + 4 - 96), acc)
    UQ = r["UQ"]
    FQ = r["FQ"]
    FQ[...] = acc
    UQ[pl.ds(8, 8, stride=2), :] = FQ[...]
    UQ[pl.ds(9, 8, stride=2), :] = FQ[...]
    UQ[8:24, :] = VQ[8:24, :] + r["WQ"][8:24, :] * UQ[8:24, :]
    for i in range(18):
        V0[1 + i, 7:25, :] = V0[1 + i, 7:25, :] + W0[1 + i, 7:25, :] * F0[(i + 1) // 2, 7:25, :]
    inject(UQ, range(2, 18), (8, 16))
    for at in (8, 16):
        c, t = sum0(V0, 2, 16, at)
        out_ref[:, at - 8 : at, :] = 0.2 * c + S * (G0[2:18, at : at + 8, :] + t)

    def drain(key, slots, count, sizes):
        for n in sizes:

            @pl.when(count == n)
            def _():
                copy(slots(n), slots(n), key, right).wait_send()

    for item in sent:
        drain(*item)
    for key, buf, n in ((21, GA, n_y - 1), (22, GB, xn - 1), (23, GC, nz - 1)):
        copy(buf.at[pl.ds(0, n)], buf.at[pl.ds(0, n)], key, right).wait_send()


def scratch(dims):
    nx, ny, nz = dims
    xn = ny // 2
    v = {
        "B0": (1, 16, 16, 128), "A0": (16, 16, 128), "CM": (8, nx * ny * nz * 8),
        "G0": (20, 32, 128), "W0": (20, 32, 128), "V0": (20, 32, 128), "INJ": (20, 32, 128),
        "GQ": (32, 128), "VQ": (32, 128), "WQ": (32, 128), "UQ": (32, 128),
        "YS": (2, 16, 2, 128), "RY": (2, 16, 2, 128), "RXY": (4, 2, 128),
        "QS": (16, 128), "QW": (16, 128), "RQ": (6, 16, 128), "QE": (2, 1, 128), "RQE": (4, 1, 128),
        "YW": (2, 16, 1, 128), "RYW": (2, 16, 1, 128), "RQW": (2, 16, 128),
        "C0": (8, 16, 128), "C1": (4, 8, 128), "C2": (4, 8, 128),
        "SW2": (4, 128), "SW3": (2, 128), "SWZ": (1, 128), "RW2": (8, 4, 128), "RWZ": (18, 1, 128),
        "RW3": (26, 2, 128), "RW3X": (18, 2, 128), "RW3Y": (18, 2, 128), "C3": (6, 16, 128),
        "A1": (14, 24, 128), "Q1": (14, 24, 128), "R2": (12, 24, 128), "PT": (12, 24, 128), "QT": (12, 24, 128),
        "G1": (14, 24, 128), "W1": (14, 24, 128), "V1": (14, 24, 128), "U1": (14, 24, 128),
        "G2": (12, 24, 128), "W2": (12, 24, 128), "V2": (12, 24, 128), "U2": (12, 24, 128),
        "P2": (12, 24, 128), "Q2": (12, 24, 128),
        "G3": (12, 24, 128), "W3": (12, 24, 128), "V3": (12, 24, 128), "U3": (12, 24, 128), "P3": (12, 24, 128), "Q3": (12, 24, 128),
        "T4": (5, 24, 128),
        "SC": (8, 128), "RC": (26, 8, 128), "TB": (3, 4, 128), "TC": (4, 128), "SE": (1, 128), "RE": (26, 1, 128), "SV": (2, 128), "RV": (26, 2, 128),
        "SA": (4, 128), "SB": (8, 128), "SZ": (2, 8, 128),
        "GA": (2 * nx, 4, 128), "GB": (xn, 8, 128), "GC": (nz, 2, 8, 128), "CP": (nx * nz, 8, 128),
        "E3": (4, 8, 128), "F2": (4, 8, 128), "E2": (6, 8, 128), "F1": (6, 16, 128),
        "E1": (10, 16, 128), "O1": (10, 16, 128), "F0": (10, 32, 128), "FQ": (8, 128),
    }
    n = "g"
    v["S1" + n] = (8, 8, 128)
    v["YS1" + n] = (2, 8, 4, 128)
    v["ZS1" + n] = (8, 128)
    v["RX1" + n] = (2, 3, 8, 128)
    v["RY1" + n] = (2, 8, 4, 128)
    v["RXY1" + n] = (4, 3, 4, 128)
    v["RZ1" + n] = (18, 8, 128)
    n = "w"
    v["S1" + n] = (8, 8, 128)
    v["YS1" + n] = (2, 8, 2, 128)
    v["ZS1" + n] = (8, 128)
    v["YZ1" + n] = (2, 2, 128)
    v["RX1" + n] = (2, 2, 8, 128)
    v["RY1" + n] = (2, 8, 2, 128)
    v["RXY1" + n] = (4, 2, 128)
    v["RZ1" + n] = (6, 8, 128)
    v["RYZ1" + n] = (4, 2, 128)
    return v


def solution(mesh):
    dims = tuple(mesh.shape[a] for a in ("gx", "gy", "gz"))
    sizes = scratch(dims)

    def body(*args):
        names = ["b", "w", "c", "out"] + list(sizes) + ["ssem", "rsem", "lsem"]
        kernel(dims, dict(zip(names, args)))

    def per_device(sources, stiffness, coarse_inverse):
        vmem = pl.BlockSpec(memory_space=pltpu.VMEM)
        e = pl.pallas_call(
            body,
            out_shape=jax.ShapeDtypeStruct((16, 16, 128), F32),
            in_specs=[pl.BlockSpec(memory_space=pltpu.HBM)] * 3,
            out_specs=vmem,
            scratch_shapes=[pltpu.VMEM(s, F32) for s in sizes.values()] + [pltpu.SemaphoreType.DMA((28,))] * 2 + [pltpu.SemaphoreType.DMA((3,))],
            compiler_params=pltpu.CompilerParams(collective_id=0, has_side_effects=True, vmem_limit_bytes=24 * 2**20),
            name="vcycle",
        )(*[pltpu.with_memory_space_constraint(a, pltpu.HBM) for a in (sources, stiffness, coarse_inverse)])
        return (e / stiffness)[None]

    return jax.shard_map(
        per_device,
        mesh=mesh,
        in_specs=(P(None, "gx", "gy", "gz"), P("gx", "gy", "gz"), P(("gx", "gy", "gz"), None)),
        out_specs=P(None, "gx", "gy", "gz"),
        check_vma=False,
    )
```

```python
import functools
import itertools

import jax
import jax.numpy as jnp
from jax import lax
from jax.experimental import pallas as pl
from jax.experimental.pallas import tpu as pltpu
from jax.sharding import PartitionSpec as P

MESH = pl.DeviceIdType.MESH
F32 = jnp.float32
S = 0.8 / 6.0
OFFS = [o for o in itertools.product((-1, 0, 1), repeat=3) if o != (0, 0, 0)]
OFFS.sort(key=lambda o: (-abs(o[1]), -abs(o[2]), -abs(o[0])))
OFF2X = [(2 * a, b, c) for a in (-1, 1) for b in (-1, 0, 1) for c in (-1, 0, 1)]
OFF2Y = [(b, 2 * a, c) for a in (-1, 1) for b in (-1, 0, 1) for c in (-1, 0, 1)]
SLOT = {o: i for i, o in enumerate(OFFS)}
ZOFFS = [o for o in OFFS if o[2] != 0]
ZSLOT = {o: i for i, o in enumerate(ZOFFS)}
XY = [(-1, -1), (-1, 1), (1, -1), (1, 1)]
XZ = [(0, -1), (0, 1)] + XY


def neg(o):
    return tuple(-v for v in o)


def roll(v, shift):
    shift = shift % 128
    return v if shift == 0 else pltpu.roll(v, shift, v.ndim - 1)


def split2(v):
    hi = v.astype(jnp.bfloat16)
    lo = (v - hi.astype(F32)).astype(jnp.bfloat16)
    return jnp.concatenate([hi, lo], axis=1)


def select_dot(v, sel):
    return jnp.dot(split2(v), sel, preferred_element_type=F32)


def kernel(dims, refs):
    nx, ny, nz = dims
    xn = ny // 2
    n_y = nx * 2
    r = refs
    ix, iy, iz = lax.axis_index("gx"), lax.axis_index("gy"), lax.axis_index("gz")
    ih, ixx = iy // xn, iy % xn

    def dev(dx, dy, dz):
        return {
            "gx": lax.rem(ix + dx + nx, nx),
            "gy": lax.rem(iy + dy + ny, ny),
            "gz": lax.rem(iz + dz + nz, nz),
        }

    def copy(src, dst, key, device):
        return pltpu.make_async_remote_copy(
            src_ref=src,
            dst_ref=dst,
            send_sem=r["ssem"].at[key],
            recv_sem=r["rsem"].at[key],
            device_id=device,
            device_id_type=MESH,
        )

    cx = {-2: ix > 1, -1: ix > 0, 1: ix < nx - 1, 2: ix < nx - 2}
    cy = {-2: iy > 1, -1: iy > 0, 1: iy < ny - 1, 2: iy < ny - 2}
    cz = {-1: iz > 0, 1: iz < nz - 1}

    def has(o):
        c = [f[v] for f, v in zip((cx, cy, cz), o) if v]
        return functools.reduce(jnp.logical_and, c)

    def keep(v, *o):
        return jnp.where(has(o), v, 0.0) if any(o) else v

    sent = []

    def round_of(key, items, slots):
        for o, src, dst in items:

            @pl.when(has(o))
            def _():
                copy(src, dst, key, dev(*o)).start()

        offs = [o for o, _, _ in items]
        count = sum(jnp.where(has(o), 1, 0) for o in offs)
        spots = [sorted({0, 1, 2, n - 3, n - 2, n - 1} & set(range(n))) for n in dims]
        sizes = {sum(all(0 <= v + p < n for v, p, n in zip(o, at, dims)) for o in offs) for at in itertools.product(*spots)}
        sizes = sorted(n for n in sizes if n)
        sent.append((key, slots, count, sizes))

        def wait():
            for n in sizes:

                @pl.when(count == n)
                def _():
                    copy(slots(n), slots(n), key, right).wait_recv()

        return wait

    def first(ref):
        return lambda n: ref.at[pl.ds(0, n)]

    def to_group(key, src, dst, group):
        for d in group:
            copy(src, dst, key, d).start()

    def from_group(key, buf, n):
        copy(buf.at[pl.ds(0, n)], buf.at[pl.ds(0, n)], key, right).wait_recv()

    def run(waits):
        for w in waits:
            w()

    me = {"gx": ix, "gy": iy, "gz": iz}
    right = {"gx": lax.rem(ix + 1, nx), "gy": iy, "gz": iz}

    group_y = []
    for k in range(1, n_y):
        t = lax.rem(ih * nx + ix + k, n_y)
        group_y.append({"gx": t % nx, "gy": (t // nx) * xn + ixx, "gz": iz})
    group_x = [{"gx": ix, "gy": ih * xn + lax.rem(ixx + k, xn), "gz": iz} for k in range(1, xn)]
    group_z = [{"gx": ix, "gy": iy, "gz": lax.rem(iz + k, nz)} for k in range(1, nz)]

    barrier = pltpu.get_barrier_semaphore()
    loads = [pltpu.make_async_copy(r[a], r[b], r["lsem"].at[i]) for i, (a, b) in enumerate((("b", "B0"), ("w", "A0"), ("c", "CM")))]
    for c in loads:
        c.start()
    for d in group_x + group_y + group_z:
        pl.semaphore_signal(barrier, inc=1, device_id=d, device_id_type=MESH)

    for o in OFFS + OFF2Y + OFF2X:

        @pl.when(has(o))
        def _():
            pl.semaphore_signal(barrier, inc=1, device_id=dev(*o), device_id_type=MESH)

    partners = sum(jnp.where(has(o), 1, 0) for o in OFFS + OFF2X + OFF2Y) + len(group_y + group_x + group_z)

    lane = lax.broadcasted_iota(jnp.int32, (8, 128), 1)
    row = lax.broadcasted_iota(jnp.int32, (8, 128), 0)
    zero = jnp.zeros((8, 128), F32)

    def flag(c):
        return jnp.where(c, jnp.float32(1), jnp.float32(0))

    mx = {-1: flag(ix > 0), 0: jnp.float32(1), 1: flag(ix < nx - 1)}
    my = {-1: flag(iy > 0), 0: jnp.float32(1), 1: flag(iy < ny - 1)}
    mz = {-1: flag(iz > 0), 0: jnp.float32(1), 1: flag(iz < nz - 1)}

    b_ref, w_ref, c_ref, out_ref = r["B0"], r["A0"], r["CM"], r["out"]

    G0, W0, V0 = r["G0"], r["W0"], r["V0"]
    loads[0].wait()
    loads[1].wait()
    w0 = w_ref[...]
    g0 = b_ref[0] / w0
    W0[2:18, 8:24, :] = w0
    G0[2:18, 8:24, :] = g0

    r["YS"][0] = G0[2:18, 8:10, :]
    r["YS"][1] = G0[2:18, 22:24, :]

    def pack_q(src, dst):
        for h in range(2):
            acc = zero
            for x in range(16):
                m = src[x + 2, 8 + 8 * h : 16 + 8 * h, :]
                base = 6 * (x + 2)
                acc = jnp.where(lane == base, roll(m, base - 1), acc)
                acc = jnp.where((lane >= base + 1) & (lane < base + 3), roll(m, base + 1 - 127), acc)
                acc = jnp.where((lane >= base + 3) & (lane < base + 5), roll(m, base + 3 - 127), acc)
                acc = jnp.where(lane == base + 5, roll(m, base + 5 - 126), acc)
            dst[8 * h : 8 * h + 8, :] = acc

    pack_q(G0, r["QS"])
    r["QE"][0] = r["QS"][0:1, :]
    r["QE"][1] = r["QS"][15:16, :]

    for name in ("G0", "W0", "V0"):
        a = r[name]
        a[:, 0:8, :] = jnp.zeros((20, 8, 128), F32)
        a[:, 24:32, :] = jnp.zeros((20, 8, 128), F32)
    for name in ("GQ", "WQ", "VQ", "UQ", "G1", "W1", "V1", "U1", "G2", "W2", "V2", "U2", "P2", "Q2", "G3", "W3", "V3", "U3", "P3", "T4", "A1", "Q1", "R2", "PT", "QT", "Q3"):
        r[name][...] = jnp.zeros(r[name].shape, F32)

    zr = lax.broadcasted_iota(jnp.int32, (256, 128), 0) % 128
    zc = lax.broadcasted_iota(jnp.int32, (256, 128), 1)
    down = jnp.where(zc == 32 + zr // 2, jnp.float32(1), jnp.float32(0)).astype(jnp.bfloat16)
    up = jnp.where(zr == 32 + zc // 2, jnp.float32(1), jnp.float32(0)).astype(jnp.bfloat16)

    C0 = r["C0"]

    def coarsen0(values, scale):
        C0[...] = jnp.sum(values.reshape(8, 2, 16, 128), axis=1)
        t = C0[:, pl.ds(0, 8, stride=2), :] + C0[:, pl.ds(1, 8, stride=2), :]
        return (select_dot(t.reshape(64, 128), down) * scale).reshape(8, 8, 128)

    def pair_z(t, dil):
        ln = lax.broadcasted_iota(jnp.int32, t.shape, t.ndim - 1)
        return t + jnp.where((ln // dil) % 2 == 0, roll(t, -dil), roll(t, dil))

    C1, C2 = r["C1"], r["C2"]

    def coarsen1(values, scale):
        n = values.shape[0] // 2
        C1[...] = jnp.sum(values.reshape(n, 2, 8, 128), axis=1)
        t = C1[:, pl.ds(0, 4, stride=2), :] + C1[:, pl.ds(1, 4, stride=2), :]
        return pair_z(t, 1) * scale

    w1 = coarsen0(w0, 0.0625)
    own1 = (lane >= 32) & (lane < 96)
    w2 = coarsen1(w1, 0.0625)
    C2[0:4, 0:4, :] = w2
    t = C2[0:4, pl.ds(0, 2, stride=2), :] + C2[0:4, pl.ds(1, 2, stride=2), :]
    w3 = pair_z(jnp.sum(t.reshape(2, 2, 2, 128), axis=1), 2) * 0.0625

    lane4 = lane[0:4]

    def pack2(v):
        halves = []
        for h in range(2):
            a = jnp.where(lane4 % 2 == 0, v[2 * h], v[2 * h + 1])
            halves.append(roll(a, -32 if h == 0 else 32))
        return jnp.where(lane4 < 64, halves[0], halves[1])

    def pack3(v):
        return jnp.where(lane[0:2] < 64, roll(v[0], -32), roll(v[1], 32))

    SW2, SW3 = r["SW2"], r["SW3"]
    SW2[...] = pack2(w2)
    SW3[...] = pack3(w3)
    def send_all(src, dst, key):
        return [round_of(key, [(o, src, dst.at[SLOT[neg(o)]]) for o in OFFS], first(dst))]

    def pack_z1(own, zs):
        acc = zero
        for x in range(8):
            acc = jnp.where((lane >= 16 * x) & (lane < 16 * x + 4), roll(own[x], 16 * x - 32), acc)
            acc = jnp.where((lane >= 16 * x + 4) & (lane < 16 * x + 8), roll(own[x], 16 * x + 4 - 92), acc)
        zs[...] = acc

    s1w, ysw, zsw, yzw = r["S1w"], r["YS1w"], r["ZS1w"], r["YZ1w"]
    s1w[...] = w1
    ysw[0] = s1w[:, 0:2, :]
    ysw[1] = s1w[:, 6:8, :]
    pack_z1(w1, zsw)
    yzw[0] = zsw[0:2, :]
    yzw[1] = zsw[6:8, :]
    RX, RY, RXY, RZ, RYZ = (r[name + "w"] for name in ("RX1", "RY1", "RXY1", "RZ1", "RYZ1"))
    r["YW"][0] = W0[2:18, 8:9, :]
    r["YW"][1] = W0[2:18, 23:24, :]
    pack_q(W0, r["QW"])

    pl.semaphore_wait(barrier, partners)

    gsl = pl.ds(8, 16)
    wait_g0 = [
        round_of(1, [((0, d, 0), r["YS"].at[i], r["RY"].at[1 - i]) for i, d in enumerate((-1, 1))], first(r["RY"])),
        round_of(
            2,
            [
                ((dx, dy, 0), r["YS"].at[(dy + 1) // 2, 0 if dx < 0 else 15], r["RXY"].at[XY.index((-dx, -dy))])
                for dx, dy in XY
            ],
            first(r["RXY"]),
        ),
        round_of(
            4,
            [((0, dy, dz), r["QE"].at[(dy + 1) // 2], r["RQE"].at[XY.index((-dy, -dz))]) for dy, dz in XY],
            first(r["RQE"]),
        ),
        round_of(3, [((dx, 0, dz), r["QS"], r["RQ"].at[XZ.index((-dx, -dz))]) for dx, dz in XZ], first(r["RQ"])),
        round_of(
            0,
            [
                ((-1, 0, 0), G0.at[pl.ds(2, 2), gsl], G0.at[pl.ds(18, 2), gsl]),
                ((1, 0, 0), G0.at[pl.ds(16, 2), gsl], G0.at[pl.ds(0, 2), gsl]),
            ],
            lambda n: G0.at[pl.ds(0, 2 * n), gsl],
        ),
    ]

    wait_w = [
        round_of(7, [((0, -1, 0), ysw.at[0], RY.at[1]), ((0, 1, 0), ysw.at[1], RY.at[0])], first(RY)),
        round_of(
            8,
            [
                ((dx, dy, 0), ysw.at[(dy + 1) // 2, 0 if dx < 0 else 7], RXY.at[XY.index((-dx, -dy))])
                for dx, dy in XY
            ],
            first(RXY),
        ),
        round_of(
            27,
            [((0, dy, dz), yzw.at[(dy + 1) // 2], RYZ.at[XY.index((-dy, -dz))]) for dy, dz in XY],
            first(RYZ),
        ),
        round_of(5, [(o, SW2, r["RW2"].at[SLOT[neg(o)]]) for o in OFFS], first(r["RW2"])),
        round_of(18, [(o, SW3, r["RW3"].at[SLOT[neg(o)]]) for o in OFFS], first(r["RW3"])),
        round_of(25, [(o, SW3, r["RW3Y"].at[OFF2Y.index(neg(o))]) for o in OFF2Y], first(r["RW3Y"])),
        round_of(24, [(o, SW3, r["RW3X"].at[OFF2X.index(neg(o))]) for o in OFF2X], first(r["RW3X"])),
        round_of(6, [((-1, 0, 0), s1w.at[pl.ds(0, 2)], RX.at[1]), ((1, 0, 0), s1w.at[pl.ds(6, 2)], RX.at[0])], first(RX)),
        round_of(9, [((dx, 0, dz), zsw, RZ.at[XZ.index((-dx, -dz))]) for dx, dz in XZ], first(RZ)),
    ]

    def recv1w(dst):
        for x in range(1, 13):
            dx = -1 if x < 3 else (1 if x > 10 else 0)
            sx = x - 3 if dx == 0 else (x + 5 if dx < 0 else x - 11)

            def ends(v, ln, lo, hi, dx, dy):
                v = jnp.where((ln >= 28) & (ln < 32), keep(roll(lo, 28 - 16 * sx - 4), dx, dy, -1), v)
                return jnp.where((ln >= 96) & (ln < 100), keep(roll(hi, 96 - 16 * sx), dx, dy, 1), v)

            base = w1[x - 3] if dx == 0 else keep(RX[(dx + 1) // 2, x - 1 if dx < 0 else x - 11], dx, 0, 0)
            lo, hi = (RZ[XZ.index((dx, dz))] for dz in (-1, 1))
            dst[x, 8:16, :] = ends(base, lane, lo, hi, dx, 0)
            for dy, at in ((-1, 6), (1, 16)):
                if dx == 0:
                    lo, hi = (RYZ[XY.index((dy, dz))] for dz in (-1, 1))
                    v = keep(RY[(dy + 1) // 2, x - 3], 0, dy, 0)
                    dst[x, at : at + 2, :] = ends(v, lane[0:2], lo, hi, 0, dy)
                elif x in (2, 11):
                    dst[x, at : at + 2, :] = keep(RXY[XY.index((dx, dy))], dx, dy, 0)

    def send1(own, n, key):
        s1, ys, zs = r["S1" + n], r["YS1" + n], r["ZS1" + n]
        s1[...] = own
        ys[0] = s1[:, 0:4, :]
        ys[1] = s1[:, 4:8, :]
        pack_z1(own, zs)
        rx, ry, rxy, rz = (r[name + n] for name in ("RX1", "RY1", "RXY1", "RZ1"))
        return [
            round_of(
                key,
                [((-1, 0, 0), s1.at[pl.ds(0, 3)], rx.at[1]), ((1, 0, 0), s1.at[pl.ds(5, 3)], rx.at[0])],
                first(rx),
            ),
            round_of(key + 1, [((0, -1, 0), ys.at[0], ry.at[1]), ((0, 1, 0), ys.at[1], ry.at[0])], first(ry)),
            round_of(
                key + 2,
                [
                    ((dx, dy, 0), ys.at[(dy + 1) // 2, pl.ds(0 if dx < 0 else 5, 3)], rxy.at[XY.index((-dx, -dy))])
                    for dx, dy in XY
                ],
                first(rxy),
            ),
            round_of(key + 3, [(o, zs, rz.at[ZSLOT[neg(o)]]) for o in ZOFFS], first(rz)),
        ]

    def recv1(own, n, key, dst):
        run(key)
        for x in range(14):
            dx = -1 if x < 3 else (1 if x > 10 else 0)
            for dy in (-1, 0, 1):
                if dx == 0 and dy == 0:
                    base = own[x - 3]
                elif dy == 0:
                    base = r["RX1" + n][(dx + 1) // 2, x if dx < 0 else x - 11]
                elif dx == 0:
                    base = r["RY1" + n][(dy + 1) // 2, x - 3]
                else:
                    base = r["RXY1" + n][XY.index((dx, dy)), x if dx < 0 else x - 11]
                sx = x - 3 if dx == 0 else (x + 5 if dx < 0 else x - 11)
                rows = slice(0, 8) if dy == 0 else (slice(4, 8) if dy < 0 else slice(0, 4))
                lo = r["RZ1" + n][ZSLOT[(dx, dy, -1)], rows, :]
                hi = r["RZ1" + n][ZSLOT[(dx, dy, 1)], rows, :]
                ln = lane[0:8] if dy == 0 else lane4
                v = keep(base, dx, dy, 0)
                v = jnp.where((ln >= 28) & (ln < 32), keep(roll(lo, 28 - 16 * sx - 4), dx, dy, -1), v)
                v = jnp.where((ln >= 96) & (ln < 100), keep(roll(hi, 96 - 16 * sx), dx, dy, 1), v)
                at = 8 if dy == 0 else (4 if dy < 0 else 16)
                dst[x, at : at + (8 if dy == 0 else 4), :] = v

    wait_w0 = [
        round_of(
            14,
            [
                ((-1, 0, 0), W0.at[pl.ds(2, 1), gsl], W0.at[pl.ds(18, 1), gsl]),
                ((1, 0, 0), W0.at[pl.ds(17, 1), gsl], W0.at[pl.ds(1, 1), gsl]),
            ],
            lambda n: W0.at[pl.ds(0, n), gsl],
        ),
        round_of(15, [((0, d, 0), r["YW"].at[i], r["RYW"].at[1 - i]) for i, d in enumerate((-1, 1))], first(r["RYW"])),
        round_of(16, [((0, 0, d), r["QW"], r["RQW"].at[1 - i]) for i, d in enumerate((-1, 1))], first(r["RQW"])),
    ]

    wi1 = 1.0 / jnp.where(own1, w1, 1.0)
    wi2 = 1.0 / jnp.where(own1[0:4], w2, 1.0)

    GQ, VQ = r["GQ"], r["VQ"]
    run(wait_g0)
    G0[0:2, 8:24, :] = keep(G0[0:2, 8:24, :], -1, 0, 0)
    G0[18:20, 8:24, :] = keep(G0[18:20, 8:24, :], 1, 0, 0)
    G0[2:18, 6:8, :] = keep(r["RY"][0], 0, -1, 0)
    G0[2:18, 24:26, :] = keep(r["RY"][1], 0, 1, 0)
    for dx, dy in XY:
        v = keep(r["RXY"][XY.index((dx, dy))], dx, dy, 0)
        G0[1 if dx < 0 else 18, 7 if dy < 0 else 24, :] = v[1 if dy < 0 else 0, :]

    def qj(ln):
        return ln % 6

    for h in range(2):
        sl = slice(8 * h, 8 * h + 8)
        own = r["QS"][sl, :]
        j = qj(lane)
        q = [keep(r["RQ"][i, sl, :], dx, 0, dz) for i, (dx, dz) in enumerate(XZ)]
        v, lo, hi = (
            jnp.where((j == 3) | (j == 5), q[2 * i], jnp.where((j == 0) | (j == 2), q[2 * i + 1], own if i == 0 else 0.0))
            for i in range(3)
        )
        v = jnp.where((lane >= 6) & (lane < 12), roll(lo, 6 - 102), jnp.where((lane >= 108) & (lane < 114), roll(hi, 108 - 12), v))
        GQ[8 + 8 * h : 16 + 8 * h, :] = jnp.where((lane >= 6) & (lane < 114), v, 0.0)
    for dy, at in ((-1, 7), (1, 24)):
        j = qj(lane[0:1])
        lo = keep(r["RQE"][XY.index((dy, -1))], 0, dy, -1)
        hi = keep(r["RQE"][XY.index((dy, 1))], 0, dy, 1)
        v = jnp.where((j == 3) | (j == 5), lo, jnp.where((j == 0) | (j == 2), hi, 0.0))
        GQ[at : at + 1, :] = jnp.where((lane[0:1] >= 12) & (lane[0:1] < 108), v, 0.0)

    INJ = r["INJ"]

    def inject(q, xs, tiles):
        for at in tiles:
            m = q[at : at + 8, :]
            for xp in xs:
                INJ[xp, at : at + 8, :] = jnp.where((lane == 0) | (lane == 127), roll(m, -(6 * xp + 3)), 0.0)

    def sum0(a, x, n, at):
        c = a[x : x + n, at : at + 8, :]
        t = a[x - 1 : x + n - 1, at : at + 8, :] + a[x + 1 : x + n + 1, at : at + 8, :]
        t = t + (a[x : x + n, at - 1 : at + 7, :] + a[x : x + n, at + 1 : at + 9, :])
        z = jnp.where(lane == 0, 0.0, roll(c, 1)) + jnp.where(lane == 127, 0.0, roll(c, -1))
        return c, t + (z + INJ[x : x + n, at : at + 8, :])

    inject(GQ, range(1, 19), (7, 15, 17))
    for at in (7, 15, 17):
        c, t = sum0(G0, 1, 18, at)
        v = S * (1.2 * c + S * t)
        if at == 7:
            v = v * jnp.where(row == 0, my[-1], 1.0)
        if at == 17:
            v = v * jnp.where(row == 7, my[1], 1.0)
        V0[1:19, at : at + 8, :] = v
    V0[1:2, 7:25, :] = V0[1:2, 7:25, :] * mx[-1]
    V0[18:19, 7:25, :] = V0[18:19, 7:25, :] * mx[1]

    for at in (8, 16):
        c = GQ[at : at + 8, :]
        t = jnp.where(qj(lane) == 3, roll(c, -1) + roll(c, -2), roll(c, 1) + roll(c, 2)) + (roll(c, 6) + roll(c, -6))
        t = t + GQ[at - 1 : at + 7, :] + GQ[at + 1 : at + 9, :]
        j = qj(lane)
        mask = jnp.where(j == 3, mz[-1], jnp.where(j == 2, mz[1], 0.0))
        mask = jnp.where((lane >= 12) & (lane < 108), mask, 0.0)
        VQ[at : at + 8, :] = S * (1.2 * c + S * t) * mask

    inject(VQ, range(2, 18), (8, 16))
    halves = []
    for at in (8, 16):
        c, t = sum0(V0, 2, 16, at)
        halves.append(W0[2:18, at : at + 8, :] * (G0[2:18, at : at + 8, :] - 6.0 * c + t))
    r0 = jnp.concatenate(halves, axis=1)
    g1 = jnp.where(own1, coarsen0(r0, 0.125) * wi1, 0.0)
    wait_g1 = send1(g1, "g", 10)

    G1, W1, V1, U1 = r["G1"], r["W1"], r["V1"], r["U1"]
    G2, W2, V2, U2, P2, Q2 = r["G2"], r["W2"], r["V2"], r["U2"], r["P2"], r["Q2"]
    G3, W3, V3, U3, P3 = r["G3"], r["W3"], r["V3"], r["U3"], r["P3"]
    run(wait_w)
    recv1w(W1)

    def spread(m0, lo, hi, l, dx, dy):
        return keep(m0, dx, dy, 0), jnp.where((l // 32) % 2 == 1, keep(lo, dx, dy, -1), keep(hi, dx, dy, 1))

    def place(m0, c, l, h):
        a = roll(m0, 32 if h == 0 else 96)
        e = roll(c, 96 if h == 0 else 32)
        return jnp.where((l >= 32) & (l < 96), a, e)

    def piece(buf, own, rows, o):
        return own[rows, :] if o == (0, 0, 0) else buf[SLOT[o], rows, :]

    def unpack2(buf, own, dst):
        rows = slice(0, 4)
        for dx in (-1, 0, 1):
            for dy in (-1, 0, 1):
                m0, c = spread(*[piece(buf, own, rows, (dx, dy, dz)) for dz in (0, -1, 1)], lane4, dx, dy)
                for p in range(2):
                    take = lane4 % 2 == p
                    a = jnp.where(take, m0, roll(m0, 1 if p == 0 else -1))
                    e = jnp.where(take, c, roll(c, 1 if p == 0 else -1))
                    for h in range(2):
                        dst[4 + 4 * dx + 2 * h + p, 8 + 4 * dy : 12 + 4 * dy, :] = place(a, e, lane4, h)

    def unpack3(get, spots, dst):
        l = lane[0:2]
        for dx, dy in spots:
            m0, c = spread(*[get((dx, dy, dz)) for dz in (0, -1, 1)], l, dx, dy)
            for h in range(2):
                dst[5 + 2 * dx + h, 12 + 2 * dy : 14 + 2 * dy, :] = place(m0, c, l, h)

    unpack2(r["RW2"], SW2, W2)

    def piece3(o):
        if o == (0, 0, 0):
            return SW3[...]
        if abs(o[0]) == 2:
            return r["RW3X"][OFF2X.index(o)]
        if abs(o[1]) == 2:
            return r["RW3Y"][OFF2Y.index(o)]
        return r["RW3"][SLOT[o]]

    unpack3(piece3, [(a, b) for a in range(-2, 3) for b in range(-2, 3) if abs(a) < 2 or abs(b) < 2], W3)

    def inverse(w):
        return jnp.where(w > 0.0, 1.0 / jnp.where(w > 0.0, w, 1.0), 0.0)

    def nsum(a, x, n, at, rows, dil):
        c = a[x : x + n, at : at + rows, :]
        t = a[x - 1 : x + n - 1, at : at + rows, :] + a[x + 1 : x + n + 1, at : at + rows, :]
        t = t + (a[x : x + n, at - 1 : at + rows - 1, :] + a[x : x + n, at + 1 : at + rows + 1, :])
        return c, t + (roll(c, dil) + roll(c, -dil))

    def rowmask(at, rows, low, high):
        y = lax.broadcasted_iota(jnp.int32, (rows, 128), 0) + at
        l = lax.broadcasted_iota(jnp.int32, (rows, 128), 1)
        m = jnp.where(y < low, my[-1], jnp.where(y >= high, my[1], 1.0))
        return m * jnp.where(l < 32, mz[-1], jnp.where(l >= 96, mz[1], 1.0))

    def xmask(a, low, high, x, n, at, rows):
        if low > x:
            a[x:low, at : at + rows, :] = a[x:low, at : at + rows, :] * mx[-1]
        if x + n > high:
            a[high : x + n, at : at + rows, :] = a[high : x + n, at : at + rows, :] * mx[1]

    A1, Q1, R2, PT, QT, Q3 = r["A1"], r["Q1"], r["R2"], r["PT"], r["QT"], r["Q3"]
    A1[3:11, 8:16, :] = g1
    for at in (4, 12):
        c, t = nsum(A1, 1, 12, at, 8, 1)
        Q1[1:13, at : at + 8, :] = S * (1.2 * c + S * t) * rowmask(at, 8, 8, 16)
    xmask(Q1, 3, 11, 1, 12, 4, 16)
    C3 = r["C3"]
    for at in (6, 10):
        c, t = nsum(Q1, 1, 12, at, 8, 1)
        res = W1[1:13, at : at + 8, :] * (A1[1:13, at : at + 8, :] - 6.0 * c + t)
        C3[:, at - 6 : at + 2, :] = jnp.sum(res.reshape(6, 2, 8, 128), axis=1)
    t = C3[:, pl.ds(0, 6, stride=2), :] + C3[:, pl.ds(1, 6, stride=2), :]
    P2[3:9, 7:13, :] = pair_z(t, 1) * 0.125 * inverse(W2[3:9, 7:13, :])
    c, t = nsum(P2, 2, 8, 6, 8, 2)
    Q2[2:10, 6:14, :] = S * (1.2 * c + S * t) * rowmask(6, 8, 8, 12)
    xmask(Q2, 4, 8, 2, 8, 6, 8)
    for at in (5, 7):
        c, t = nsum(Q2, 1, 10, at, 8, 2)
        R2[1:11, at : at + 8, :] = W2[1:11, at : at + 8, :] * (P2[1:11, at : at + 8, :] - 6.0 * c + t)
    C3[...] = jnp.sum(R2[:, 4:20, :].reshape(6, 2, 16, 128), axis=1)
    t = C3[:, pl.ds(0, 6, stride=2), :] + C3[:, pl.ds(1, 6, stride=2), :]
    b3 = pair_z(t, 2) * 0.125
    P3[3:9, 10:16, :] = b3 * inverse(W3[3:9, 10:16, :])
    c, t = nsum(P3, 2, 8, 9, 8, 4)
    Q3[2:10, 9:17, :] = S * (1.2 * c + S * t) * rowmask(9, 8, 12, 14)
    xmask(Q3, 5, 7, 2, 8, 9, 8)
    T4 = r["T4"]
    for at in (8, 10):
        c, t = nsum(Q3, 1, 10, at, 8, 4)
        res = W3[1:11, at : at + 8, :] * (P3[1:11, at : at + 8, :] - 6.0 * c + t)
        T4[:, at : at + 8, :] = jnp.sum(res.reshape(5, 2, 8, 128), axis=1)
    t = T4[:, pl.ds(8, 8, stride=2), :] + T4[:, pl.ds(9, 8, stride=2), :]
    patch = pair_z(t, 4) * 0.125

    lines = []
    for dx in range(5):
        v = patch[dx]
        main = zero
        for q in range(4):
            lo = 32 + 16 * q + 7
            main = jnp.where((lane >= 2 * q) & (lane < 2 * q + 2), roll(v, 2 * q - lo), main)
        edge = jnp.where(lane < 2, roll(v, 0 - 23), jnp.where(lane < 4, roll(v, 2 - 103), 0.0))
        line = pltpu.roll(main, 0, 1, stride=8, stride_axis=0) + pltpu.roll(edge, 40, 1, stride=4, stride_axis=0)
        lines.append(jnp.sum(line, axis=0, keepdims=True))
    GA, GB, GC = r["GA"], r["GB"], r["GC"]
    SA, SB, SZ = r["SA"], r["SB"], r["SZ"]
    for p in range(2):
        SA[p : p + 1, :] = lines[2 * p] + roll(lines[2 * p + 1], 64)
    SA[2:3, :] = lines[4]
    SA[3:4, :] = jnp.zeros((1, 128), F32)
    ga_at = ih * nx + ix
    to_group(21, SA, GA.at[ga_at], group_y)

    cp = r["CP"]
    loads[2].wait()

    @pl.loop(0, nx)
    def _(x):
        for z in range(nz):
            acc = zero
            for p in range(ny // 2):
                tile = c_ref[:, pl.ds(pl.multiple_of((x * (ny // 2) + p) * 128, 128), 128)]
                for q in range(2):
                    y = 2 * p + q
                    at = 8 * y
                    acc = jnp.where((lane >= at) & (lane < at + 8), roll(tile, at - 64 * q - 8 * z), acc)
            cp[x * nz + z] = acc

    run(wait_w0)
    W0[1:2, 8:24, :] = keep(W0[1:2, 8:24, :], -1, 0, 0)
    W0[18:19, 8:24, :] = keep(W0[18:19, 8:24, :], 1, 0, 0)
    W0[2:18, 7:8, :] = keep(r["RYW"][0], 0, -1, 0)
    W0[2:18, 24:25, :] = keep(r["RYW"][1], 0, 1, 0)
    for h in range(2):
        sl = slice(8 * h, 8 * h + 8)
        j = qj(lane)
        v = jnp.where(j == 3, keep(r["RQW"][0, sl, :], 0, 0, -1), jnp.where(j == 2, keep(r["RQW"][1, sl, :], 0, 0, 1), 0.0))
        r["WQ"][8 + 8 * h : 16 + 8 * h, :] = v

    from_group(21, GA, n_y - 1)
    GA[ga_at] = SA[...]
    sums = []
    for h in range(2):
        even, odd = zero, zero
        for p in range(3):
            m = zero
            for g in range(nx):
                m = jnp.where(row == g, GA[h * nx + g, p : p + 1, :], m)
            even = even + (m if p == 1 else pltpu.roll(m, (2 * p - 2) % 8, 0))
            if p < 2:
                odd = odd + pltpu.roll(m, (2 * p - 1) % 8, 0)
        sums.append(jnp.where(lane < 64, even, 0.0) + roll(jnp.where(lane < 64, 0.0, odd), 64))
    SB[...] = sums[0] + roll(sums[1], 64)
    to_group(22, SB, GB.at[ixx], group_x)

    recv1(g1, "g", wait_g1, G1)
    for at in (4, 12):
        c, t = nsum(G1, 1, 12, at, 8, 1)
        V1[1:13, at : at + 8, :] = S * (1.2 * c + S * t) * rowmask(at, 8, 8, 16)
    xmask(V1, 3, 11, 1, 12, 4, 16)
    c, t = nsum(V1, 3, 8, 8, 8, 1)
    r1 = W1[3:11, 8:16, :] * (G1[3:11, 8:16, :] - 6.0 * c + t)
    g2 = jnp.where(own1[0:4], coarsen1(r1, 0.125) * wi2, 0.0)

    PT[4:8, 8:12, :] = g2
    c, t = nsum(PT, 2, 8, 6, 8, 2)
    QT[2:10, 6:14, :] = S * (1.2 * c + S * t) * rowmask(6, 8, 8, 12)
    xmask(QT, 4, 8, 2, 8, 6, 8)
    c, t = nsum(QT, 2, 8, 6, 8, 2)
    res = W2[2:10, 6:14, :] * (PT[2:10, 6:14, :] - 6.0 * c + t)
    C2[...] = jnp.sum(res.reshape(4, 2, 8, 128), axis=1)
    t = C2[:, pl.ds(0, 4, stride=2), :] + C2[:, pl.ds(1, 4, stride=2), :]
    b3 = pair_z(t, 2) * 0.125
    SC = r["SC"]
    SC[0:4, :] = pack2(g2)
    l4 = lane4 % 4
    SC[4:8, :] = jnp.where(l4 < 2, jnp.where(l4 == 0, b3[0], b3[1]), jnp.where(l4 == 2, b3[2], b3[3]))
    wait_c = send_all(SC, r["RC"], 19)

    from_group(22, GB, xn - 1)
    GB[ixx] = SB[...]
    main = zero
    edges = [zero] * 5
    for k in range(xn):
        v = GB[k]
        for h in range(2):
            if xn == 8 and h == 1:
                continue
            shift = 8 * k - 16 + h * (8 * xn - 64)
            m = roll(v, shift)
            src = (lane - shift + 256) % 128
            if xn != 8:
                m = jnp.where(src // 64 == h, m, 0.0)
            main = main + jnp.where(src % 64 < 40, m, 0.0)
            for dy in range(5):
                a = 40 + 4 * dy
                edges[dy] = edges[dy] + jnp.where((src % 64 >= a) & (src % 64 < a + 4), m, 0.0)
    edge = zero
    for dy in range(5):
        edge = edge + roll(edges[dy], 4 * dy - 40)
    SZ[0] = main
    SZ[1] = edge
    to_group(23, SZ, GC.at[iz], group_z)

    run(wait_c)
    unpack2(r["RC"], SC, G2)
    c, t = nsum(G2, 2, 8, 6, 8, 2)
    V2[2:10, 6:14, :] = S * (1.2 * c + S * t) * rowmask(6, 8, 8, 12)
    xmask(V2, 4, 8, 2, 8, 6, 8)

    TB, TC, RC = r["TB"], r["TC"], r["RC"]
    for dy in (-1, 0, 1):
        acc = jnp.zeros((4, 128), F32)
        for dx in (-1, 0, 1):
            m0, lo, hi = (keep(piece(RC, SC, slice(4, 8), (dx, dy, dz)), dx, dy, dz) for dz in (0, -1, 1))
            e = jnp.where((lane4 >= 92) & (lane4 < 100), lo, jnp.where((lane4 >= 28) & (lane4 < 36), hi, 0.0))
            q = m0 + roll(e, 64)
            if dx < 0:
                q = jnp.where(l4 < 2, roll(q, -2), 0.0)
            if dx > 0:
                q = jnp.where(l4 >= 2, roll(q, 2), 0.0)
            acc = acc + q
        TB[dy + 1] = acc
    TC[0:2, :] = TB[1, 0:2, :] + TB[0, 2:4, :]
    TC[2:4, :] = TB[1, 2:4, :] + TB[2, 0:2, :]
    for i in range(4):
        v = roll(jnp.where(l4 == i, TC[...], 0.0), -i)
        v = v + roll(v, 1)
        v = v + roll(v, 2)
        G3[4 + i, 11:15, :] = v * inverse(W3[4 + i, 11:15, :])
    c, t = nsum(G3, 5, 2, 12, 2, 4)
    v3 = jnp.where(own1[0:2], S * (1.2 * c + S * t), 0.0)
    SE, SV, RE, RV = r["SE"], r["SV"], r["RE"], r["RV"]
    SV[...] = pack3(v3)
    wait_v = send_all(SV, RV, 26)

    def drain(key, slots, count, sizes):
        for n in sizes:

            @pl.when(count == n)
            def _():
                copy(slots(n), slots(n), key, right).wait_send()

    early = len(sent) - 1
    for item in sent[:early]:
        drain(*item)

    from_group(23, GC, nz - 1)
    GC[iz, 0] = SZ[0]
    GC[iz, 1] = SZ[1]
    acc = [zero] * 4
    for z in range(nz):
        v = GC[z, 0]
        if z + 1 < nz:
            v = v + jnp.where(lane % 8 >= 6, roll(GC[z + 1, 1], 6), 0.0)
        if z > 0:
            v = v + jnp.where(lane % 8 < 2, roll(GC[z - 1, 1], -2), 0.0)
        for x in range(nx):
            acc[x % 4] = acc[x % 4] + cp[x * nz + z] * v[x : x + 1, :]
    acc = (acc[0] + acc[1]) + (acc[2] + acc[3])
    tot = jnp.sum(acc, axis=1, keepdims=True)
    e4 = jnp.sum(jnp.where((lane >= 32 + 8 * row) & (lane < 40 + 8 * row), tot, 0.0), axis=0, keepdims=True)
    SE[...] = e4
    wait_e = send_all(SE, RE, 20)
    run(wait_v)

    near = [(a, b) for a in (-1, 0, 1) for b in (-1, 0, 1)]
    unpack3(lambda o: SV[...] if o == (0, 0, 0) else RV[SLOT[o]], near, V3)
    run(wait_e)
    l1 = lane[0:1]
    par = []
    for dx in (-1, 0, 1):
        v = zero
        for dy in (-1, 0, 1):
            o = (dx, dy, 0)
            own = SE[...] if o == (0, 0, 0) else keep(RE[SLOT[o], 0:1, :], *o)
            lo, hi = (keep(RE[SLOT[(dx, dy, dz)], 0:1, :], dx, dy, dz) for dz in (-1, 1))
            e = jnp.where((l1 >= 32) & (l1 < 96), own, roll(jnp.where(l1 < 64, hi, lo), 64))
            y = 4 + 2 * dy
            v = jnp.where((row == y) | (row == y + 1), e, v)
        par.append(v)
    for i in range(6):
        U3[3 + i, 8:16, :] = V3[3 + i, 8:16, :] + W3[3 + i, 8:16, :] * par[i // 2]
    c, t = nsum(U3, 4, 4, 8, 8, 4)
    E3 = r["E3"]
    E3[...] = (0.2 * c + S * (G3[4:8, 8:16, :] + t)) * inverse(W3[4:8, 8:16, :])
    F2 = r["F2"]
    F2[:, pl.ds(0, 4, stride=2), :] = E3[:, 3:7, :]
    F2[:, pl.ds(1, 4, stride=2), :] = E3[:, 3:7, :]
    for i in range(8):
        U2[2 + i, 6:14, :] = V2[2 + i, 6:14, :] + W2[2 + i, 6:14, :] * F2[i // 2]
    c, t = nsum(U2, 3, 6, 6, 8, 2)
    E2 = r["E2"]
    E2[...] = (0.2 * c + S * (G2[3:9, 6:14, :] + t)) * inverse(W2[3:9, 6:14, :])
    F1 = r["F1"]
    F1[:, pl.ds(2, 6, stride=2), :] = E2[:, 1:7, :]
    F1[:, pl.ds(3, 6, stride=2), :] = E2[:, 1:7, :]
    for i in range(12):
        U1[1 + i, 6:18, :] = V1[1 + i, 6:18, :] + W1[1 + i, 6:18, :] * F1[i // 2, 2:14, :]
    E1 = r["E1"]
    for at in (7, 9):
        c, t = nsum(U1, 2, 10, at, 8, 1)
        E1[:, at - 7 : at + 1, :] = (0.2 * c + S * (G1[2:12, at : at + 8, :] + t)) * inverse(W1[2:12, at : at + 8, :])
    o = select_dot(E1[...].reshape(160, 128), up).reshape(10, 16, 128)
    F0 = r["F0"]
    O1 = r["O1"]
    O1[...] = o
    F0[:, pl.ds(6, 10, stride=2), :] = O1[:, 0:10, :]
    F0[:, pl.ds(7, 10, stride=2), :] = O1[:, 0:10, :]
    acc = zero
    for x in range(8):
        e = E1[x + 1, 1:9, :]
        for p in range(2):
            base = 6 * (2 * x + p + 2)
            acc = jnp.where(lane == base + 3, roll(e, base + 3 - 31), acc)
            acc = jnp.where(lane == base + 2, roll(e, base + 2 - 96), acc)
    UQ = r["UQ"]
    FQ = r["FQ"]
    FQ[...] = acc
    UQ[pl.ds(8, 8, stride=2), :] = FQ[...]
    UQ[pl.ds(9, 8, stride=2), :] = FQ[...]
    UQ[8:24, :] = VQ[8:24, :] + r["WQ"][8:24, :] * UQ[8:24, :]
    for i in range(18):
        V0[1 + i, 7:25, :] = V0[1 + i, 7:25, :] + W0[1 + i, 7:25, :] * F0[(i + 1) // 2, 7:25, :]
    inject(UQ, range(2, 18), (8, 16))
    for at in (8, 16):
        c, t = sum0(V0, 2, 16, at)
        out_ref[:, at - 8 : at, :] = 0.2 * c + S * (G0[2:18, at : at + 8, :] + t)

    for item in sent[early:]:
        drain(*item)
    for key, buf, n in ((21, GA, n_y - 1), (22, GB, xn - 1), (23, GC, nz - 1)):
        copy(buf.at[pl.ds(0, n)], buf.at[pl.ds(0, n)], key, right).wait_send()


def scratch(dims):
    nx, ny, nz = dims
    xn = ny // 2
    v = {
        "B0": (1, 16, 16, 128), "A0": (16, 16, 128), "CM": (8, nx * ny * nz * 8),
        "G0": (20, 32, 128), "W0": (20, 32, 128), "V0": (20, 32, 128), "INJ": (20, 32, 128),
        "GQ": (32, 128), "VQ": (32, 128), "WQ": (32, 128), "UQ": (32, 128),
        "YS": (2, 16, 2, 128), "RY": (2, 16, 2, 128), "RXY": (4, 2, 128),
        "QS": (16, 128), "QW": (16, 128), "RQ": (6, 16, 128), "QE": (2, 1, 128), "RQE": (4, 1, 128),
        "YW": (2, 16, 1, 128), "RYW": (2, 16, 1, 128), "RQW": (2, 16, 128),
        "C0": (8, 16, 128), "C1": (4, 8, 128), "C2": (4, 8, 128),
        "SW2": (4, 128), "SW3": (2, 128), "RW2": (26, 4, 128),
        "RW3": (26, 2, 128), "RW3X": (18, 2, 128), "RW3Y": (18, 2, 128), "C3": (6, 16, 128),
        "A1": (14, 24, 128), "Q1": (14, 24, 128), "R2": (12, 24, 128), "PT": (12, 24, 128), "QT": (12, 24, 128),
        "G1": (14, 24, 128), "W1": (14, 24, 128), "V1": (14, 24, 128), "U1": (14, 24, 128),
        "G2": (12, 24, 128), "W2": (12, 24, 128), "V2": (12, 24, 128), "U2": (12, 24, 128),
        "P2": (12, 24, 128), "Q2": (12, 24, 128),
        "G3": (12, 24, 128), "W3": (12, 24, 128), "V3": (12, 24, 128), "U3": (12, 24, 128), "P3": (12, 24, 128), "Q3": (12, 24, 128),
        "T4": (5, 24, 128),
        "SC": (8, 128), "RC": (26, 8, 128), "TB": (3, 4, 128), "TC": (4, 128), "SE": (1, 128), "RE": (26, 1, 128), "SV": (2, 128), "RV": (26, 2, 128),
        "SA": (4, 128), "SB": (8, 128), "SZ": (2, 8, 128),
        "GA": (2 * nx, 4, 128), "GB": (xn, 8, 128), "GC": (nz, 2, 8, 128), "CP": (nx * nz, 8, 128),
        "E3": (4, 8, 128), "F2": (4, 8, 128), "E2": (6, 8, 128), "F1": (6, 16, 128),
        "E1": (10, 16, 128), "O1": (10, 16, 128), "F0": (10, 32, 128), "FQ": (8, 128),
    }
    n = "g"
    v["S1" + n] = (8, 8, 128)
    v["YS1" + n] = (2, 8, 4, 128)
    v["ZS1" + n] = (8, 128)
    v["RX1" + n] = (2, 3, 8, 128)
    v["RY1" + n] = (2, 8, 4, 128)
    v["RXY1" + n] = (4, 3, 4, 128)
    v["RZ1" + n] = (18, 8, 128)
    n = "w"
    v["S1" + n] = (8, 8, 128)
    v["YS1" + n] = (2, 8, 2, 128)
    v["ZS1" + n] = (8, 128)
    v["YZ1" + n] = (2, 2, 128)
    v["RX1" + n] = (2, 2, 8, 128)
    v["RY1" + n] = (2, 8, 2, 128)
    v["RXY1" + n] = (4, 2, 128)
    v["RZ1" + n] = (6, 8, 128)
    v["RYZ1" + n] = (4, 2, 128)
    return v


def solution(mesh):
    dims = tuple(mesh.shape[a] for a in ("gx", "gy", "gz"))
    sizes = scratch(dims)

    def body(*args):
        names = ["b", "w", "c", "out"] + list(sizes) + ["ssem", "rsem", "lsem"]
        kernel(dims, dict(zip(names, args)))

    def per_device(sources, stiffness, coarse_inverse):
        vmem = pl.BlockSpec(memory_space=pltpu.VMEM)
        e = pl.pallas_call(
            body,
            out_shape=jax.ShapeDtypeStruct((16, 16, 128), F32),
            in_specs=[pl.BlockSpec(memory_space=pltpu.HBM)] * 3,
            out_specs=vmem,
            scratch_shapes=[pltpu.VMEM(s, F32) for s in sizes.values()] + [pltpu.SemaphoreType.DMA((28,))] * 2 + [pltpu.SemaphoreType.DMA((3,))],
            compiler_params=pltpu.CompilerParams(collective_id=0, has_side_effects=True, vmem_limit_bytes=24 * 2**20),
            name="vcycle",
        )(*[pltpu.with_memory_space_constraint(a, pltpu.HBM) for a in (sources, stiffness, coarse_inverse)])
        return (e / stiffness)[None]

    return jax.shard_map(
        per_device,
        mesh=mesh,
        in_specs=(P(None, "gx", "gy", "gz"), P("gx", "gy", "gz"), P(("gx", "gy", "gz"), None)),
        out_specs=P(None, "gx", "gy", "gz"),
        check_vma=False,
    )
```

```python
import functools
import itertools

import jax
import jax.numpy as jnp
from jax import lax
from jax.experimental import pallas as pl
from jax.experimental.pallas import tpu as pltpu
from jax.sharding import PartitionSpec as P

MESH = pl.DeviceIdType.MESH
F32 = jnp.float32
S = 0.8 / 6.0
OFFS = [o for o in itertools.product((-1, 0, 1), repeat=3) if o != (0, 0, 0)]
OFFS.sort(key=lambda o: (-abs(o[1]), -abs(o[2]), -abs(o[0])))
OFF2X = [(2 * a, b, 0) for a in (-1, 1) for b in (-1, 0, 1)]
OFF2Y = [(b, 2 * a, 0) for a in (-1, 1) for b in (-1, 0, 1)]
FLAT = [o for o in OFFS if o[2] == 0]
SLOT = {o: i for i, o in enumerate(OFFS)}
ZOFFS = [o for o in OFFS if o[2] != 0]
ZSLOT = {o: i for i, o in enumerate(ZOFFS)}
ZY = [o for o in ZOFFS if o[1] != 0]
XY = [(-1, -1), (-1, 1), (1, -1), (1, 1)]
XZ = [(0, -1), (0, 1)] + XY


def neg(o):
    return tuple(-v for v in o)


def roll(v, shift):
    shift = shift % 128
    return v if shift == 0 else pltpu.roll(v, shift, v.ndim - 1)


def split2(v):
    hi = v.astype(jnp.bfloat16)
    lo = (v - hi.astype(F32)).astype(jnp.bfloat16)
    return jnp.concatenate([hi, lo], axis=1)


def select_dot(v, sel):
    return jnp.dot(split2(v), sel, preferred_element_type=F32)


def kernel(dims, refs):
    nx, ny, nz = dims
    xn = ny // 2
    n_y = nx * 2
    r = refs
    ix, iy, iz = lax.axis_index("gx"), lax.axis_index("gy"), lax.axis_index("gz")
    ih, ixx = iy // xn, iy % xn

    def dev(dx, dy, dz):
        return {
            "gx": lax.rem(ix + dx + nx, nx),
            "gy": lax.rem(iy + dy + ny, ny),
            "gz": lax.rem(iz + dz + nz, nz),
        }

    def copy(src, dst, key, device):
        return pltpu.make_async_remote_copy(
            src_ref=src,
            dst_ref=dst,
            send_sem=r["ssem"].at[key],
            recv_sem=r["rsem"].at[key],
            device_id=device,
            device_id_type=MESH,
        )

    cx = {-2: ix > 1, -1: ix > 0, 1: ix < nx - 1, 2: ix < nx - 2}
    cy = {-2: iy > 1, -1: iy > 0, 1: iy < ny - 1, 2: iy < ny - 2}
    cz = {-1: iz > 0, 1: iz < nz - 1}

    def has(o):
        c = [f[v] for f, v in zip((cx, cy, cz), o) if v]
        return functools.reduce(jnp.logical_and, c)

    def keep(v, *o):
        return jnp.where(has(o), v, 0.0) if any(o) else v

    sent = []

    def round_of(key, items, slots):
        for o, src, dst in items:

            @pl.when(has(o))
            def _():
                copy(src, dst, key, dev(*o)).start()

        offs = [o for o, _, _ in items]
        count = sum(jnp.where(has(o), 1, 0) for o in offs)
        spots = [sorted({0, 1, 2, n - 3, n - 2, n - 1} & set(range(n))) for n in dims]
        sizes = {sum(all(0 <= v + p < n for v, p, n in zip(o, at, dims)) for o in offs) for at in itertools.product(*spots)}
        sizes = sorted(n for n in sizes if n)
        sent.append((key, slots, count, sizes))

        def wait():
            for n in sizes:

                @pl.when(count == n)
                def _():
                    copy(slots(n), slots(n), key, right).wait_recv()

        return wait

    def first(ref):
        return lambda n: ref.at[pl.ds(0, n)]

    def to_group(key, src, dst, group):
        for d in group:
            copy(src, dst, key, d).start()

    def from_group(key, buf, n):
        copy(buf.at[pl.ds(0, n)], buf.at[pl.ds(0, n)], key, right).wait_recv()

    def run(waits):
        for w in waits:
            w()

    me = {"gx": ix, "gy": iy, "gz": iz}
    right = {"gx": lax.rem(ix + 1, nx), "gy": iy, "gz": iz}

    group_y = []
    for k in range(1, n_y):
        t = lax.rem(ih * nx + ix + k, n_y)
        group_y.append({"gx": t % nx, "gy": (t // nx) * xn + ixx, "gz": iz})
    group_x = [{"gx": ix, "gy": ih * xn + lax.rem(ixx + k, xn), "gz": iz} for k in range(1, xn)]
    group_z = [{"gx": ix, "gy": iy, "gz": lax.rem(iz + k, nz)} for k in range(1, nz)]

    barrier = pltpu.get_barrier_semaphore()
    loads = [pltpu.make_async_copy(r[a], r[b], r["lsem"].at[i]) for i, (a, b) in enumerate((("b", "B0"), ("w", "A0"), ("c", "CM")))]
    for c in loads:
        c.start()
    for d in group_x + group_y + group_z:
        pl.semaphore_signal(barrier, inc=1, device_id=d, device_id_type=MESH)

    for o in OFFS + OFF2Y + OFF2X:

        @pl.when(has(o))
        def _():
            pl.semaphore_signal(barrier, inc=1, device_id=dev(*o), device_id_type=MESH)

    partners = sum(jnp.where(has(o), 1, 0) for o in OFFS + OFF2X + OFF2Y) + len(group_y + group_x + group_z)

    lane = lax.broadcasted_iota(jnp.int32, (8, 128), 1)
    row = lax.broadcasted_iota(jnp.int32, (8, 128), 0)
    zero = jnp.zeros((8, 128), F32)

    def flag(c):
        return jnp.where(c, jnp.float32(1), jnp.float32(0))

    mx = {-1: flag(ix > 0), 0: jnp.float32(1), 1: flag(ix < nx - 1)}
    my = {-1: flag(iy > 0), 0: jnp.float32(1), 1: flag(iy < ny - 1)}
    mz = {-1: flag(iz > 0), 0: jnp.float32(1), 1: flag(iz < nz - 1)}

    b_ref, w_ref, c_ref, out_ref = r["B0"], r["A0"], r["CM"], r["out"]

    G0, W0, V0 = r["G0"], r["W0"], r["V0"]
    loads[0].wait()
    loads[1].wait()
    w0 = w_ref[...]
    g0 = b_ref[0] / w0
    W0[2:18, 8:24, :] = w0
    G0[2:18, 8:24, :] = g0

    r["YS"][0] = G0[2:18, 8:10, :]
    r["YS"][1] = G0[2:18, 22:24, :]

    def pack_q(src, dst):
        for h in range(2):
            acc = zero
            for x in range(16):
                m = src[x + 2, 8 + 8 * h : 16 + 8 * h, :]
                base = 6 * (x + 2)
                acc = jnp.where(lane == base, roll(m, base - 1), acc)
                acc = jnp.where((lane >= base + 1) & (lane < base + 3), roll(m, base + 1 - 127), acc)
                acc = jnp.where((lane >= base + 3) & (lane < base + 5), roll(m, base + 3 - 127), acc)
                acc = jnp.where(lane == base + 5, roll(m, base + 5 - 126), acc)
            dst[8 * h : 8 * h + 8, :] = acc

    pack_q(G0, r["QS"])
    r["QE"][0] = r["QS"][0:1, :]
    r["QE"][1] = r["QS"][15:16, :]

    for name in ("G0", "W0", "V0"):
        a = r[name]
        a[:, 0:8, :] = jnp.zeros((20, 8, 128), F32)
        a[:, 24:32, :] = jnp.zeros((20, 8, 128), F32)
    for name in ("GQ", "WQ", "VQ", "UQ", "G1", "W1", "V1", "U1", "G2", "W2", "V2", "U2", "P2", "Q2", "G3", "W3", "V3", "U3", "P3", "T4", "A1", "Q1", "R2", "PT", "QT", "Q3"):
        r[name][...] = jnp.zeros(r[name].shape, F32)

    zr = lax.broadcasted_iota(jnp.int32, (256, 128), 0) % 128
    zc = lax.broadcasted_iota(jnp.int32, (256, 128), 1)
    down = jnp.where(zc == 32 + zr // 2, jnp.float32(1), jnp.float32(0)).astype(jnp.bfloat16)
    up = jnp.where(zr == 32 + zc // 2, jnp.float32(1), jnp.float32(0)).astype(jnp.bfloat16)

    C0 = r["C0"]

    def coarsen0(values, scale):
        C0[...] = jnp.sum(values.reshape(8, 2, 16, 128), axis=1)
        t = C0[:, pl.ds(0, 8, stride=2), :] + C0[:, pl.ds(1, 8, stride=2), :]
        return (select_dot(t.reshape(64, 128), down) * scale).reshape(8, 8, 128)

    def pair_z(t, dil):
        ln = lax.broadcasted_iota(jnp.int32, t.shape, t.ndim - 1)
        return t + jnp.where((ln // dil) % 2 == 0, roll(t, -dil), roll(t, dil))

    C1, C2 = r["C1"], r["C2"]

    def coarsen1(values, scale):
        n = values.shape[0] // 2
        C1[...] = jnp.sum(values.reshape(n, 2, 8, 128), axis=1)
        t = C1[:, pl.ds(0, 4, stride=2), :] + C1[:, pl.ds(1, 4, stride=2), :]
        return pair_z(t, 1) * scale

    w1 = coarsen0(w0, 0.0625)
    own1 = (lane >= 32) & (lane < 96)
    w2 = coarsen1(w1, 0.0625)
    C2[0:4, 0:4, :] = w2
    t = C2[0:4, pl.ds(0, 2, stride=2), :] + C2[0:4, pl.ds(1, 2, stride=2), :]
    w3 = pair_z(jnp.sum(t.reshape(2, 2, 2, 128), axis=1), 2) * 0.0625

    lane4 = lane[0:4]

    def pack2(v):
        halves = []
        for h in range(2):
            a = jnp.where(lane4 % 2 == 0, v[2 * h], v[2 * h + 1])
            halves.append(roll(a, -32 if h == 0 else 32))
        return jnp.where(lane4 < 64, halves[0], halves[1])

    def pack3(v):
        return jnp.where(lane[0:2] < 64, roll(v[0], -32), roll(v[1], 32))

    SW2, SW3 = r["SW2"], r["SW3"]
    p2 = pack2(w2)
    SW2[...] = p2
    SW3[...] = pack3(w3)
    zp = jnp.zeros((4, 128), F32)
    for h in range(2):
        zp = jnp.where((lane4 >= 16 * h) & (lane4 < 16 * h + 8), roll(p2, -48 * h), zp)
        zp = jnp.where((lane4 >= 16 * h + 8) & (lane4 < 16 * h + 16), roll(p2, -48 * h - 48), zp)
    row4 = row[0:4]
    SWZ = r["SWZ"]
    SWZ[...] = sum(roll(jnp.sum(jnp.where(row4 == y, zp, 0.0), axis=0, keepdims=True), 32 * y) for y in range(4))

    def send_all(src, dst, key):
        return [round_of(key, [(o, src, dst.at[SLOT[neg(o)]]) for o in OFFS], first(dst))]

    def pack_z1(own, zs):
        acc = zero
        for x in range(8):
            acc = jnp.where((lane >= 16 * x) & (lane < 16 * x + 4), roll(own[x], 16 * x - 32), acc)
            acc = jnp.where((lane >= 16 * x + 4) & (lane < 16 * x + 8), roll(own[x], 16 * x + 4 - 92), acc)
        zs[...] = acc

    def place(m0, c, l, h):
        a = roll(m0, 32 if h == 0 else 96)
        e = roll(c, 96 if h == 0 else 32)
        return jnp.where((l >= 32) & (l < 96), a, e)

    s1w, ysw, zsw, yzw = r["S1w"], r["YS1w"], r["ZS1w"], r["YZ1w"]
    s1w[...] = w1
    ysw[0] = s1w[:, 0:2, :]
    ysw[1] = s1w[:, 6:8, :]
    pack_z1(w1, zsw)
    yzw[0] = zsw[0:2, :]
    yzw[1] = zsw[6:8, :]
    RX, RY, RXY, RZ, RYZ = (r[name + "w"] for name in ("RX1", "RY1", "RXY1", "RZ1", "RYZ1"))
    r["YW"][0] = W0[2:18, 8:9, :]
    r["YW"][1] = W0[2:18, 23:24, :]
    pack_q(W0, r["QW"])

    pl.semaphore_wait(barrier, partners)

    gsl = pl.ds(8, 16)
    wait_g0 = [
        round_of(1, [((0, d, 0), r["YS"].at[i], r["RY"].at[1 - i]) for i, d in enumerate((-1, 1))], first(r["RY"])),
        round_of(
            2,
            [
                ((dx, dy, 0), r["YS"].at[(dy + 1) // 2, 0 if dx < 0 else 15], r["RXY"].at[XY.index((-dx, -dy))])
                for dx, dy in XY
            ],
            first(r["RXY"]),
        ),
        round_of(
            4,
            [((0, dy, dz), r["QE"].at[(dy + 1) // 2], r["RQE"].at[XY.index((-dy, -dz))]) for dy, dz in XY],
            first(r["RQE"]),
        ),
        round_of(3, [((dx, 0, dz), r["QS"], r["RQ"].at[XZ.index((-dx, -dz))]) for dx, dz in XZ], first(r["RQ"])),
        round_of(
            0,
            [
                ((-1, 0, 0), G0.at[pl.ds(2, 2), gsl], G0.at[pl.ds(18, 2), gsl]),
                ((1, 0, 0), G0.at[pl.ds(16, 2), gsl], G0.at[pl.ds(0, 2), gsl]),
            ],
            lambda n: G0.at[pl.ds(0, 2 * n), gsl],
        ),
    ]

    wait_z = round_of(28, [((0, 0, d), SW3, r["RW3"].at[1 - i]) for i, d in enumerate((-1, 1))], first(r["RW3"]))
    wait_w = [
        round_of(7, [((0, -1, 0), ysw.at[0], RY.at[1]), ((0, 1, 0), ysw.at[1], RY.at[0])], first(RY)),
        round_of(
            8,
            [
                ((dx, dy, 0), ysw.at[(dy + 1) // 2, 0 if dx < 0 else 7], RXY.at[XY.index((-dx, -dy))])
                for dx, dy in XY
            ],
            first(RXY),
        ),
        round_of(
            27,
            [((0, dy, dz), yzw.at[(dy + 1) // 2], RYZ.at[XY.index((-dy, -dz))]) for dy, dz in XY],
            first(RYZ),
        ),
        round_of(5, [(o, SW2, r["RW2"].at[FLAT.index(neg(o))]) for o in FLAT], first(r["RW2"])),
        round_of(17, [(o, SWZ, r["RWZ"].at[ZSLOT[neg(o)]]) for o in ZOFFS], first(r["RWZ"])),
        round_of(6, [((-1, 0, 0), s1w.at[pl.ds(0, 2)], RX.at[1]), ((1, 0, 0), s1w.at[pl.ds(6, 2)], RX.at[0])], first(RX)),
        round_of(9, [((dx, 0, dz), zsw, RZ.at[XZ.index((-dx, -dz))]) for dx, dz in XZ], first(RZ)),
    ]

    def recv1w(dst):
        for x in range(1, 13):
            dx = -1 if x < 3 else (1 if x > 10 else 0)
            sx = x - 3 if dx == 0 else (x + 5 if dx < 0 else x - 11)

            def ends(v, ln, lo, hi, dx, dy):
                v = jnp.where((ln >= 28) & (ln < 32), keep(roll(lo, 28 - 16 * sx - 4), dx, dy, -1), v)
                return jnp.where((ln >= 96) & (ln < 100), keep(roll(hi, 96 - 16 * sx), dx, dy, 1), v)

            base = w1[x - 3] if dx == 0 else keep(RX[(dx + 1) // 2, x - 1 if dx < 0 else x - 11], dx, 0, 0)
            lo, hi = (RZ[XZ.index((dx, dz))] for dz in (-1, 1))
            dst[x, 8:16, :] = ends(base, lane, lo, hi, dx, 0)
            for dy, at in ((-1, 6), (1, 16)):
                if dx == 0:
                    lo, hi = (RYZ[XY.index((dy, dz))] for dz in (-1, 1))
                    v = keep(RY[(dy + 1) // 2, x - 3], 0, dy, 0)
                    dst[x, at : at + 2, :] = ends(v, lane[0:2], lo, hi, 0, dy)
                elif x in (2, 11):
                    dst[x, at : at + 2, :] = keep(RXY[XY.index((dx, dy))], dx, dy, 0)

    def send1(own, n, key):
        s1, ys, zs = r["S1" + n], r["YS1" + n], r["ZS1" + n]
        s1[...] = own
        for q in range(4):
            v = jnp.where(lane < 64, roll(own[2 * q], -32), roll(own[2 * q + 1], 32))
            ys[0, q] = v[0:4]
            ys[1, q] = v[4:8]
        pack_z1(own, zs)
        zy = r["ZY1g"]
        zy[0] = zs[0:4, :]
        zy[1] = zs[4:8, :]
        rx, ry, rxy, rz, rzy = (r[name + n] for name in ("RX1", "RY1", "RXY1", "RZ1", "RZY1"))
        return [
            round_of(key + 1, [((0, -1, 0), ys.at[0], ry.at[1]), ((0, 1, 0), ys.at[1], ry.at[0])], first(ry)),
            round_of(
                key + 2,
                [
                    ((dx, dy, 0), ys.at[(dy + 1) // 2, 0 if dx < 0 else 3], rxy.at[XY.index((-dx, -dy))])
                    for dx, dy in XY
                ],
                first(rxy),
            ),
            round_of(29, [(o, zy.at[(o[1] + 1) // 2], rzy.at[ZY.index(neg(o))]) for o in ZY], first(rzy)),
            round_of(
                key,
                [((-1, 0, 0), s1.at[pl.ds(0, 3)], rx.at[1]), ((1, 0, 0), s1.at[pl.ds(5, 3)], rx.at[0])],
                first(rx),
            ),
            round_of(key + 3, [((dx, 0, dz), zs, rz.at[XZ.index((-dx, -dz))]) for dx, dz in XZ], first(rz)),
        ]

    def half(m, q):
        return jnp.where((lane4 >= 32) & (lane4 < 96), roll(m, 32 if q == 0 else 96), 0.0)

    def recv1(own, n, key, dst):
        run(key)
        for x in range(14):
            dx = -1 if x < 3 else (1 if x > 10 else 0)
            for dy in (-1, 0, 1):
                if dx == 0 and dy == 0:
                    base = own[x - 3]
                elif dy == 0:
                    base = r["RX1" + n][(dx + 1) // 2, x if dx < 0 else x - 11]
                elif dx == 0:
                    base = half(r["RY1" + n][(dy + 1) // 2, (x - 3) // 2], (x - 3) % 2)
                elif x in (0, 13):
                    base = jnp.zeros((4, 128), F32)
                else:
                    base = half(r["RXY1" + n][XY.index((dx, dy))], (x - 1 if dx < 0 else x - 11) % 2)
                sx = x - 3 if dx == 0 else (x + 5 if dx < 0 else x - 11)
                if dy == 0:
                    lo, hi = (r["RZ1" + n][XZ.index((dx, dz))] for dz in (-1, 1))
                else:
                    lo, hi = (r["RZY1" + n][ZY.index((dx, dy, dz))] for dz in (-1, 1))
                ln = lane[0:8] if dy == 0 else lane4
                v = keep(base, dx, dy, 0)
                v = jnp.where((ln >= 28) & (ln < 32), keep(roll(lo, 28 - 16 * sx - 4), dx, dy, -1), v)
                v = jnp.where((ln >= 96) & (ln < 100), keep(roll(hi, 96 - 16 * sx), dx, dy, 1), v)
                at = 8 if dy == 0 else (4 if dy < 0 else 16)
                dst[x, at : at + (8 if dy == 0 else 4), :] = v

    wait_z()
    l2, l1 = lane[0:2], lane[0:1]
    ends3 = jnp.where((l2 // 32) % 2 == 1, keep(r["RW3"][0], 0, 0, -1), keep(r["RW3"][1], 0, 0, 1))
    own3 = [place(SW3[...], ends3, l2, h) for h in range(2)]
    XW3 = r["XW3"]
    XW3[...] = jnp.where(
        l1 % 4 < 2,
        jnp.where(l1 % 4 == 0, own3[0][0:1], own3[0][1:2]),
        jnp.where(l1 % 4 == 2, own3[1][0:1], own3[1][1:2]),
    )
    wait_w += [
        round_of(18, [(o, XW3, r["RWF"].at[FLAT.index(neg(o))]) for o in FLAT], first(r["RWF"])),
        round_of(25, [(o, XW3, r["RW3Y"].at[OFF2Y.index(neg(o))]) for o in OFF2Y], first(r["RW3Y"])),
        round_of(24, [(o, XW3, r["RW3X"].at[OFF2X.index(neg(o))]) for o in OFF2X], first(r["RW3X"])),
    ]

    wi1 = 1.0 / jnp.where(own1, w1, 1.0)
    wi2 = 1.0 / jnp.where(own1[0:4], w2, 1.0)

    GQ, VQ = r["GQ"], r["VQ"]
    run(wait_g0)
    G0[0:2, 8:24, :] = keep(G0[0:2, 8:24, :], -1, 0, 0)
    G0[18:20, 8:24, :] = keep(G0[18:20, 8:24, :], 1, 0, 0)
    G0[2:18, 6:8, :] = keep(r["RY"][0], 0, -1, 0)
    G0[2:18, 24:26, :] = keep(r["RY"][1], 0, 1, 0)
    for dx, dy in XY:
        v = keep(r["RXY"][XY.index((dx, dy))], dx, dy, 0)
        G0[1 if dx < 0 else 18, 7 if dy < 0 else 24, :] = v[1 if dy < 0 else 0, :]

    def qj(ln):
        return ln % 6

    for h in range(2):
        sl = slice(8 * h, 8 * h + 8)
        own = r["QS"][sl, :]
        j = qj(lane)
        q = [keep(r["RQ"][i, sl, :], dx, 0, dz) for i, (dx, dz) in enumerate(XZ)]
        v, lo, hi = (
            jnp.where((j == 3) | (j == 5), q[2 * i], jnp.where((j == 0) | (j == 2), q[2 * i + 1], own if i == 0 else 0.0))
            for i in range(3)
        )
        v = jnp.where((lane >= 6) & (lane < 12), roll(lo, 6 - 102), jnp.where((lane >= 108) & (lane < 114), roll(hi, 108 - 12), v))
        GQ[8 + 8 * h : 16 + 8 * h, :] = jnp.where((lane >= 6) & (lane < 114), v, 0.0)
    for dy, at in ((-1, 7), (1, 24)):
        j = qj(lane[0:1])
        lo = keep(r["RQE"][XY.index((dy, -1))], 0, dy, -1)
        hi = keep(r["RQE"][XY.index((dy, 1))], 0, dy, 1)
        v = jnp.where((j == 3) | (j == 5), lo, jnp.where((j == 0) | (j == 2), hi, 0.0))
        GQ[at : at + 1, :] = jnp.where((lane[0:1] >= 12) & (lane[0:1] < 108), v, 0.0)

    INJ = r["INJ"]

    def inject(q, xs, tiles):
        for at in tiles:
            m = q[at : at + 8, :]
            for xp in xs:
                INJ[xp, at : at + 8, :] = jnp.where((lane == 0) | (lane == 127), roll(m, -(6 * xp + 3)), 0.0)

    def sum0(a, x, n, at):
        c = a[x : x + n, at : at + 8, :]
        t = a[x - 1 : x + n - 1, at : at + 8, :] + a[x + 1 : x + n + 1, at : at + 8, :]
        t = t + (a[x : x + n, at - 1 : at + 7, :] + a[x : x + n, at + 1 : at + 9, :])
        z = jnp.where(lane == 0, 0.0, roll(c, 1)) + jnp.where(lane == 127, 0.0, roll(c, -1))
        return c, t + (z + INJ[x : x + n, at : at + 8, :])

    inject(GQ, range(1, 19), (7, 15, 17))
    for at in (7, 15, 17):
        c, t = sum0(G0, 1, 18, at)
        v = S * (1.2 * c + S * t)
        if at == 7:
            v = v * jnp.where(row == 0, my[-1], 1.0)
        if at == 17:
            v = v * jnp.where(row == 7, my[1], 1.0)
        V0[1:19, at : at + 8, :] = v
    V0[1:2, 7:25, :] = V0[1:2, 7:25, :] * mx[-1]
    V0[18:19, 7:25, :] = V0[18:19, 7:25, :] * mx[1]

    for at in (8, 16):
        c = GQ[at : at + 8, :]
        t = jnp.where(qj(lane) == 3, roll(c, -1) + roll(c, -2), roll(c, 1) + roll(c, 2)) + (roll(c, 6) + roll(c, -6))
        t = t + GQ[at - 1 : at + 7, :] + GQ[at + 1 : at + 9, :]
        j = qj(lane)
        mask = jnp.where(j == 3, mz[-1], jnp.where(j == 2, mz[1], 0.0))
        mask = jnp.where((lane >= 12) & (lane < 108), mask, 0.0)
        VQ[at : at + 8, :] = S * (1.2 * c + S * t) * mask

    inject(VQ, range(2, 18), (8, 16))
    halves = []
    for at in (8, 16):
        c, t = sum0(V0, 2, 16, at)
        halves.append(W0[2:18, at : at + 8, :] * (G0[2:18, at : at + 8, :] - 6.0 * c + t))
    r0 = jnp.concatenate(halves, axis=1)
    g1 = jnp.where(own1, coarsen0(r0, 0.125) * wi1, 0.0)
    wait_g1 = send1(g1, "g", 10)

    G1, W1, V1, U1 = r["G1"], r["W1"], r["V1"], r["U1"]
    G2, W2, V2, U2, P2, Q2 = r["G2"], r["W2"], r["V2"], r["U2"], r["P2"], r["Q2"]
    G3, W3, V3, U3, P3 = r["G3"], r["W3"], r["V3"], r["U3"], r["P3"]
    run(wait_w)
    recv1w(W1)

    def spread(m0, lo, hi, l, dx, dy):
        return keep(m0, dx, dy, 0), jnp.where((l // 32) % 2 == 1, keep(lo, dx, dy, -1), keep(hi, dx, dy, 1))

    def piece(buf, own, rows, o):
        return own[rows, :] if o == (0, 0, 0) else buf[SLOT[o], rows, :]

    def unpack2(buf, own, dst):
        rows = slice(0, 4)
        for dx in (-1, 0, 1):
            for dy in (-1, 0, 1):
                m0, c = spread(*[piece(buf, own, rows, (dx, dy, dz)) for dz in (0, -1, 1)], lane4, dx, dy)
                spread2(m0, c, dst, dx, dy)

    def spread2(m0, c, dst, dx, dy):
        for p in range(2):
            take = lane4 % 2 == p
            a = jnp.where(take, m0, roll(m0, 1 if p == 0 else -1))
            e = jnp.where(take, c, roll(c, 1 if p == 0 else -1))
            for h in range(2):
                dst[4 + 4 * dx + 2 * h + p, 8 + 4 * dy : 12 + 4 * dy, :] = place(a, e, lane4, h)

    def unpack3(get, spots, dst):
        l = lane[0:2]
        for dx, dy in spots:
            m0, c = spread(*[get((dx, dy, dz)) for dz in (0, -1, 1)], l, dx, dy)
            for h in range(2):
                dst[5 + 2 * dx + h, 12 + 2 * dy : 14 + 2 * dy, :] = place(m0, c, l, h)

    for dx in (-1, 0, 1):
        for dy in (-1, 0, 1):
            m0 = keep(SW2[...] if dx == dy == 0 else r["RW2"][FLAT.index((dx, dy, 0))], dx, dy, 0)
            lo, hi = (keep(r["RWZ"][ZSLOT[(dx, dy, dz)]], dx, dy, dz) for dz in (-1, 1))
            line = jnp.where(lane[0:1] % 16 >= 8, lo, hi)
            e = jnp.zeros((4, 128), F32)
            for y in range(4):
                e = jnp.where(row4 == y, roll(line, -32 * y), e)
            c = jnp.zeros((4, 128), F32)
            for h in range(2):
                c = jnp.where((lane4 >= 64 * h) & (lane4 < 64 * h + 8), roll(e, 48 * h), c)
                c = jnp.where((lane4 >= 64 * h + 56) & (lane4 < 64 * h + 64), roll(e, 48 * h + 48), c)
            spread2(m0, c, W2, dx, dy)

    W3[5, 12:14, :] = own3[0]
    W3[6, 12:14, :] = own3[1]
    ST, SU = r["ST"], r["SU"]
    spots = [(o, r[n], i) for n, offs in (("RWF", FLAT), ("RW3Y", OFF2Y), ("RW3X", OFF2X)) for i, o in enumerate(offs)]
    for k, (o, buf, i) in enumerate(spots):
        ST[k : k + 1, :] = keep(buf[i], *o)
    for q in range(4):
        t = roll(jnp.where(lax.broadcasted_iota(jnp.int32, (24, 128), 1) % 4 == q, ST[...], 0.0), -q)
        t = t + roll(t, 1)
        SU[q] = t + roll(t, 2)
    for k, ((dx, dy, _), _, _) in enumerate(spots):
        for q in range(4):
            at = 12 + 2 * dy + q % 2
            W3[5 + 2 * dx + q // 2, at : at + 1, :] = SU[q, k : k + 1, :]

    def inverse(w):
        return jnp.where(w > 0.0, 1.0 / jnp.where(w > 0.0, w, 1.0), 0.0)

    def nsum(a, x, n, at, rows, dil):
        c = a[x : x + n, at : at + rows, :]
        t = a[x - 1 : x + n - 1, at : at + rows, :] + a[x + 1 : x + n + 1, at : at + rows, :]
        t = t + (a[x : x + n, at - 1 : at + rows - 1, :] + a[x : x + n, at + 1 : at + rows + 1, :])
        return c, t + (roll(c, dil) + roll(c, -dil))

    def rowmask(at, rows, low, high):
        y = lax.broadcasted_iota(jnp.int32, (rows, 128), 0) + at
        l = lax.broadcasted_iota(jnp.int32, (rows, 128), 1)
        m = jnp.where(y < low, my[-1], jnp.where(y >= high, my[1], 1.0))
        return m * jnp.where(l < 32, mz[-1], jnp.where(l >= 96, mz[1], 1.0))

    def xmask(a, low, high, x, n, at, rows):
        if low > x:
            a[x:low, at : at + rows, :] = a[x:low, at : at + rows, :] * mx[-1]
        if x + n > high:
            a[high : x + n, at : at + rows, :] = a[high : x + n, at : at + rows, :] * mx[1]

    A1, Q1, R2, PT, QT, Q3 = r["A1"], r["Q1"], r["R2"], r["PT"], r["QT"], r["Q3"]
    A1[3:11, 8:16, :] = g1
    for at in (4, 12):
        c, t = nsum(A1, 1, 12, at, 8, 1)
        Q1[1:13, at : at + 8, :] = S * (1.2 * c + S * t) * rowmask(at, 8, 8, 16)
    xmask(Q1, 3, 11, 1, 12, 4, 16)
    C3 = r["C3"]
    for at in (6, 10):
        c, t = nsum(Q1, 1, 12, at, 8, 1)
        res = W1[1:13, at : at + 8, :] * (A1[1:13, at : at + 8, :] - 6.0 * c + t)
        C3[:, at - 6 : at + 2, :] = jnp.sum(res.reshape(6, 2, 8, 128), axis=1)
    t = C3[:, pl.ds(0, 6, stride=2), :] + C3[:, pl.ds(1, 6, stride=2), :]
    P2[3:9, 7:13, :] = pair_z(t, 1) * 0.125 * inverse(W2[3:9, 7:13, :])
    c, t = nsum(P2, 2, 8, 6, 8, 2)
    Q2[2:10, 6:14, :] = S * (1.2 * c + S * t) * rowmask(6, 8, 8, 12)
    xmask(Q2, 4, 8, 2, 8, 6, 8)
    for at in (5, 7):
        c, t = nsum(Q2, 1, 10, at, 8, 2)
        R2[1:11, at : at + 8, :] = W2[1:11, at : at + 8, :] * (P2[1:11, at : at + 8, :] - 6.0 * c + t)
    C3[...] = jnp.sum(R2[:, 4:20, :].reshape(6, 2, 16, 128), axis=1)
    t = C3[:, pl.ds(0, 6, stride=2), :] + C3[:, pl.ds(1, 6, stride=2), :]
    b3 = pair_z(t, 2) * 0.125
    P3[3:9, 10:16, :] = b3 * inverse(W3[3:9, 10:16, :])
    c, t = nsum(P3, 2, 8, 9, 8, 4)
    Q3[2:10, 9:17, :] = S * (1.2 * c + S * t) * rowmask(9, 8, 12, 14)
    xmask(Q3, 5, 7, 2, 8, 9, 8)
    T4 = r["T4"]
    for at in (8, 10):
        c, t = nsum(Q3, 1, 10, at, 8, 4)
        res = W3[1:11, at : at + 8, :] * (P3[1:11, at : at + 8, :] - 6.0 * c + t)
        T4[:, at : at + 8, :] = jnp.sum(res.reshape(5, 2, 8, 128), axis=1)
    t = T4[:, pl.ds(8, 8, stride=2), :] + T4[:, pl.ds(9, 8, stride=2), :]
    patch = pair_z(t, 4) * 0.125

    lines = []
    for dx in range(5):
        v = patch[dx]
        main = zero
        for q in range(4):
            lo = 32 + 16 * q + 7
            main = jnp.where((lane >= 2 * q) & (lane < 2 * q + 2), roll(v, 2 * q - lo), main)
        edge = jnp.where(lane < 2, roll(v, 0 - 23), jnp.where(lane < 4, roll(v, 2 - 103), 0.0))
        line = pltpu.roll(main, 0, 1, stride=8, stride_axis=0) + pltpu.roll(edge, 40, 1, stride=4, stride_axis=0)
        lines.append(jnp.sum(line, axis=0, keepdims=True))
    GA, GB, GC = r["GA"], r["GB"], r["GC"]
    SA, SB, SZ = r["SA"], r["SB"], r["SZ"]
    for p in range(2):
        SA[p : p + 1, :] = lines[2 * p] + roll(lines[2 * p + 1], 64)
    SA[2:3, :] = lines[4]
    SA[3:4, :] = jnp.zeros((1, 128), F32)
    ga_at = ih * nx + ix
    to_group(21, SA, GA.at[ga_at], group_y)

    wait_w0 = [
        round_of(
            14,
            [
                ((-1, 0, 0), W0.at[pl.ds(2, 1), gsl], W0.at[pl.ds(18, 1), gsl]),
                ((1, 0, 0), W0.at[pl.ds(17, 1), gsl], W0.at[pl.ds(1, 1), gsl]),
            ],
            lambda n: W0.at[pl.ds(0, n), gsl],
        ),
        round_of(15, [((0, d, 0), r["YW"].at[i], r["RYW"].at[1 - i]) for i, d in enumerate((-1, 1))], first(r["RYW"])),
        round_of(16, [((0, 0, d), r["QW"], r["RQW"].at[1 - i]) for i, d in enumerate((-1, 1))], first(r["RQW"])),
    ]

    cp = r["CP"]
    loads[2].wait()

    @pl.loop(0, nx)
    def _(x):
        for z in range(nz):
            acc = zero
            for p in range(ny // 2):
                tile = c_ref[:, pl.ds(pl.multiple_of((x * (ny // 2) + p) * 128, 128), 128)]
                for q in range(2):
                    y = 2 * p + q
                    at = 8 * y
                    acc = jnp.where((lane >= at) & (lane < at + 8), roll(tile, at - 64 * q - 8 * z), acc)
            cp[x * nz + z] = acc

    from_group(21, GA, n_y - 1)
    GA[ga_at] = SA[...]
    sums = []
    for h in range(2):
        even, odd = zero, zero
        for p in range(3):
            m = zero
            for g in range(nx):
                m = jnp.where(row == g, GA[h * nx + g, p : p + 1, :], m)
            even = even + (m if p == 1 else pltpu.roll(m, (2 * p - 2) % 8, 0))
            if p < 2:
                odd = odd + pltpu.roll(m, (2 * p - 1) % 8, 0)
        sums.append(jnp.where(lane < 64, even, 0.0) + roll(jnp.where(lane < 64, 0.0, odd), 64))
    SB[...] = sums[0] + roll(sums[1], 64)
    to_group(22, SB, GB.at[ixx], group_x)

    recv1(g1, "g", wait_g1, G1)
    for at in (4, 12):
        c, t = nsum(G1, 1, 12, at, 8, 1)
        V1[1:13, at : at + 8, :] = S * (1.2 * c + S * t) * rowmask(at, 8, 8, 16)
    xmask(V1, 3, 11, 1, 12, 4, 16)
    c, t = nsum(V1, 3, 8, 8, 8, 1)
    r1 = W1[3:11, 8:16, :] * (G1[3:11, 8:16, :] - 6.0 * c + t)
    g2 = jnp.where(own1[0:4], coarsen1(r1, 0.125) * wi2, 0.0)

    PT[4:8, 8:12, :] = g2
    c, t = nsum(PT, 2, 8, 6, 8, 2)
    QT[2:10, 6:14, :] = S * (1.2 * c + S * t) * rowmask(6, 8, 8, 12)
    xmask(QT, 4, 8, 2, 8, 6, 8)
    c, t = nsum(QT, 2, 8, 6, 8, 2)
    res = W2[2:10, 6:14, :] * (PT[2:10, 6:14, :] - 6.0 * c + t)
    C2[...] = jnp.sum(res.reshape(4, 2, 8, 128), axis=1)
    t = C2[:, pl.ds(0, 4, stride=2), :] + C2[:, pl.ds(1, 4, stride=2), :]
    b3 = pair_z(t, 2) * 0.125
    SC = r["SC"]
    SC[0:4, :] = pack2(g2)
    l4 = lane4 % 4
    SC[4:8, :] = jnp.where(l4 < 2, jnp.where(l4 == 0, b3[0], b3[1]), jnp.where(l4 == 2, b3[2], b3[3]))
    wait_c = send_all(SC, r["RC"], 19)

    from_group(22, GB, xn - 1)
    GB[ixx] = SB[...]
    main = zero
    edges = [zero] * 5
    for k in range(xn):
        v = GB[k]
        for h in range(2):
            if xn == 8 and h == 1:
                continue
            shift = 8 * k - 16 + h * (8 * xn - 64)
            m = roll(v, shift)
            src = (lane - shift + 256) % 128
            if xn != 8:
                m = jnp.where(src // 64 == h, m, 0.0)
            main = main + jnp.where(src % 64 < 40, m, 0.0)
            for dy in range(5):
                a = 40 + 4 * dy
                edges[dy] = edges[dy] + jnp.where((src % 64 >= a) & (src % 64 < a + 4), m, 0.0)
    edge = zero
    for dy in range(5):
        edge = edge + roll(edges[dy], 4 * dy - 40)
    SZ[0] = main
    SZ[1] = edge
    to_group(23, SZ, GC.at[iz], group_z)

    run(wait_w0)
    W0[1:2, 8:24, :] = keep(W0[1:2, 8:24, :], -1, 0, 0)
    W0[18:19, 8:24, :] = keep(W0[18:19, 8:24, :], 1, 0, 0)
    W0[2:18, 7:8, :] = keep(r["RYW"][0], 0, -1, 0)
    W0[2:18, 24:25, :] = keep(r["RYW"][1], 0, 1, 0)
    for h in range(2):
        sl = slice(8 * h, 8 * h + 8)
        j = qj(lane)
        v = jnp.where(j == 3, keep(r["RQW"][0, sl, :], 0, 0, -1), jnp.where(j == 2, keep(r["RQW"][1, sl, :], 0, 0, 1), 0.0))
        r["WQ"][8 + 8 * h : 16 + 8 * h, :] = v

    run(wait_c)
    unpack2(r["RC"], SC, G2)
    c, t = nsum(G2, 2, 8, 6, 8, 2)
    V2[2:10, 6:14, :] = S * (1.2 * c + S * t) * rowmask(6, 8, 8, 12)
    xmask(V2, 4, 8, 2, 8, 6, 8)

    TB, TC, RC = r["TB"], r["TC"], r["RC"]
    for dy in (-1, 0, 1):
        acc = jnp.zeros((4, 128), F32)
        for dx in (-1, 0, 1):
            m0, lo, hi = (keep(piece(RC, SC, slice(4, 8), (dx, dy, dz)), dx, dy, dz) for dz in (0, -1, 1))
            e = jnp.where((lane4 >= 92) & (lane4 < 100), lo, jnp.where((lane4 >= 28) & (lane4 < 36), hi, 0.0))
            q = m0 + roll(e, 64)
            if dx < 0:
                q = jnp.where(l4 < 2, roll(q, -2), 0.0)
            if dx > 0:
                q = jnp.where(l4 >= 2, roll(q, 2), 0.0)
            acc = acc + q
        TB[dy + 1] = acc
    TC[0:2, :] = TB[1, 0:2, :] + TB[0, 2:4, :]
    TC[2:4, :] = TB[1, 2:4, :] + TB[2, 0:2, :]
    for i in range(4):
        v = roll(jnp.where(l4 == i, TC[...], 0.0), -i)
        v = v + roll(v, 1)
        v = v + roll(v, 2)
        G3[4 + i, 11:15, :] = v * inverse(W3[4 + i, 11:15, :])
    c, t = nsum(G3, 5, 2, 12, 2, 4)
    v3 = jnp.where(own1[0:2], S * (1.2 * c + S * t), 0.0)
    SE, SV, RE, RV = r["SE"], r["SV"], r["RE"], r["RV"]
    SV[...] = pack3(v3)
    wait_v = send_all(SV, RV, 26)

    def drain(key, slots, count, sizes):
        for n in sizes:

            @pl.when(count == n)
            def _():
                copy(slots(n), slots(n), key, right).wait_send()

    early = len(sent) - 1
    for item in sent[:early]:
        drain(*item)

    from_group(23, GC, nz - 1)
    GC[iz, 0] = SZ[0]
    GC[iz, 1] = SZ[1]
    acc = [zero] * 4
    for z in range(nz):
        v = GC[z, 0]
        if z + 1 < nz:
            v = v + jnp.where(lane % 8 >= 6, roll(GC[z + 1, 1], 6), 0.0)
        if z > 0:
            v = v + jnp.where(lane % 8 < 2, roll(GC[z - 1, 1], -2), 0.0)
        for x in range(nx):
            acc[x % 4] = acc[x % 4] + cp[x * nz + z] * v[x : x + 1, :]
    acc = (acc[0] + acc[1]) + (acc[2] + acc[3])
    tot = jnp.sum(acc, axis=1, keepdims=True)
    e4 = jnp.sum(jnp.where((lane >= 32 + 8 * row) & (lane < 40 + 8 * row), tot, 0.0), axis=0, keepdims=True)
    SE[...] = e4
    wait_e = send_all(SE, RE, 20)
    run(wait_v)

    near = [(a, b) for a in (-1, 0, 1) for b in (-1, 0, 1)]
    unpack3(lambda o: SV[...] if o == (0, 0, 0) else RV[SLOT[o]], near, V3)
    run(wait_e)
    l1 = lane[0:1]
    par = []
    for dx in (-1, 0, 1):
        v = zero
        for dy in (-1, 0, 1):
            o = (dx, dy, 0)
            own = SE[...] if o == (0, 0, 0) else keep(RE[SLOT[o], 0:1, :], *o)
            lo, hi = (keep(RE[SLOT[(dx, dy, dz)], 0:1, :], dx, dy, dz) for dz in (-1, 1))
            e = jnp.where((l1 >= 32) & (l1 < 96), own, roll(jnp.where(l1 < 64, hi, lo), 64))
            y = 4 + 2 * dy
            v = jnp.where((row == y) | (row == y + 1), e, v)
        par.append(v)
    for i in range(6):
        U3[3 + i, 8:16, :] = V3[3 + i, 8:16, :] + W3[3 + i, 8:16, :] * par[i // 2]
    c, t = nsum(U3, 4, 4, 8, 8, 4)
    E3 = r["E3"]
    E3[...] = (0.2 * c + S * (G3[4:8, 8:16, :] + t)) * inverse(W3[4:8, 8:16, :])
    F2 = r["F2"]
    F2[:, pl.ds(0, 4, stride=2), :] = E3[:, 3:7, :]
    F2[:, pl.ds(1, 4, stride=2), :] = E3[:, 3:7, :]
    for i in range(8):
        U2[2 + i, 6:14, :] = V2[2 + i, 6:14, :] + W2[2 + i, 6:14, :] * F2[i // 2]
    c, t = nsum(U2, 3, 6, 6, 8, 2)
    E2 = r["E2"]
    E2[...] = (0.2 * c + S * (G2[3:9, 6:14, :] + t)) * inverse(W2[3:9, 6:14, :])
    F1 = r["F1"]
    F1[:, pl.ds(2, 6, stride=2), :] = E2[:, 1:7, :]
    F1[:, pl.ds(3, 6, stride=2), :] = E2[:, 1:7, :]
    for i in range(12):
        U1[1 + i, 6:18, :] = V1[1 + i, 6:18, :] + W1[1 + i, 6:18, :] * F1[i // 2, 2:14, :]
    E1 = r["E1"]
    for at in (7, 9):
        c, t = nsum(U1, 2, 10, at, 8, 1)
        E1[:, at - 7 : at + 1, :] = (0.2 * c + S * (G1[2:12, at : at + 8, :] + t)) * inverse(W1[2:12, at : at + 8, :])
    o = select_dot(E1[...].reshape(160, 128), up).reshape(10, 16, 128)
    F0 = r["F0"]
    O1 = r["O1"]
    O1[...] = o
    F0[:, pl.ds(6, 10, stride=2), :] = O1[:, 0:10, :]
    F0[:, pl.ds(7, 10, stride=2), :] = O1[:, 0:10, :]
    acc = zero
    for x in range(8):
        e = E1[x + 1, 1:9, :]
        for p in range(2):
            base = 6 * (2 * x + p + 2)
            acc = jnp.where(lane == base + 3, roll(e, base + 3 - 31), acc)
            acc = jnp.where(lane == base + 2, roll(e, base + 2 - 96), acc)
    UQ = r["UQ"]
    FQ = r["FQ"]
    FQ[...] = acc
    UQ[pl.ds(8, 8, stride=2), :] = FQ[...]
    UQ[pl.ds(9, 8, stride=2), :] = FQ[...]
    UQ[8:24, :] = VQ[8:24, :] + r["WQ"][8:24, :] * UQ[8:24, :]
    for i in range(18):
        V0[1 + i, 7:25, :] = V0[1 + i, 7:25, :] + W0[1 + i, 7:25, :] * F0[(i + 1) // 2, 7:25, :]
    inject(UQ, range(2, 18), (8, 16))
    for at in (8, 16):
        c, t = sum0(V0, 2, 16, at)
        out_ref[:, at - 8 : at, :] = 0.2 * c + S * (G0[2:18, at : at + 8, :] + t)

    for item in sent[early:]:
        drain(*item)
    for key, buf, n in ((21, GA, n_y - 1), (22, GB, xn - 1), (23, GC, nz - 1)):
        copy(buf.at[pl.ds(0, n)], buf.at[pl.ds(0, n)], key, right).wait_send()


def scratch(dims):
    nx, ny, nz = dims
    xn = ny // 2
    v = {
        "B0": (1, 16, 16, 128), "A0": (16, 16, 128), "CM": (8, nx * ny * nz * 8),
        "G0": (20, 32, 128), "W0": (20, 32, 128), "V0": (20, 32, 128), "INJ": (20, 32, 128),
        "GQ": (32, 128), "VQ": (32, 128), "WQ": (32, 128), "UQ": (32, 128),
        "YS": (2, 16, 2, 128), "RY": (2, 16, 2, 128), "RXY": (4, 2, 128),
        "QS": (16, 128), "QW": (16, 128), "RQ": (6, 16, 128), "QE": (2, 1, 128), "RQE": (4, 1, 128),
        "YW": (2, 16, 1, 128), "RYW": (2, 16, 1, 128), "RQW": (2, 16, 128),
        "C0": (8, 16, 128), "C1": (4, 8, 128), "C2": (4, 8, 128),
        "SW2": (4, 128), "SW3": (2, 128), "SWZ": (1, 128), "RW2": (8, 4, 128), "RWZ": (18, 1, 128), "XW3": (1, 128),
        "RW3": (2, 2, 128), "RWF": (8, 1, 128), "RW3X": (6, 1, 128), "RW3Y": (6, 1, 128), "ST": (24, 128), "SU": (4, 24, 128), "C3": (6, 16, 128),
        "A1": (14, 24, 128), "Q1": (14, 24, 128), "R2": (12, 24, 128), "PT": (12, 24, 128), "QT": (12, 24, 128),
        "G1": (14, 24, 128), "W1": (14, 24, 128), "V1": (14, 24, 128), "U1": (14, 24, 128),
        "G2": (12, 24, 128), "W2": (12, 24, 128), "V2": (12, 24, 128), "U2": (12, 24, 128),
        "P2": (12, 24, 128), "Q2": (12, 24, 128),
        "G3": (12, 24, 128), "W3": (12, 24, 128), "V3": (12, 24, 128), "U3": (12, 24, 128), "P3": (12, 24, 128), "Q3": (12, 24, 128),
        "T4": (5, 24, 128),
        "SC": (8, 128), "RC": (26, 8, 128), "TB": (3, 4, 128), "TC": (4, 128), "SE": (1, 128), "RE": (26, 1, 128), "SV": (2, 128), "RV": (26, 2, 128),
        "SA": (4, 128), "SB": (8, 128), "SZ": (2, 8, 128),
        "GA": (2 * nx, 4, 128), "GB": (xn, 8, 128), "GC": (nz, 2, 8, 128), "CP": (nx * nz, 8, 128),
        "E3": (4, 8, 128), "F2": (4, 8, 128), "E2": (6, 8, 128), "F1": (6, 16, 128),
        "E1": (10, 16, 128), "O1": (10, 16, 128), "F0": (10, 32, 128), "FQ": (8, 128),
    }
    n = "g"
    v["S1" + n] = (8, 8, 128)
    v["YS1" + n] = (2, 4, 4, 128)
    v["ZS1" + n] = (8, 128)
    v["ZY1" + n] = (2, 4, 128)
    v["RX1" + n] = (2, 3, 8, 128)
    v["RY1" + n] = (2, 4, 4, 128)
    v["RXY1" + n] = (4, 4, 128)
    v["RZ1" + n] = (6, 8, 128)
    v["RZY1" + n] = (12, 4, 128)
    n = "w"
    v["S1" + n] = (8, 8, 128)
    v["YS1" + n] = (2, 8, 2, 128)
    v["ZS1" + n] = (8, 128)
    v["YZ1" + n] = (2, 2, 128)
    v["RX1" + n] = (2, 2, 8, 128)
    v["RY1" + n] = (2, 8, 2, 128)
    v["RXY1" + n] = (4, 2, 128)
    v["RZ1" + n] = (6, 8, 128)
    v["RYZ1" + n] = (4, 2, 128)
    return v


def solution(mesh):
    dims = tuple(mesh.shape[a] for a in ("gx", "gy", "gz"))
    sizes = scratch(dims)

    def body(*args):
        names = ["b", "w", "c", "out"] + list(sizes) + ["ssem", "rsem", "lsem"]
        kernel(dims, dict(zip(names, args)))

    def per_device(sources, stiffness, coarse_inverse):
        vmem = pl.BlockSpec(memory_space=pltpu.VMEM)
        e = pl.pallas_call(
            body,
            out_shape=jax.ShapeDtypeStruct((16, 16, 128), F32),
            in_specs=[pl.BlockSpec(memory_space=pltpu.HBM)] * 3,
            out_specs=vmem,
            scratch_shapes=[pltpu.VMEM(s, F32) for s in sizes.values()] + [pltpu.SemaphoreType.DMA((30,))] * 2 + [pltpu.SemaphoreType.DMA((3,))],
            compiler_params=pltpu.CompilerParams(collective_id=0, has_side_effects=True, vmem_limit_bytes=24 * 2**20),
            name="vcycle",
        )(*[pltpu.with_memory_space_constraint(a, pltpu.HBM) for a in (sources, stiffness, coarse_inverse)])
        return (e / stiffness)[None]

    return jax.shard_map(
        per_device,
        mesh=mesh,
        in_specs=(P(None, "gx", "gy", "gz"), P("gx", "gy", "gz"), P(("gx", "gy", "gz"), None)),
        out_specs=P(None, "gx", "gy", "gz"),
        check_vma=False,
    )
```

```python
import functools
import itertools

import jax
import jax.numpy as jnp
from jax import lax
from jax.experimental import pallas as pl
from jax.experimental.pallas import tpu as pltpu
from jax.sharding import PartitionSpec as P

MESH = pl.DeviceIdType.MESH
F32 = jnp.float32
S = 0.8 / 6.0
OFFS = [o for o in itertools.product((-1, 0, 1), repeat=3) if o != (0, 0, 0)]
OFFS.sort(key=lambda o: (-abs(o[1]), -abs(o[2]), -abs(o[0])))
OFF2X = [(2 * a, b, 0) for a in (-1, 1) for b in (-1, 0, 1)]
OFF2Y = [(b, 2 * a, 0) for a in (-1, 1) for b in (-1, 0, 1)]
FLAT = [o for o in OFFS if o[2] == 0]
SLOT = {o: i for i, o in enumerate(OFFS)}
ZOFFS = [o for o in OFFS if o[2] != 0]
ZSLOT = {o: i for i, o in enumerate(ZOFFS)}
ZY = [o for o in ZOFFS if o[1] != 0]
XY = [(-1, -1), (-1, 1), (1, -1), (1, 1)]
XZ = [(0, -1), (0, 1)] + XY


def neg(o):
    return tuple(-v for v in o)


def roll(v, shift):
    shift = shift % 128
    return v if shift == 0 else pltpu.roll(v, shift, v.ndim - 1)


def split2(v):
    hi = v.astype(jnp.bfloat16)
    lo = (v - hi.astype(F32)).astype(jnp.bfloat16)
    return jnp.concatenate([hi, lo], axis=1)


def select_dot(v, sel):
    return jnp.dot(split2(v), sel, preferred_element_type=F32)


def kernel(dims, refs):
    nx, ny, nz = dims
    xn = ny // 2
    n_y = nx * 2
    r = refs
    ix, iy, iz = lax.axis_index("gx"), lax.axis_index("gy"), lax.axis_index("gz")
    ih, ixx = iy // xn, iy % xn

    def dev(dx, dy, dz):
        return {
            "gx": lax.rem(ix + dx + nx, nx),
            "gy": lax.rem(iy + dy + ny, ny),
            "gz": lax.rem(iz + dz + nz, nz),
        }

    def copy(src, dst, key, device):
        return pltpu.make_async_remote_copy(
            src_ref=src,
            dst_ref=dst,
            send_sem=r["ssem"].at[key],
            recv_sem=r["rsem"].at[key],
            device_id=device,
            device_id_type=MESH,
        )

    cx = {-2: ix > 1, -1: ix > 0, 1: ix < nx - 1, 2: ix < nx - 2}
    cy = {-2: iy > 1, -1: iy > 0, 1: iy < ny - 1, 2: iy < ny - 2}
    cz = {-1: iz > 0, 1: iz < nz - 1}

    def has(o):
        c = [f[v] for f, v in zip((cx, cy, cz), o) if v]
        return functools.reduce(jnp.logical_and, c)

    def keep(v, *o):
        return jnp.where(has(o), v, 0.0) if any(o) else v

    sent = []

    def round_of(key, items, slots):
        for o, src, dst in items:

            @pl.when(has(o))
            def _():
                copy(src, dst, key, dev(*o)).start()

        offs = [o for o, _, _ in items]
        count = sum(jnp.where(has(o), 1, 0) for o in offs)
        spots = [sorted({0, 1, 2, n - 3, n - 2, n - 1} & set(range(n))) for n in dims]
        sizes = {sum(all(0 <= v + p < n for v, p, n in zip(o, at, dims)) for o in offs) for at in itertools.product(*spots)}
        sizes = sorted(n for n in sizes if n)
        sent.append((key, slots, count, sizes))

        def wait():
            for n in sizes:

                @pl.when(count == n)
                def _():
                    copy(slots(n), slots(n), key, right).wait_recv()

        return wait

    def first(ref):
        return lambda n: ref.at[pl.ds(0, n)]

    def to_group(key, src, dst, group):
        for d in group:
            copy(src, dst, key, d).start()

    def from_group(key, buf, n):
        copy(buf.at[pl.ds(0, n)], buf.at[pl.ds(0, n)], key, right).wait_recv()

    def run(waits):
        for w in waits:
            w()

    me = {"gx": ix, "gy": iy, "gz": iz}
    right = {"gx": lax.rem(ix + 1, nx), "gy": iy, "gz": iz}

    group_y = []
    for k in range(1, n_y):
        t = lax.rem(ih * nx + ix + k, n_y)
        group_y.append({"gx": t % nx, "gy": (t // nx) * xn + ixx, "gz": iz})
    group_x = [{"gx": ix, "gy": ih * xn + lax.rem(ixx + k, xn), "gz": iz} for k in range(1, xn)]
    group_z = [{"gx": ix, "gy": iy, "gz": lax.rem(iz + k, nz)} for k in range(1, nz)]

    barrier = pltpu.get_barrier_semaphore()
    loads = [pltpu.make_async_copy(r[a], r[b], r["lsem"].at[i]) for i, (a, b) in enumerate((("b", "B0"), ("w", "A0"), ("c", "CM")))]
    for c in loads:
        c.start()
    for d in group_x + group_y + group_z:
        pl.semaphore_signal(barrier, inc=1, device_id=d, device_id_type=MESH)

    for o in OFFS + OFF2Y + OFF2X:

        @pl.when(has(o))
        def _():
            pl.semaphore_signal(barrier, inc=1, device_id=dev(*o), device_id_type=MESH)

    partners = sum(jnp.where(has(o), 1, 0) for o in OFFS + OFF2X + OFF2Y) + len(group_y + group_x + group_z)

    lane = lax.broadcasted_iota(jnp.int32, (8, 128), 1)
    row = lax.broadcasted_iota(jnp.int32, (8, 128), 0)
    zero = jnp.zeros((8, 128), F32)

    def flag(c):
        return jnp.where(c, jnp.float32(1), jnp.float32(0))

    mx = {-1: flag(ix > 0), 0: jnp.float32(1), 1: flag(ix < nx - 1)}
    my = {-1: flag(iy > 0), 0: jnp.float32(1), 1: flag(iy < ny - 1)}
    mz = {-1: flag(iz > 0), 0: jnp.float32(1), 1: flag(iz < nz - 1)}

    b_ref, w_ref, c_ref, out_ref = r["B0"], r["A0"], r["CM"], r["out"]

    G0, W0, V0 = r["G0"], r["W0"], r["V0"]
    loads[0].wait()
    loads[1].wait()
    w0 = w_ref[...]
    g0 = b_ref[0] / w0
    W0[2:18, 8:24, :] = w0
    G0[2:18, 8:24, :] = g0

    r["YS"][0] = G0[2:18, 8:10, :]
    r["YS"][1] = G0[2:18, 22:24, :]

    def pack_q(src, dst):
        for h in range(2):
            acc = zero
            for x in range(16):
                m = src[x + 2, 8 + 8 * h : 16 + 8 * h, :]
                base = 6 * (x + 2)
                acc = jnp.where(lane == base, roll(m, base - 1), acc)
                acc = jnp.where((lane >= base + 1) & (lane < base + 3), roll(m, base + 1 - 127), acc)
                acc = jnp.where((lane >= base + 3) & (lane < base + 5), roll(m, base + 3 - 127), acc)
                acc = jnp.where(lane == base + 5, roll(m, base + 5 - 126), acc)
            dst[8 * h : 8 * h + 8, :] = acc

    pack_q(G0, r["QS"])
    r["QE"][0] = r["QS"][0:1, :]
    r["QE"][1] = r["QS"][15:16, :]

    for name in ("G0", "W0", "V0"):
        a = r[name]
        a[:, 0:8, :] = jnp.zeros((20, 8, 128), F32)
        a[:, 24:32, :] = jnp.zeros((20, 8, 128), F32)
    for name in ("GQ", "WQ", "VQ", "UQ", "G1", "W1", "V1", "U1", "G2", "W2", "V2", "U2", "P2", "Q2", "G3", "W3", "V3", "U3", "P3", "T4", "A1", "Q1", "R2", "PT", "QT", "Q3"):
        r[name][...] = jnp.zeros(r[name].shape, F32)

    zr = lax.broadcasted_iota(jnp.int32, (256, 128), 0) % 128
    zc = lax.broadcasted_iota(jnp.int32, (256, 128), 1)
    down = jnp.where(zc == 32 + zr // 2, jnp.float32(1), jnp.float32(0)).astype(jnp.bfloat16)
    up = jnp.where(zr == 32 + zc // 2, jnp.float32(1), jnp.float32(0)).astype(jnp.bfloat16)

    C0 = r["C0"]

    def coarsen0(values, scale):
        C0[...] = jnp.sum(values.reshape(8, 2, 16, 128), axis=1)
        t = C0[:, pl.ds(0, 8, stride=2), :] + C0[:, pl.ds(1, 8, stride=2), :]
        return (select_dot(t.reshape(64, 128), down) * scale).reshape(8, 8, 128)

    def pair_z(t, dil):
        ln = lax.broadcasted_iota(jnp.int32, t.shape, t.ndim - 1)
        return t + jnp.where((ln // dil) % 2 == 0, roll(t, -dil), roll(t, dil))

    C1, C2 = r["C1"], r["C2"]

    def coarsen1(values, scale):
        n = values.shape[0] // 2
        C1[...] = jnp.sum(values.reshape(n, 2, 8, 128), axis=1)
        t = C1[:, pl.ds(0, 4, stride=2), :] + C1[:, pl.ds(1, 4, stride=2), :]
        return pair_z(t, 1) * scale

    w1 = coarsen0(w0, 0.0625)
    own1 = (lane >= 32) & (lane < 96)
    w2 = coarsen1(w1, 0.0625)
    C2[0:4, 0:4, :] = w2
    t = C2[0:4, pl.ds(0, 2, stride=2), :] + C2[0:4, pl.ds(1, 2, stride=2), :]
    w3 = pair_z(jnp.sum(t.reshape(2, 2, 2, 128), axis=1), 2) * 0.0625

    lane4 = lane[0:4]

    def pack2(v):
        halves = []
        for h in range(2):
            a = jnp.where(lane4 % 2 == 0, v[2 * h], v[2 * h + 1])
            halves.append(roll(a, -32 if h == 0 else 32))
        return jnp.where(lane4 < 64, halves[0], halves[1])

    def pack3(v):
        return jnp.where(lane[0:2] < 64, roll(v[0], -32), roll(v[1], 32))

    SW2, SW3 = r["SW2"], r["SW3"]
    p2 = pack2(w2)
    SW2[...] = p2
    SW3[...] = pack3(w3)
    zp = jnp.zeros((4, 128), F32)
    for h in range(2):
        zp = jnp.where((lane4 >= 16 * h) & (lane4 < 16 * h + 8), roll(p2, -48 * h), zp)
        zp = jnp.where((lane4 >= 16 * h + 8) & (lane4 < 16 * h + 16), roll(p2, -48 * h - 48), zp)
    row4 = row[0:4]
    SWZ = r["SWZ"]
    SWZ[...] = sum(roll(jnp.sum(jnp.where(row4 == y, zp, 0.0), axis=0, keepdims=True), 32 * y) for y in range(4))

    def send_all(src, dst, key):
        return [round_of(key, [(o, src, dst.at[SLOT[neg(o)]]) for o in OFFS], first(dst))]

    def pack_z1(own, zs):
        acc = zero
        for x in range(8):
            acc = jnp.where((lane >= 16 * x) & (lane < 16 * x + 4), roll(own[x], 16 * x - 32), acc)
            acc = jnp.where((lane >= 16 * x + 4) & (lane < 16 * x + 8), roll(own[x], 16 * x + 4 - 92), acc)
        zs[...] = acc

    def place(m0, c, l, h):
        a = roll(m0, 32 if h == 0 else 96)
        e = roll(c, 96 if h == 0 else 32)
        return jnp.where((l >= 32) & (l < 96), a, e)

    s1w, ysw, zsw, yzw = r["S1w"], r["YS1w"], r["ZS1w"], r["YZ1w"]
    s1w[...] = w1
    ysw[0] = s1w[:, 0:2, :]
    ysw[1] = s1w[:, 6:8, :]
    pack_z1(w1, zsw)
    yzw[0] = zsw[0:2, :]
    yzw[1] = zsw[6:8, :]
    RX, RY, RXY, RZ, RYZ = (r[name + "w"] for name in ("RX1", "RY1", "RXY1", "RZ1", "RYZ1"))
    r["YW"][0] = W0[2:18, 8:9, :]
    r["YW"][1] = W0[2:18, 23:24, :]
    pack_q(W0, r["QW"])

    pl.semaphore_wait(barrier, partners)

    gsl = pl.ds(8, 16)
    wait_g0 = [
        round_of(1, [((0, d, 0), r["YS"].at[i], r["RY"].at[1 - i]) for i, d in enumerate((-1, 1))], first(r["RY"])),
        round_of(
            2,
            [
                ((dx, dy, 0), r["YS"].at[(dy + 1) // 2, 0 if dx < 0 else 15], r["RXY"].at[XY.index((-dx, -dy))])
                for dx, dy in XY
            ],
            first(r["RXY"]),
        ),
        round_of(
            4,
            [((0, dy, dz), r["QE"].at[(dy + 1) // 2], r["RQE"].at[XY.index((-dy, -dz))]) for dy, dz in XY],
            first(r["RQE"]),
        ),
        round_of(3, [((dx, 0, dz), r["QS"], r["RQ"].at[XZ.index((-dx, -dz))]) for dx, dz in XZ], first(r["RQ"])),
        round_of(
            0,
            [
                ((-1, 0, 0), G0.at[pl.ds(2, 2), gsl], G0.at[pl.ds(18, 2), gsl]),
                ((1, 0, 0), G0.at[pl.ds(16, 2), gsl], G0.at[pl.ds(0, 2), gsl]),
            ],
            lambda n: G0.at[pl.ds(0, 2 * n), gsl],
        ),
    ]

    wait_z = round_of(24, [((0, 0, d), SW3, r["RW3"].at[1 - i]) for i, d in enumerate((-1, 1))], first(r["RW3"]))
    wait_w = [
        round_of(7, [((0, -1, 0), ysw.at[0], RY.at[1]), ((0, 1, 0), ysw.at[1], RY.at[0])], first(RY)),
        round_of(
            8,
            [
                ((dx, dy, 0), ysw.at[(dy + 1) // 2, 0 if dx < 0 else 7], RXY.at[XY.index((-dx, -dy))])
                for dx, dy in XY
            ],
            first(RXY),
        ),
        round_of(
            27,
            [((0, dy, dz), yzw.at[(dy + 1) // 2], RYZ.at[XY.index((-dy, -dz))]) for dy, dz in XY],
            first(RYZ),
        ),
        round_of(5, [(o, SW2, r["RW2"].at[FLAT.index(neg(o))]) for o in FLAT], first(r["RW2"])),
        round_of(17, [(o, SWZ, r["RWZ"].at[ZSLOT[neg(o)]]) for o in ZOFFS], first(r["RWZ"])),
        round_of(6, [((-1, 0, 0), s1w.at[pl.ds(0, 2)], RX.at[1]), ((1, 0, 0), s1w.at[pl.ds(6, 2)], RX.at[0])], first(RX)),
        round_of(9, [((dx, 0, dz), zsw, RZ.at[XZ.index((-dx, -dz))]) for dx, dz in XZ], first(RZ)),
    ]

    def recv1w(dst):
        for x in range(1, 13):
            dx = -1 if x < 3 else (1 if x > 10 else 0)
            sx = x - 3 if dx == 0 else (x + 5 if dx < 0 else x - 11)

            def ends(v, ln, lo, hi, dx, dy):
                v = jnp.where((ln >= 28) & (ln < 32), keep(roll(lo, 28 - 16 * sx - 4), dx, dy, -1), v)
                return jnp.where((ln >= 96) & (ln < 100), keep(roll(hi, 96 - 16 * sx), dx, dy, 1), v)

            base = w1[x - 3] if dx == 0 else keep(RX[(dx + 1) // 2, x - 1 if dx < 0 else x - 11], dx, 0, 0)
            lo, hi = (RZ[XZ.index((dx, dz))] for dz in (-1, 1))
            dst[x, 8:16, :] = ends(base, lane, lo, hi, dx, 0)
            for dy, at in ((-1, 6), (1, 16)):
                if dx == 0:
                    lo, hi = (RYZ[XY.index((dy, dz))] for dz in (-1, 1))
                    v = keep(RY[(dy + 1) // 2, x - 3], 0, dy, 0)
                    dst[x, at : at + 2, :] = ends(v, lane[0:2], lo, hi, 0, dy)
                elif x in (2, 11):
                    dst[x, at : at + 2, :] = keep(RXY[XY.index((dx, dy))], dx, dy, 0)

    def send1(own, n, key):
        s1, ys, zs = r["S1" + n], r["YS1" + n], r["ZS1" + n]
        s1[...] = own
        for q in range(4):
            v = jnp.where(lane < 64, roll(own[2 * q], -32), roll(own[2 * q + 1], 32))
            ys[0, q] = v[0:4]
            ys[1, q] = v[4:8]
        pack_z1(own, zs)
        zy = r["ZY1g"]
        zy[0] = zs[0:4, :]
        zy[1] = zs[4:8, :]
        rx, ry, rxy, rz, rzy = (r[name + n] for name in ("RX1", "RY1", "RXY1", "RZ1", "RZY1"))
        return [
            round_of(key + 1, [((0, -1, 0), ys.at[0], ry.at[1]), ((0, 1, 0), ys.at[1], ry.at[0])], first(ry)),
            round_of(
                key + 2,
                [
                    ((dx, dy, 0), ys.at[(dy + 1) // 2, 0 if dx < 0 else 3], rxy.at[XY.index((-dx, -dy))])
                    for dx, dy in XY
                ],
                first(rxy),
            ),
            round_of(25, [(o, zy.at[(o[1] + 1) // 2], rzy.at[ZY.index(neg(o))]) for o in ZY], first(rzy)),
            round_of(
                key,
                [((-1, 0, 0), s1.at[pl.ds(0, 3)], rx.at[1]), ((1, 0, 0), s1.at[pl.ds(5, 3)], rx.at[0])],
                first(rx),
            ),
            round_of(key + 3, [((dx, 0, dz), zs, rz.at[XZ.index((-dx, -dz))]) for dx, dz in XZ], first(rz)),
        ]

    def half(m, q):
        return jnp.where((lane4 >= 32) & (lane4 < 96), roll(m, 32 if q == 0 else 96), 0.0)

    def recv1(own, n, key, dst):
        run(key)
        for x in range(14):
            dx = -1 if x < 3 else (1 if x > 10 else 0)
            for dy in (-1, 0, 1):
                if dx == 0 and dy == 0:
                    base = own[x - 3]
                elif dy == 0:
                    base = r["RX1" + n][(dx + 1) // 2, x if dx < 0 else x - 11]
                elif dx == 0:
                    base = half(r["RY1" + n][(dy + 1) // 2, (x - 3) // 2], (x - 3) % 2)
                elif x in (0, 13):
                    base = jnp.zeros((4, 128), F32)
                else:
                    base = half(r["RXY1" + n][XY.index((dx, dy))], (x - 1 if dx < 0 else x - 11) % 2)
                sx = x - 3 if dx == 0 else (x + 5 if dx < 0 else x - 11)
                if dy == 0:
                    lo, hi = (r["RZ1" + n][XZ.index((dx, dz))] for dz in (-1, 1))
                else:
                    lo, hi = (r["RZY1" + n][ZY.index((dx, dy, dz))] for dz in (-1, 1))
                ln = lane[0:8] if dy == 0 else lane4
                v = keep(base, dx, dy, 0)
                v = jnp.where((ln >= 28) & (ln < 32), keep(roll(lo, 28 - 16 * sx - 4), dx, dy, -1), v)
                v = jnp.where((ln >= 96) & (ln < 100), keep(roll(hi, 96 - 16 * sx), dx, dy, 1), v)
                at = 8 if dy == 0 else (4 if dy < 0 else 16)
                dst[x, at : at + (8 if dy == 0 else 4), :] = v

    wait_z()
    l2, l1 = lane[0:2], lane[0:1]
    ends3 = jnp.where((l2 // 32) % 2 == 1, keep(r["RW3"][0], 0, 0, -1), keep(r["RW3"][1], 0, 0, 1))
    own3 = [place(SW3[...], ends3, l2, h) for h in range(2)]
    XW3 = r["XW3"]
    XW3[...] = jnp.where(
        l1 % 4 < 2,
        jnp.where(l1 % 4 == 0, own3[0][0:1], own3[0][1:2]),
        jnp.where(l1 % 4 == 2, own3[1][0:1], own3[1][1:2]),
    )
    FAR = FLAT + OFF2Y + OFF2X
    wait_w3 = round_of(18, [(o, XW3, r["RWF"].at[FAR.index(neg(o))]) for o in FAR], first(r["RWF"]))

    wi1 = 1.0 / jnp.where(own1, w1, 1.0)
    wi2 = 1.0 / jnp.where(own1[0:4], w2, 1.0)

    GQ, VQ = r["GQ"], r["VQ"]
    run(wait_g0)
    G0[0:2, 8:24, :] = keep(G0[0:2, 8:24, :], -1, 0, 0)
    G0[18:20, 8:24, :] = keep(G0[18:20, 8:24, :], 1, 0, 0)
    G0[2:18, 6:8, :] = keep(r["RY"][0], 0, -1, 0)
    G0[2:18, 24:26, :] = keep(r["RY"][1], 0, 1, 0)
    for dx, dy in XY:
        v = keep(r["RXY"][XY.index((dx, dy))], dx, dy, 0)
        G0[1 if dx < 0 else 18, 7 if dy < 0 else 24, :] = v[1 if dy < 0 else 0, :]

    def qj(ln):
        return ln % 6

    for h in range(2):
        sl = slice(8 * h, 8 * h + 8)
        own = r["QS"][sl, :]
        j = qj(lane)
        q = [keep(r["RQ"][i, sl, :], dx, 0, dz) for i, (dx, dz) in enumerate(XZ)]
        v, lo, hi = (
            jnp.where((j == 3) | (j == 5), q[2 * i], jnp.where((j == 0) | (j == 2), q[2 * i + 1], own if i == 0 else 0.0))
            for i in range(3)
        )
        v = jnp.where((lane >= 6) & (lane < 12), roll(lo, 6 - 102), jnp.where((lane >= 108) & (lane < 114), roll(hi, 108 - 12), v))
        GQ[8 + 8 * h : 16 + 8 * h, :] = jnp.where((lane >= 6) & (lane < 114), v, 0.0)
    for dy, at in ((-1, 7), (1, 24)):
        j = qj(lane[0:1])
        lo = keep(r["RQE"][XY.index((dy, -1))], 0, dy, -1)
        hi = keep(r["RQE"][XY.index((dy, 1))], 0, dy, 1)
        v = jnp.where((j == 3) | (j == 5), lo, jnp.where((j == 0) | (j == 2), hi, 0.0))
        GQ[at : at + 1, :] = jnp.where((lane[0:1] >= 12) & (lane[0:1] < 108), v, 0.0)

    INJ = r["INJ"]

    def inject(q, xs, tiles):
        for at in tiles:
            m = q[at : at + 8, :]
            for xp in xs:
                INJ[xp, at : at + 8, :] = jnp.where((lane == 0) | (lane == 127), roll(m, -(6 * xp + 3)), 0.0)

    def sum0(a, x, n, at):
        c = a[x : x + n, at : at + 8, :]
        t = a[x - 1 : x + n - 1, at : at + 8, :] + a[x + 1 : x + n + 1, at : at + 8, :]
        t = t + (a[x : x + n, at - 1 : at + 7, :] + a[x : x + n, at + 1 : at + 9, :])
        z = jnp.where(lane == 0, 0.0, roll(c, 1)) + jnp.where(lane == 127, 0.0, roll(c, -1))
        return c, t + (z + INJ[x : x + n, at : at + 8, :])

    inject(GQ, range(1, 19), (7, 15, 17))
    for at in (7, 15, 17):
        c, t = sum0(G0, 1, 18, at)
        v = S * (1.2 * c + S * t)
        if at == 7:
            v = v * jnp.where(row == 0, my[-1], 1.0)
        if at == 17:
            v = v * jnp.where(row == 7, my[1], 1.0)
        V0[1:19, at : at + 8, :] = v
    V0[1:2, 7:25, :] = V0[1:2, 7:25, :] * mx[-1]
    V0[18:19, 7:25, :] = V0[18:19, 7:25, :] * mx[1]

    for at in (8, 16):
        c = GQ[at : at + 8, :]
        t = jnp.where(qj(lane) == 3, roll(c, -1) + roll(c, -2), roll(c, 1) + roll(c, 2)) + (roll(c, 6) + roll(c, -6))
        t = t + GQ[at - 1 : at + 7, :] + GQ[at + 1 : at + 9, :]
        j = qj(lane)
        mask = jnp.where(j == 3, mz[-1], jnp.where(j == 2, mz[1], 0.0))
        mask = jnp.where((lane >= 12) & (lane < 108), mask, 0.0)
        VQ[at : at + 8, :] = S * (1.2 * c + S * t) * mask

    inject(VQ, range(2, 18), (8, 16))
    halves = []
    for at in (8, 16):
        c, t = sum0(V0, 2, 16, at)
        halves.append(W0[2:18, at : at + 8, :] * (G0[2:18, at : at + 8, :] - 6.0 * c + t))
    r0 = jnp.concatenate(halves, axis=1)
    g1 = jnp.where(own1, coarsen0(r0, 0.125) * wi1, 0.0)
    wait_g1 = send1(g1, "g", 10)

    G1, W1, V1, U1 = r["G1"], r["W1"], r["V1"], r["U1"]
    G2, W2, V2, U2, P2, Q2 = r["G2"], r["W2"], r["V2"], r["U2"], r["P2"], r["Q2"]
    G3, W3, V3, U3, P3 = r["G3"], r["W3"], r["V3"], r["U3"], r["P3"]
    run(wait_w)
    recv1w(W1)

    def spread(m0, lo, hi, l, dx, dy):
        return keep(m0, dx, dy, 0), jnp.where((l // 32) % 2 == 1, keep(lo, dx, dy, -1), keep(hi, dx, dy, 1))

    def piece(buf, own, rows, o):
        return own[rows, :] if o == (0, 0, 0) else buf[SLOT[o], rows, :]

    def unpack2(buf, own, dst):
        rows = slice(0, 4)
        for dx in (-1, 0, 1):
            for dy in (-1, 0, 1):
                m0, c = spread(*[piece(buf, own, rows, (dx, dy, dz)) for dz in (0, -1, 1)], lane4, dx, dy)
                spread2(m0, c, dst, dx, dy)

    def spread2(m0, c, dst, dx, dy):
        for p in range(2):
            take = lane4 % 2 == p
            a = jnp.where(take, m0, roll(m0, 1 if p == 0 else -1))
            e = jnp.where(take, c, roll(c, 1 if p == 0 else -1))
            for h in range(2):
                dst[4 + 4 * dx + 2 * h + p, 8 + 4 * dy : 12 + 4 * dy, :] = place(a, e, lane4, h)

    def unpack3(get, spots, dst):
        l = lane[0:2]
        for dx, dy in spots:
            m0, c = spread(*[get((dx, dy, dz)) for dz in (0, -1, 1)], l, dx, dy)
            for h in range(2):
                dst[5 + 2 * dx + h, 12 + 2 * dy : 14 + 2 * dy, :] = place(m0, c, l, h)

    for dx in (-1, 0, 1):
        for dy in (-1, 0, 1):
            m0 = keep(SW2[...] if dx == dy == 0 else r["RW2"][FLAT.index((dx, dy, 0))], dx, dy, 0)
            lo, hi = (keep(r["RWZ"][ZSLOT[(dx, dy, dz)]], dx, dy, dz) for dz in (-1, 1))
            line = jnp.where(lane[0:1] % 16 >= 8, lo, hi)
            e = jnp.zeros((4, 128), F32)
            for y in range(4):
                e = jnp.where(row4 == y, roll(line, -32 * y), e)
            c = jnp.zeros((4, 128), F32)
            for h in range(2):
                c = jnp.where((lane4 >= 64 * h) & (lane4 < 64 * h + 8), roll(e, 48 * h), c)
                c = jnp.where((lane4 >= 64 * h + 56) & (lane4 < 64 * h + 64), roll(e, 48 * h + 48), c)
            spread2(m0, c, W2, dx, dy)

    def inverse(w):
        return jnp.where(w > 0.0, 1.0 / jnp.where(w > 0.0, w, 1.0), 0.0)

    def nsum(a, x, n, at, rows, dil):
        c = a[x : x + n, at : at + rows, :]
        t = a[x - 1 : x + n - 1, at : at + rows, :] + a[x + 1 : x + n + 1, at : at + rows, :]
        t = t + (a[x : x + n, at - 1 : at + rows - 1, :] + a[x : x + n, at + 1 : at + rows + 1, :])
        return c, t + (roll(c, dil) + roll(c, -dil))

    def rowmask(at, rows, low, high):
        y = lax.broadcasted_iota(jnp.int32, (rows, 128), 0) + at
        l = lax.broadcasted_iota(jnp.int32, (rows, 128), 1)
        m = jnp.where(y < low, my[-1], jnp.where(y >= high, my[1], 1.0))
        return m * jnp.where(l < 32, mz[-1], jnp.where(l >= 96, mz[1], 1.0))

    def xmask(a, low, high, x, n, at, rows):
        if low > x:
            a[x:low, at : at + rows, :] = a[x:low, at : at + rows, :] * mx[-1]
        if x + n > high:
            a[high : x + n, at : at + rows, :] = a[high : x + n, at : at + rows, :] * mx[1]

    A1, Q1, R2, PT, QT, Q3 = r["A1"], r["Q1"], r["R2"], r["PT"], r["QT"], r["Q3"]
    A1[3:11, 8:16, :] = g1
    for at in (4, 12):
        c, t = nsum(A1, 1, 12, at, 8, 1)
        Q1[1:13, at : at + 8, :] = S * (1.2 * c + S * t) * rowmask(at, 8, 8, 16)
    xmask(Q1, 3, 11, 1, 12, 4, 16)
    C3 = r["C3"]
    for at in (6, 10):
        c, t = nsum(Q1, 1, 12, at, 8, 1)
        res = W1[1:13, at : at + 8, :] * (A1[1:13, at : at + 8, :] - 6.0 * c + t)
        C3[:, at - 6 : at + 2, :] = jnp.sum(res.reshape(6, 2, 8, 128), axis=1)
    t = C3[:, pl.ds(0, 6, stride=2), :] + C3[:, pl.ds(1, 6, stride=2), :]
    P2[3:9, 7:13, :] = pair_z(t, 1) * 0.125 * inverse(W2[3:9, 7:13, :])
    c, t = nsum(P2, 2, 8, 6, 8, 2)
    Q2[2:10, 6:14, :] = S * (1.2 * c + S * t) * rowmask(6, 8, 8, 12)
    xmask(Q2, 4, 8, 2, 8, 6, 8)
    for at in (5, 7):
        c, t = nsum(Q2, 1, 10, at, 8, 2)
        R2[1:11, at : at + 8, :] = W2[1:11, at : at + 8, :] * (P2[1:11, at : at + 8, :] - 6.0 * c + t)
    C3[...] = jnp.sum(R2[:, 4:20, :].reshape(6, 2, 16, 128), axis=1)
    t = C3[:, pl.ds(0, 6, stride=2), :] + C3[:, pl.ds(1, 6, stride=2), :]
    b3 = pair_z(t, 2) * 0.125
    wait_w3()
    W3[5, 12:14, :] = own3[0]
    W3[6, 12:14, :] = own3[1]
    ST, SU = r["ST"], r["SU"]
    for k, o in enumerate(FAR):
        ST[k : k + 1, :] = keep(r["RWF"][k], *o)
    for q in range(4):
        t = roll(jnp.where(lax.broadcasted_iota(jnp.int32, (24, 128), 1) % 4 == q, ST[...], 0.0), -q)
        t = t + roll(t, 1)
        SU[q] = t + roll(t, 2)
    for k, (dx, dy, _) in enumerate(FAR):
        for q in range(4):
            at = 12 + 2 * dy + q % 2
            W3[5 + 2 * dx + q // 2, at : at + 1, :] = SU[q, k : k + 1, :]
    P3[3:9, 10:16, :] = b3 * inverse(W3[3:9, 10:16, :])
    c, t = nsum(P3, 2, 8, 9, 8, 4)
    Q3[2:10, 9:17, :] = S * (1.2 * c + S * t) * rowmask(9, 8, 12, 14)
    xmask(Q3, 5, 7, 2, 8, 9, 8)
    T4 = r["T4"]
    for at in (8, 10):
        c, t = nsum(Q3, 1, 10, at, 8, 4)
        res = W3[1:11, at : at + 8, :] * (P3[1:11, at : at + 8, :] - 6.0 * c + t)
        T4[:, at : at + 8, :] = jnp.sum(res.reshape(5, 2, 8, 128), axis=1)
    t = T4[:, pl.ds(8, 8, stride=2), :] + T4[:, pl.ds(9, 8, stride=2), :]
    patch = pair_z(t, 4) * 0.125

    lines = []
    for dx in range(5):
        v = patch[dx]
        main = zero
        for q in range(4):
            lo = 32 + 16 * q + 7
            main = jnp.where((lane >= 2 * q) & (lane < 2 * q + 2), roll(v, 2 * q - lo), main)
        edge = jnp.where(lane < 2, roll(v, 0 - 23), jnp.where(lane < 4, roll(v, 2 - 103), 0.0))
        line = pltpu.roll(main, 0, 1, stride=8, stride_axis=0) + pltpu.roll(edge, 40, 1, stride=4, stride_axis=0)
        lines.append(jnp.sum(line, axis=0, keepdims=True))
    GA, GB, GC = r["GA"], r["GB"], r["GC"]
    SA, SB, SZ = r["SA"], r["SB"], r["SZ"]
    for p in range(2):
        SA[p : p + 1, :] = lines[2 * p] + roll(lines[2 * p + 1], 64)
    SA[2:3, :] = lines[4]
    SA[3:4, :] = jnp.zeros((1, 128), F32)
    ga_at = ih * nx + ix
    to_group(21, SA, GA.at[ga_at], group_y)

    wait_w0 = [
        round_of(
            14,
            [
                ((-1, 0, 0), W0.at[pl.ds(2, 1), gsl], W0.at[pl.ds(18, 1), gsl]),
                ((1, 0, 0), W0.at[pl.ds(17, 1), gsl], W0.at[pl.ds(1, 1), gsl]),
            ],
            lambda n: W0.at[pl.ds(0, n), gsl],
        ),
        round_of(15, [((0, d, 0), r["YW"].at[i], r["RYW"].at[1 - i]) for i, d in enumerate((-1, 1))], first(r["RYW"])),
        round_of(16, [((0, 0, d), r["QW"], r["RQW"].at[1 - i]) for i, d in enumerate((-1, 1))], first(r["RQW"])),
    ]

    cp = r["CP"]
    loads[2].wait()

    @pl.loop(0, nx)
    def _(x):
        for z in range(nz):
            acc = zero
            for p in range(ny // 2):
                tile = c_ref[:, pl.ds(pl.multiple_of((x * (ny // 2) + p) * 128, 128), 128)]
                for q in range(2):
                    y = 2 * p + q
                    at = 8 * y
                    acc = jnp.where((lane >= at) & (lane < at + 8), roll(tile, at - 64 * q - 8 * z), acc)
            cp[x * nz + z] = acc

    from_group(21, GA, n_y - 1)
    GA[ga_at] = SA[...]
    sums = []
    for h in range(2):
        even, odd = zero, zero
        for p in range(3):
            m = zero
            for g in range(nx):
                m = jnp.where(row == g, GA[h * nx + g, p : p + 1, :], m)
            even = even + (m if p == 1 else pltpu.roll(m, (2 * p - 2) % 8, 0))
            if p < 2:
                odd = odd + pltpu.roll(m, (2 * p - 1) % 8, 0)
        sums.append(jnp.where(lane < 64, even, 0.0) + roll(jnp.where(lane < 64, 0.0, odd), 64))
    SB[...] = sums[0] + roll(sums[1], 64)
    to_group(22, SB, GB.at[ixx], group_x)

    recv1(g1, "g", wait_g1, G1)
    for at in (4, 12):
        c, t = nsum(G1, 1, 12, at, 8, 1)
        V1[1:13, at : at + 8, :] = S * (1.2 * c + S * t) * rowmask(at, 8, 8, 16)
    xmask(V1, 3, 11, 1, 12, 4, 16)
    c, t = nsum(V1, 3, 8, 8, 8, 1)
    r1 = W1[3:11, 8:16, :] * (G1[3:11, 8:16, :] - 6.0 * c + t)
    g2 = jnp.where(own1[0:4], coarsen1(r1, 0.125) * wi2, 0.0)

    PT[4:8, 8:12, :] = g2
    c, t = nsum(PT, 2, 8, 6, 8, 2)
    QT[2:10, 6:14, :] = S * (1.2 * c + S * t) * rowmask(6, 8, 8, 12)
    xmask(QT, 4, 8, 2, 8, 6, 8)
    c, t = nsum(QT, 2, 8, 6, 8, 2)
    res = W2[2:10, 6:14, :] * (PT[2:10, 6:14, :] - 6.0 * c + t)
    C2[...] = jnp.sum(res.reshape(4, 2, 8, 128), axis=1)
    t = C2[:, pl.ds(0, 4, stride=2), :] + C2[:, pl.ds(1, 4, stride=2), :]
    b3 = pair_z(t, 2) * 0.125
    SC = r["SC"]
    SC[0:4, :] = pack2(g2)
    l4 = lane4 % 4
    SC[4:8, :] = jnp.where(l4 < 2, jnp.where(l4 == 0, b3[0], b3[1]), jnp.where(l4 == 2, b3[2], b3[3]))
    wait_c = send_all(SC, r["RC"], 19)

    from_group(22, GB, xn - 1)
    GB[ixx] = SB[...]
    main = zero
    edges = [zero] * 5
    for k in range(xn):
        v = GB[k]
        for h in range(2):
            if xn == 8 and h == 1:
                continue
            shift = 8 * k - 16 + h * (8 * xn - 64)
            m = roll(v, shift)
            src = (lane - shift + 256) % 128
            if xn != 8:
                m = jnp.where(src // 64 == h, m, 0.0)
            main = main + jnp.where(src % 64 < 40, m, 0.0)
            for dy in range(5):
                a = 40 + 4 * dy
                edges[dy] = edges[dy] + jnp.where((src % 64 >= a) & (src % 64 < a + 4), m, 0.0)
    edge = zero
    for dy in range(5):
        edge = edge + roll(edges[dy], 4 * dy - 40)
    SZ[0] = main
    SZ[1] = edge
    to_group(23, SZ, GC.at[iz], group_z)

    run(wait_w0)
    W0[1:2, 8:24, :] = keep(W0[1:2, 8:24, :], -1, 0, 0)
    W0[18:19, 8:24, :] = keep(W0[18:19, 8:24, :], 1, 0, 0)
    W0[2:18, 7:8, :] = keep(r["RYW"][0], 0, -1, 0)
    W0[2:18, 24:25, :] = keep(r["RYW"][1], 0, 1, 0)
    for h in range(2):
        sl = slice(8 * h, 8 * h + 8)
        j = qj(lane)
        v = jnp.where(j == 3, keep(r["RQW"][0, sl, :], 0, 0, -1), jnp.where(j == 2, keep(r["RQW"][1, sl, :], 0, 0, 1), 0.0))
        r["WQ"][8 + 8 * h : 16 + 8 * h, :] = v

    run(wait_c)
    unpack2(r["RC"], SC, G2)
    c, t = nsum(G2, 2, 8, 6, 8, 2)
    V2[2:10, 6:14, :] = S * (1.2 * c + S * t) * rowmask(6, 8, 8, 12)
    xmask(V2, 4, 8, 2, 8, 6, 8)

    TB, TC, RC = r["TB"], r["TC"], r["RC"]
    for dy in (-1, 0, 1):
        acc = jnp.zeros((4, 128), F32)
        for dx in (-1, 0, 1):
            m0, lo, hi = (keep(piece(RC, SC, slice(4, 8), (dx, dy, dz)), dx, dy, dz) for dz in (0, -1, 1))
            e = jnp.where((lane4 >= 92) & (lane4 < 100), lo, jnp.where((lane4 >= 28) & (lane4 < 36), hi, 0.0))
            q = m0 + roll(e, 64)
            if dx < 0:
                q = jnp.where(l4 < 2, roll(q, -2), 0.0)
            if dx > 0:
                q = jnp.where(l4 >= 2, roll(q, 2), 0.0)
            acc = acc + q
        TB[dy + 1] = acc
    TC[0:2, :] = TB[1, 0:2, :] + TB[0, 2:4, :]
    TC[2:4, :] = TB[1, 2:4, :] + TB[2, 0:2, :]
    for i in range(4):
        v = roll(jnp.where(l4 == i, TC[...], 0.0), -i)
        v = v + roll(v, 1)
        v = v + roll(v, 2)
        G3[4 + i, 11:15, :] = v * inverse(W3[4 + i, 11:15, :])
    c, t = nsum(G3, 5, 2, 12, 2, 4)
    v3 = jnp.where(own1[0:2], S * (1.2 * c + S * t), 0.0)
    SE, SV, RE, RV = r["SE"], r["SV"], r["RE"], r["RV"]
    SV[...] = pack3(v3)
    wait_v = send_all(SV, RV, 26)

    def drain(key, slots, count, sizes):
        for n in sizes:

            @pl.when(count == n)
            def _():
                copy(slots(n), slots(n), key, right).wait_send()

    early = len(sent) - 1
    for item in sent[:early]:
        drain(*item)

    from_group(23, GC, nz - 1)
    GC[iz, 0] = SZ[0]
    GC[iz, 1] = SZ[1]
    acc = [zero] * 4
    for z in range(nz):
        v = GC[z, 0]
        if z + 1 < nz:
            v = v + jnp.where(lane % 8 >= 6, roll(GC[z + 1, 1], 6), 0.0)
        if z > 0:
            v = v + jnp.where(lane % 8 < 2, roll(GC[z - 1, 1], -2), 0.0)
        for x in range(nx):
            acc[x % 4] = acc[x % 4] + cp[x * nz + z] * v[x : x + 1, :]
    acc = (acc[0] + acc[1]) + (acc[2] + acc[3])
    tot = jnp.sum(acc, axis=1, keepdims=True)
    e4 = jnp.sum(jnp.where((lane >= 32 + 8 * row) & (lane < 40 + 8 * row), tot, 0.0), axis=0, keepdims=True)
    SE[...] = e4
    wait_e = send_all(SE, RE, 20)
    run(wait_v)

    near = [(a, b) for a in (-1, 0, 1) for b in (-1, 0, 1)]
    unpack3(lambda o: SV[...] if o == (0, 0, 0) else RV[SLOT[o]], near, V3)
    run(wait_e)
    l1 = lane[0:1]
    par = []
    for dx in (-1, 0, 1):
        v = zero
        for dy in (-1, 0, 1):
            o = (dx, dy, 0)
            own = SE[...] if o == (0, 0, 0) else keep(RE[SLOT[o], 0:1, :], *o)
            lo, hi = (keep(RE[SLOT[(dx, dy, dz)], 0:1, :], dx, dy, dz) for dz in (-1, 1))
            e = jnp.where((l1 >= 32) & (l1 < 96), own, roll(jnp.where(l1 < 64, hi, lo), 64))
            y = 4 + 2 * dy
            v = jnp.where((row == y) | (row == y + 1), e, v)
        par.append(v)
    for i in range(6):
        U3[3 + i, 8:16, :] = V3[3 + i, 8:16, :] + W3[3 + i, 8:16, :] * par[i // 2]
    c, t = nsum(U3, 4, 4, 8, 8, 4)
    E3 = r["E3"]
    E3[...] = (0.2 * c + S * (G3[4:8, 8:16, :] + t)) * inverse(W3[4:8, 8:16, :])
    F2 = r["F2"]
    F2[:, pl.ds(0, 4, stride=2), :] = E3[:, 3:7, :]
    F2[:, pl.ds(1, 4, stride=2), :] = E3[:, 3:7, :]
    for i in range(8):
        U2[2 + i, 6:14, :] = V2[2 + i, 6:14, :] + W2[2 + i, 6:14, :] * F2[i // 2]
    c, t = nsum(U2, 3, 6, 6, 8, 2)
    E2 = r["E2"]
    E2[...] = (0.2 * c + S * (G2[3:9, 6:14, :] + t)) * inverse(W2[3:9, 6:14, :])
    F1 = r["F1"]
    F1[:, pl.ds(2, 6, stride=2), :] = E2[:, 1:7, :]
    F1[:, pl.ds(3, 6, stride=2), :] = E2[:, 1:7, :]
    for i in range(12):
        U1[1 + i, 6:18, :] = V1[1 + i, 6:18, :] + W1[1 + i, 6:18, :] * F1[i // 2, 2:14, :]
    E1 = r["E1"]
    for at in (7, 9):
        c, t = nsum(U1, 2, 10, at, 8, 1)
        E1[:, at - 7 : at + 1, :] = (0.2 * c + S * (G1[2:12, at : at + 8, :] + t)) * inverse(W1[2:12, at : at + 8, :])
    o = select_dot(E1[...].reshape(160, 128), up).reshape(10, 16, 128)
    F0 = r["F0"]
    O1 = r["O1"]
    O1[...] = o
    F0[:, pl.ds(6, 10, stride=2), :] = O1[:, 0:10, :]
    F0[:, pl.ds(7, 10, stride=2), :] = O1[:, 0:10, :]
    acc = zero
    for x in range(8):
        e = E1[x + 1, 1:9, :]
        for p in range(2):
            base = 6 * (2 * x + p + 2)
            acc = jnp.where(lane == base + 3, roll(e, base + 3 - 31), acc)
            acc = jnp.where(lane == base + 2, roll(e, base + 2 - 96), acc)
    UQ = r["UQ"]
    FQ = r["FQ"]
    FQ[...] = acc
    UQ[pl.ds(8, 8, stride=2), :] = FQ[...]
    UQ[pl.ds(9, 8, stride=2), :] = FQ[...]
    UQ[8:24, :] = VQ[8:24, :] + r["WQ"][8:24, :] * UQ[8:24, :]
    for i in range(18):
        V0[1 + i, 7:25, :] = V0[1 + i, 7:25, :] + W0[1 + i, 7:25, :] * F0[(i + 1) // 2, 7:25, :]
    inject(UQ, range(2, 18), (8, 16))
    for at in (8, 16):
        c, t = sum0(V0, 2, 16, at)
        out_ref[:, at - 8 : at, :] = 0.2 * c + S * (G0[2:18, at : at + 8, :] + t)

    for item in sent[early:]:
        drain(*item)
    for key, buf, n in ((21, GA, n_y - 1), (22, GB, xn - 1), (23, GC, nz - 1)):
        copy(buf.at[pl.ds(0, n)], buf.at[pl.ds(0, n)], key, right).wait_send()


def scratch(dims):
    nx, ny, nz = dims
    xn = ny // 2
    v = {
        "B0": (1, 16, 16, 128), "A0": (16, 16, 128), "CM": (8, nx * ny * nz * 8),
        "G0": (20, 32, 128), "W0": (20, 32, 128), "V0": (20, 32, 128), "INJ": (20, 32, 128),
        "GQ": (32, 128), "VQ": (32, 128), "WQ": (32, 128), "UQ": (32, 128),
        "YS": (2, 16, 2, 128), "RY": (2, 16, 2, 128), "RXY": (4, 2, 128),
        "QS": (16, 128), "QW": (16, 128), "RQ": (6, 16, 128), "QE": (2, 1, 128), "RQE": (4, 1, 128),
        "YW": (2, 16, 1, 128), "RYW": (2, 16, 1, 128), "RQW": (2, 16, 128),
        "C0": (8, 16, 128), "C1": (4, 8, 128), "C2": (4, 8, 128),
        "SW2": (4, 128), "SW3": (2, 128), "SWZ": (1, 128), "RW2": (8, 4, 128), "RWZ": (18, 1, 128), "XW3": (1, 128),
        "RW3": (2, 2, 128), "RWF": (20, 1, 128), "ST": (24, 128), "SU": (4, 24, 128), "C3": (6, 16, 128),
        "A1": (14, 24, 128), "Q1": (14, 24, 128), "R2": (12, 24, 128), "PT": (12, 24, 128), "QT": (12, 24, 128),
        "G1": (14, 24, 128), "W1": (14, 24, 128), "V1": (14, 24, 128), "U1": (14, 24, 128),
        "G2": (12, 24, 128), "W2": (12, 24, 128), "V2": (12, 24, 128), "U2": (12, 24, 128),
        "P2": (12, 24, 128), "Q2": (12, 24, 128),
        "G3": (12, 24, 128), "W3": (12, 24, 128), "V3": (12, 24, 128), "U3": (12, 24, 128), "P3": (12, 24, 128), "Q3": (12, 24, 128),
        "T4": (5, 24, 128),
        "SC": (8, 128), "RC": (26, 8, 128), "TB": (3, 4, 128), "TC": (4, 128), "SE": (1, 128), "RE": (26, 1, 128), "SV": (2, 128), "RV": (26, 2, 128),
        "SA": (4, 128), "SB": (8, 128), "SZ": (2, 8, 128),
        "GA": (2 * nx, 4, 128), "GB": (xn, 8, 128), "GC": (nz, 2, 8, 128), "CP": (nx * nz, 8, 128),
        "E3": (4, 8, 128), "F2": (4, 8, 128), "E2": (6, 8, 128), "F1": (6, 16, 128),
        "E1": (10, 16, 128), "O1": (10, 16, 128), "F0": (10, 32, 128), "FQ": (8, 128),
    }
    n = "g"
    v["S1" + n] = (8, 8, 128)
    v["YS1" + n] = (2, 4, 4, 128)
    v["ZS1" + n] = (8, 128)
    v["ZY1" + n] = (2, 4, 128)
    v["RX1" + n] = (2, 3, 8, 128)
    v["RY1" + n] = (2, 4, 4, 128)
    v["RXY1" + n] = (4, 4, 128)
    v["RZ1" + n] = (6, 8, 128)
    v["RZY1" + n] = (12, 4, 128)
    n = "w"
    v["S1" + n] = (8, 8, 128)
    v["YS1" + n] = (2, 8, 2, 128)
    v["ZS1" + n] = (8, 128)
    v["YZ1" + n] = (2, 2, 128)
    v["RX1" + n] = (2, 2, 8, 128)
    v["RY1" + n] = (2, 8, 2, 128)
    v["RXY1" + n] = (4, 2, 128)
    v["RZ1" + n] = (6, 8, 128)
    v["RYZ1" + n] = (4, 2, 128)
    return v


def solution(mesh):
    dims = tuple(mesh.shape[a] for a in ("gx", "gy", "gz"))
    sizes = scratch(dims)

    def body(*args):
        names = ["b", "w", "c", "out"] + list(sizes) + ["ssem", "rsem", "lsem"]
        kernel(dims, dict(zip(names, args)))

    def per_device(sources, stiffness, coarse_inverse):
        vmem = pl.BlockSpec(memory_space=pltpu.VMEM)
        e = pl.pallas_call(
            body,
            out_shape=jax.ShapeDtypeStruct((16, 16, 128), F32),
            in_specs=[pl.BlockSpec(memory_space=pltpu.HBM)] * 3,
            out_specs=vmem,
            scratch_shapes=[pltpu.VMEM(s, F32) for s in sizes.values()] + [pltpu.SemaphoreType.DMA((28,))] * 2 + [pltpu.SemaphoreType.DMA((3,))],
            compiler_params=pltpu.CompilerParams(collective_id=0, has_side_effects=True, vmem_limit_bytes=24 * 2**20),
            name="vcycle",
        )(*[pltpu.with_memory_space_constraint(a, pltpu.HBM) for a in (sources, stiffness, coarse_inverse)])
        return (e / stiffness)[None]

    return jax.shard_map(
        per_device,
        mesh=mesh,
        in_specs=(P(None, "gx", "gy", "gz"), P("gx", "gy", "gz"), P(("gx", "gy", "gz"), None)),
        out_specs=P(None, "gx", "gy", "gz"),
        check_vma=False,
    )
```

```python
import functools
import itertools

import jax
import jax.numpy as jnp
from jax import lax
from jax.experimental import pallas as pl
from jax.experimental.pallas import tpu as pltpu
from jax.sharding import PartitionSpec as P

MESH = pl.DeviceIdType.MESH
F32 = jnp.float32
S = 0.8 / 6.0
OFFS = [o for o in itertools.product((-1, 0, 1), repeat=3) if o != (0, 0, 0)]
OFFS.sort(key=lambda o: (-abs(o[1]), -abs(o[2]), -abs(o[0])))
OFF2X = [(2 * a, b, c) for a in (-1, 1) for b in (-1, 0, 1) for c in (-1, 0, 1)]
OFF2Y = [(b, 2 * a, c) for a in (-1, 1) for b in (-1, 0, 1) for c in (-1, 0, 1)]
FLAT = [o for o in OFFS if o[2] == 0]
SLOT = {o: i for i, o in enumerate(OFFS)}
ZOFFS = [o for o in OFFS if o[2] != 0]
ZSLOT = {o: i for i, o in enumerate(ZOFFS)}
ZY = [o for o in ZOFFS if o[1] != 0]
XY = [(-1, -1), (-1, 1), (1, -1), (1, 1)]
XZ = [(0, -1), (0, 1)] + XY


def neg(o):
    return tuple(-v for v in o)


def roll(v, shift):
    shift = shift % 128
    return v if shift == 0 else pltpu.roll(v, shift, v.ndim - 1)


def split2(v):
    hi = v.astype(jnp.bfloat16)
    lo = (v - hi.astype(F32)).astype(jnp.bfloat16)
    return jnp.concatenate([hi, lo], axis=1)


def select_dot(v, sel):
    return jnp.dot(split2(v), sel, preferred_element_type=F32)


def kernel(dims, refs):
    nx, ny, nz = dims
    xn = ny // 2
    n_y = nx * 2
    r = refs
    ix, iy, iz = lax.axis_index("gx"), lax.axis_index("gy"), lax.axis_index("gz")
    ih, ixx = iy // xn, iy % xn

    def dev(dx, dy, dz):
        return {
            "gx": lax.rem(ix + dx + nx, nx),
            "gy": lax.rem(iy + dy + ny, ny),
            "gz": lax.rem(iz + dz + nz, nz),
        }

    def copy(src, dst, key, device):
        return pltpu.make_async_remote_copy(
            src_ref=src,
            dst_ref=dst,
            send_sem=r["ssem"].at[key],
            recv_sem=r["rsem"].at[key],
            device_id=device,
            device_id_type=MESH,
        )

    cx = {-2: ix > 1, -1: ix > 0, 1: ix < nx - 1, 2: ix < nx - 2}
    cy = {-2: iy > 1, -1: iy > 0, 1: iy < ny - 1, 2: iy < ny - 2}
    cz = {-1: iz > 0, 1: iz < nz - 1}

    def has(o):
        c = [f[v] for f, v in zip((cx, cy, cz), o) if v]
        return functools.reduce(jnp.logical_and, c)

    def keep(v, *o):
        return jnp.where(has(o), v, 0.0) if any(o) else v

    sent = []

    def round_of(key, items, slots):
        for o, src, dst in items:

            @pl.when(has(o))
            def _():
                copy(src, dst, key, dev(*o)).start()

        offs = [o for o, _, _ in items]
        count = sum(jnp.where(has(o), 1, 0) for o in offs)
        spots = [sorted({0, 1, 2, n - 3, n - 2, n - 1} & set(range(n))) for n in dims]
        sizes = {sum(all(0 <= v + p < n for v, p, n in zip(o, at, dims)) for o in offs) for at in itertools.product(*spots)}
        sizes = sorted(n for n in sizes if n)
        sent.append((key, slots, count, sizes))

        def wait():
            for n in sizes:

                @pl.when(count == n)
                def _():
                    copy(slots(n), slots(n), key, right).wait_recv()

        return wait

    def first(ref):
        return lambda n: ref.at[pl.ds(0, n)]

    def to_group(key, src, dst, group):
        for d in group:
            copy(src, dst, key, d).start()

    def from_group(key, buf, n):
        copy(buf.at[pl.ds(0, n)], buf.at[pl.ds(0, n)], key, right).wait_recv()

    def run(waits):
        for w in waits:
            w()

    me = {"gx": ix, "gy": iy, "gz": iz}
    right = {"gx": lax.rem(ix + 1, nx), "gy": iy, "gz": iz}

    group_y = []
    for k in range(1, n_y):
        t = lax.rem(ih * nx + ix + k, n_y)
        group_y.append({"gx": t % nx, "gy": (t // nx) * xn + ixx, "gz": iz})
    group_x = [{"gx": ix, "gy": ih * xn + lax.rem(ixx + k, xn), "gz": iz} for k in range(1, xn)]
    group_z = [{"gx": ix, "gy": iy, "gz": lax.rem(iz + k, nz)} for k in range(1, nz)]

    barrier = pltpu.get_barrier_semaphore()
    loads = [pltpu.make_async_copy(r[a], r[b], r["lsem"].at[i]) for i, (a, b) in enumerate((("b", "B0"), ("w", "A0"), ("c", "CM")))]
    for c in loads:
        c.start()
    for d in group_x + group_y + group_z:
        pl.semaphore_signal(barrier, inc=1, device_id=d, device_id_type=MESH)

    for o in OFFS + OFF2Y + OFF2X:

        @pl.when(has(o))
        def _():
            pl.semaphore_signal(barrier, inc=1, device_id=dev(*o), device_id_type=MESH)

    partners = sum(jnp.where(has(o), 1, 0) for o in OFFS + OFF2X + OFF2Y) + len(group_y + group_x + group_z)

    lane = lax.broadcasted_iota(jnp.int32, (8, 128), 1)
    row = lax.broadcasted_iota(jnp.int32, (8, 128), 0)
    zero = jnp.zeros((8, 128), F32)

    def flag(c):
        return jnp.where(c, jnp.float32(1), jnp.float32(0))

    mx = {-1: flag(ix > 0), 0: jnp.float32(1), 1: flag(ix < nx - 1)}
    my = {-1: flag(iy > 0), 0: jnp.float32(1), 1: flag(iy < ny - 1)}
    mz = {-1: flag(iz > 0), 0: jnp.float32(1), 1: flag(iz < nz - 1)}

    b_ref, w_ref, c_ref, out_ref = r["B0"], r["A0"], r["CM"], r["out"]

    G0, W0, V0 = r["G0"], r["W0"], r["V0"]
    loads[0].wait()
    loads[1].wait()
    w0 = w_ref[...]
    g0 = b_ref[0] / w0
    W0[2:18, 8:24, :] = w0
    G0[2:18, 8:24, :] = g0

    r["YS"][0] = G0[2:18, 8:10, :]
    r["YS"][1] = G0[2:18, 22:24, :]

    def pack_q(src, dst):
        for h in range(2):
            acc = zero
            for x in range(16):
                m = src[x + 2, 8 + 8 * h : 16 + 8 * h, :]
                base = 6 * (x + 2)
                acc = jnp.where(lane == base, roll(m, base - 1), acc)
                acc = jnp.where((lane >= base + 1) & (lane < base + 3), roll(m, base + 1 - 127), acc)
                acc = jnp.where((lane >= base + 3) & (lane < base + 5), roll(m, base + 3 - 127), acc)
                acc = jnp.where(lane == base + 5, roll(m, base + 5 - 126), acc)
            dst[8 * h : 8 * h + 8, :] = acc

    pack_q(G0, r["QS"])
    r["QE"][0] = r["QS"][0:1, :]
    r["QE"][1] = r["QS"][15:16, :]

    for name in ("G0", "W0", "V0"):
        a = r[name]
        a[:, 0:8, :] = jnp.zeros((20, 8, 128), F32)
        a[:, 24:32, :] = jnp.zeros((20, 8, 128), F32)
    for name in ("GQ", "WQ", "VQ", "UQ", "G1", "W1", "V1", "U1", "G2", "W2", "V2", "U2", "P2", "Q2", "G3", "W3", "V3", "U3", "P3", "T4", "A1", "Q1", "R2", "PT", "QT", "Q3"):
        r[name][...] = jnp.zeros(r[name].shape, F32)

    zr = lax.broadcasted_iota(jnp.int32, (256, 128), 0) % 128
    zc = lax.broadcasted_iota(jnp.int32, (256, 128), 1)
    down = jnp.where(zc == 32 + zr // 2, jnp.float32(1), jnp.float32(0)).astype(jnp.bfloat16)
    up = jnp.where(zr == 32 + zc // 2, jnp.float32(1), jnp.float32(0)).astype(jnp.bfloat16)

    C0 = r["C0"]

    def coarsen0(values, scale):
        C0[...] = jnp.sum(values.reshape(8, 2, 16, 128), axis=1)
        t = C0[:, pl.ds(0, 8, stride=2), :] + C0[:, pl.ds(1, 8, stride=2), :]
        return (select_dot(t.reshape(64, 128), down) * scale).reshape(8, 8, 128)

    def pair_z(t, dil):
        ln = lax.broadcasted_iota(jnp.int32, t.shape, t.ndim - 1)
        return t + jnp.where((ln // dil) % 2 == 0, roll(t, -dil), roll(t, dil))

    C1, C2 = r["C1"], r["C2"]

    def coarsen1(values, scale):
        n = values.shape[0] // 2
        C1[...] = jnp.sum(values.reshape(n, 2, 8, 128), axis=1)
        t = C1[:, pl.ds(0, 4, stride=2), :] + C1[:, pl.ds(1, 4, stride=2), :]
        return pair_z(t, 1) * scale

    w1 = coarsen0(w0, 0.0625)
    own1 = (lane >= 32) & (lane < 96)
    w2 = coarsen1(w1, 0.0625)
    C2[0:4, 0:4, :] = w2
    t = C2[0:4, pl.ds(0, 2, stride=2), :] + C2[0:4, pl.ds(1, 2, stride=2), :]
    w3 = pair_z(jnp.sum(t.reshape(2, 2, 2, 128), axis=1), 2) * 0.0625

    lane4 = lane[0:4]

    def pack2(v):
        halves = []
        for h in range(2):
            a = jnp.where(lane4 % 2 == 0, v[2 * h], v[2 * h + 1])
            halves.append(roll(a, -32 if h == 0 else 32))
        return jnp.where(lane4 < 64, halves[0], halves[1])

    def pack3(v):
        return jnp.where(lane[0:2] < 64, roll(v[0], -32), roll(v[1], 32))

    SW2, SW3 = r["SW2"], r["SW3"]
    p2 = pack2(w2)
    SW2[...] = p2
    SW3[...] = pack3(w3)
    zp = jnp.zeros((4, 128), F32)
    for h in range(2):
        zp = jnp.where((lane4 >= 16 * h) & (lane4 < 16 * h + 8), roll(p2, -48 * h), zp)
        zp = jnp.where((lane4 >= 16 * h + 8) & (lane4 < 16 * h + 16), roll(p2, -48 * h - 48), zp)
    row4 = row[0:4]
    SWZ = r["SWZ"]
    SWZ[...] = sum(roll(jnp.sum(jnp.where(row4 == y, zp, 0.0), axis=0, keepdims=True), 32 * y) for y in range(4))

    def send_all(src, dst, key):
        return [round_of(key, [(o, src, dst.at[SLOT[neg(o)]]) for o in OFFS], first(dst))]

    def pack_z1(own, zs):
        acc = zero
        for x in range(8):
            acc = jnp.where((lane >= 16 * x) & (lane < 16 * x + 4), roll(own[x], 16 * x - 32), acc)
            acc = jnp.where((lane >= 16 * x + 4) & (lane < 16 * x + 8), roll(own[x], 16 * x + 4 - 92), acc)
        zs[...] = acc

    s1w, ysw, zsw, yzw = r["S1w"], r["YS1w"], r["ZS1w"], r["YZ1w"]
    s1w[...] = w1
    ysw[0] = s1w[:, 0:2, :]
    ysw[1] = s1w[:, 6:8, :]
    pack_z1(w1, zsw)
    yzw[0] = zsw[0:2, :]
    yzw[1] = zsw[6:8, :]
    RX, RY, RXY, RZ, RYZ = (r[name + "w"] for name in ("RX1", "RY1", "RXY1", "RZ1", "RYZ1"))
    r["YW"][0] = W0[2:18, 8:9, :]
    r["YW"][1] = W0[2:18, 23:24, :]
    pack_q(W0, r["QW"])

    pl.semaphore_wait(barrier, partners)

    gsl = pl.ds(8, 16)
    wait_g0 = [
        round_of(1, [((0, d, 0), r["YS"].at[i], r["RY"].at[1 - i]) for i, d in enumerate((-1, 1))], first(r["RY"])),
        round_of(
            2,
            [
                ((dx, dy, 0), r["YS"].at[(dy + 1) // 2, 0 if dx < 0 else 15], r["RXY"].at[XY.index((-dx, -dy))])
                for dx, dy in XY
            ],
            first(r["RXY"]),
        ),
        round_of(
            4,
            [((0, dy, dz), r["QE"].at[(dy + 1) // 2], r["RQE"].at[XY.index((-dy, -dz))]) for dy, dz in XY],
            first(r["RQE"]),
        ),
        round_of(3, [((dx, 0, dz), r["QS"], r["RQ"].at[XZ.index((-dx, -dz))]) for dx, dz in XZ], first(r["RQ"])),
        round_of(
            0,
            [
                ((-1, 0, 0), G0.at[pl.ds(2, 2), gsl], G0.at[pl.ds(18, 2), gsl]),
                ((1, 0, 0), G0.at[pl.ds(16, 2), gsl], G0.at[pl.ds(0, 2), gsl]),
            ],
            lambda n: G0.at[pl.ds(0, 2 * n), gsl],
        ),
    ]

    wait_w = [
        round_of(7, [((0, -1, 0), ysw.at[0], RY.at[1]), ((0, 1, 0), ysw.at[1], RY.at[0])], first(RY)),
        round_of(
            8,
            [
                ((dx, dy, 0), ysw.at[(dy + 1) // 2, 0 if dx < 0 else 7], RXY.at[XY.index((-dx, -dy))])
                for dx, dy in XY
            ],
            first(RXY),
        ),
        round_of(
            27,
            [((0, dy, dz), yzw.at[(dy + 1) // 2], RYZ.at[XY.index((-dy, -dz))]) for dy, dz in XY],
            first(RYZ),
        ),
        round_of(5, [(o, SW2, r["RW2"].at[FLAT.index(neg(o))]) for o in FLAT], first(r["RW2"])),
        round_of(17, [(o, SWZ, r["RWZ"].at[ZSLOT[neg(o)]]) for o in ZOFFS], first(r["RWZ"])),
        round_of(6, [((-1, 0, 0), s1w.at[pl.ds(0, 2)], RX.at[1]), ((1, 0, 0), s1w.at[pl.ds(6, 2)], RX.at[0])], first(RX)),
        round_of(9, [((dx, 0, dz), zsw, RZ.at[XZ.index((-dx, -dz))]) for dx, dz in XZ], first(RZ)),
    ]
    wait_w3 = [
        round_of(18, [(o, SW3, r["RW3"].at[SLOT[neg(o)]]) for o in OFFS], first(r["RW3"])),
        round_of(25, [(o, SW3, r["RW3Y"].at[OFF2Y.index(neg(o))]) for o in OFF2Y], first(r["RW3Y"])),
        round_of(24, [(o, SW3, r["RW3X"].at[OFF2X.index(neg(o))]) for o in OFF2X], first(r["RW3X"])),
    ]

    def recv1w(dst):
        for x in range(1, 13):
            dx = -1 if x < 3 else (1 if x > 10 else 0)
            sx = x - 3 if dx == 0 else (x + 5 if dx < 0 else x - 11)

            def ends(v, ln, lo, hi, dx, dy):
                v = jnp.where((ln >= 28) & (ln < 32), keep(roll(lo, 28 - 16 * sx - 4), dx, dy, -1), v)
                return jnp.where((ln >= 96) & (ln < 100), keep(roll(hi, 96 - 16 * sx), dx, dy, 1), v)

            base = w1[x - 3] if dx == 0 else keep(RX[(dx + 1) // 2, x - 1 if dx < 0 else x - 11], dx, 0, 0)
            lo, hi = (RZ[XZ.index((dx, dz))] for dz in (-1, 1))
            dst[x, 8:16, :] = ends(base, lane, lo, hi, dx, 0)
            for dy, at in ((-1, 6), (1, 16)):
                if dx == 0:
                    lo, hi = (RYZ[XY.index((dy, dz))] for dz in (-1, 1))
                    v = keep(RY[(dy + 1) // 2, x - 3], 0, dy, 0)
                    dst[x, at : at + 2, :] = ends(v, lane[0:2], lo, hi, 0, dy)
                elif x in (2, 11):
                    dst[x, at : at + 2, :] = keep(RXY[XY.index((dx, dy))], dx, dy, 0)

    def send1(own, n, key):
        s1, ys, zs = r["S1" + n], r["YS1" + n], r["ZS1" + n]
        s1[...] = own
        for q in range(4):
            v = jnp.where(lane < 64, roll(own[2 * q], -32), roll(own[2 * q + 1], 32))
            ys[0, q] = v[0:4]
            ys[1, q] = v[4:8]
        pack_z1(own, zs)
        zy = r["ZY1g"]
        zy[0] = zs[0:4, :]
        zy[1] = zs[4:8, :]
        rx, ry, rxy, rz, rzy = (r[name + n] for name in ("RX1", "RY1", "RXY1", "RZ1", "RZY1"))
        return [
            round_of(key + 1, [((0, -1, 0), ys.at[0], ry.at[1]), ((0, 1, 0), ys.at[1], ry.at[0])], first(ry)),
            round_of(
                key + 2,
                [
                    ((dx, dy, 0), ys.at[(dy + 1) // 2, 0 if dx < 0 else 3], rxy.at[XY.index((-dx, -dy))])
                    for dx, dy in XY
                ],
                first(rxy),
            ),
            round_of(28, [(o, zy.at[(o[1] + 1) // 2], rzy.at[ZY.index(neg(o))]) for o in ZY], first(rzy)),
            round_of(
                key,
                [((-1, 0, 0), s1.at[pl.ds(0, 3)], rx.at[1]), ((1, 0, 0), s1.at[pl.ds(5, 3)], rx.at[0])],
                first(rx),
            ),
            round_of(key + 3, [((dx, 0, dz), zs, rz.at[XZ.index((-dx, -dz))]) for dx, dz in XZ], first(rz)),
        ]

    def half(m, q):
        return jnp.where((lane4 >= 32) & (lane4 < 96), roll(m, 32 if q == 0 else 96), 0.0)

    def recv1(own, n, key, dst):
        run(key)
        for x in range(14):
            dx = -1 if x < 3 else (1 if x > 10 else 0)
            for dy in (-1, 0, 1):
                if dx == 0 and dy == 0:
                    base = own[x - 3]
                elif dy == 0:
                    base = r["RX1" + n][(dx + 1) // 2, x if dx < 0 else x - 11]
                elif dx == 0:
                    base = half(r["RY1" + n][(dy + 1) // 2, (x - 3) // 2], (x - 3) % 2)
                elif x in (0, 13):
                    base = jnp.zeros((4, 128), F32)
                else:
                    base = half(r["RXY1" + n][XY.index((dx, dy))], (x - 1 if dx < 0 else x - 11) % 2)
                sx = x - 3 if dx == 0 else (x + 5 if dx < 0 else x - 11)
                if dy == 0:
                    lo, hi = (r["RZ1" + n][XZ.index((dx, dz))] for dz in (-1, 1))
                else:
                    lo, hi = (r["RZY1" + n][ZY.index((dx, dy, dz))] for dz in (-1, 1))
                ln = lane[0:8] if dy == 0 else lane4
                v = keep(base, dx, dy, 0)
                v = jnp.where((ln >= 28) & (ln < 32), keep(roll(lo, 28 - 16 * sx - 4), dx, dy, -1), v)
                v = jnp.where((ln >= 96) & (ln < 100), keep(roll(hi, 96 - 16 * sx), dx, dy, 1), v)
                at = 8 if dy == 0 else (4 if dy < 0 else 16)
                dst[x, at : at + (8 if dy == 0 else 4), :] = v

    wi1 = 1.0 / jnp.where(own1, w1, 1.0)
    wi2 = 1.0 / jnp.where(own1[0:4], w2, 1.0)

    GQ, VQ = r["GQ"], r["VQ"]
    run(wait_g0)
    G0[0:2, 8:24, :] = keep(G0[0:2, 8:24, :], -1, 0, 0)
    G0[18:20, 8:24, :] = keep(G0[18:20, 8:24, :], 1, 0, 0)
    G0[2:18, 6:8, :] = keep(r["RY"][0], 0, -1, 0)
    G0[2:18, 24:26, :] = keep(r["RY"][1], 0, 1, 0)
    for dx, dy in XY:
        v = keep(r["RXY"][XY.index((dx, dy))], dx, dy, 0)
        G0[1 if dx < 0 else 18, 7 if dy < 0 else 24, :] = v[1 if dy < 0 else 0, :]

    def qj(ln):
        return ln % 6

    for h in range(2):
        sl = slice(8 * h, 8 * h + 8)
        own = r["QS"][sl, :]
        j = qj(lane)
        q = [keep(r["RQ"][i, sl, :], dx, 0, dz) for i, (dx, dz) in enumerate(XZ)]
        v, lo, hi = (
            jnp.where((j == 3) | (j == 5), q[2 * i], jnp.where((j == 0) | (j == 2), q[2 * i + 1], own if i == 0 else 0.0))
            for i in range(3)
        )
        v = jnp.where((lane >= 6) & (lane < 12), roll(lo, 6 - 102), jnp.where((lane >= 108) & (lane < 114), roll(hi, 108 - 12), v))
        GQ[8 + 8 * h : 16 + 8 * h, :] = jnp.where((lane >= 6) & (lane < 114), v, 0.0)
    for dy, at in ((-1, 7), (1, 24)):
        j = qj(lane[0:1])
        lo = keep(r["RQE"][XY.index((dy, -1))], 0, dy, -1)
        hi = keep(r["RQE"][XY.index((dy, 1))], 0, dy, 1)
        v = jnp.where((j == 3) | (j == 5), lo, jnp.where((j == 0) | (j == 2), hi, 0.0))
        GQ[at : at + 1, :] = jnp.where((lane[0:1] >= 12) & (lane[0:1] < 108), v, 0.0)

    INJ = r["INJ"]

    def inject(q, xs, tiles):
        for at in tiles:
            m = q[at : at + 8, :]
            for xp in xs:
                INJ[xp, at : at + 8, :] = jnp.where((lane == 0) | (lane == 127), roll(m, -(6 * xp + 3)), 0.0)

    def sum0(a, x, n, at):
        c = a[x : x + n, at : at + 8, :]
        t = a[x - 1 : x + n - 1, at : at + 8, :] + a[x + 1 : x + n + 1, at : at + 8, :]
        t = t + (a[x : x + n, at - 1 : at + 7, :] + a[x : x + n, at + 1 : at + 9, :])
        z = jnp.where(lane == 0, 0.0, roll(c, 1)) + jnp.where(lane == 127, 0.0, roll(c, -1))
        return c, t + (z + INJ[x : x + n, at : at + 8, :])

    inject(GQ, range(1, 19), (7, 15, 17))
    for at in (7, 15, 17):
        c, t = sum0(G0, 1, 18, at)
        v = S * (1.2 * c + S * t)
        if at == 7:
            v = v * jnp.where(row == 0, my[-1], 1.0)
        if at == 17:
            v = v * jnp.where(row == 7, my[1], 1.0)
        V0[1:19, at : at + 8, :] = v
    V0[1:2, 7:25, :] = V0[1:2, 7:25, :] * mx[-1]
    V0[18:19, 7:25, :] = V0[18:19, 7:25, :] * mx[1]

    for at in (8, 16):
        c = GQ[at : at + 8, :]
        t = jnp.where(qj(lane) == 3, roll(c, -1) + roll(c, -2), roll(c, 1) + roll(c, 2)) + (roll(c, 6) + roll(c, -6))
        t = t + GQ[at - 1 : at + 7, :] + GQ[at + 1 : at + 9, :]
        j = qj(lane)
        mask = jnp.where(j == 3, mz[-1], jnp.where(j == 2, mz[1], 0.0))
        mask = jnp.where((lane >= 12) & (lane < 108), mask, 0.0)
        VQ[at : at + 8, :] = S * (1.2 * c + S * t) * mask

    inject(VQ, range(2, 18), (8, 16))
    halves = []
    for at in (8, 16):
        c, t = sum0(V0, 2, 16, at)
        halves.append(W0[2:18, at : at + 8, :] * (G0[2:18, at : at + 8, :] - 6.0 * c + t))
    r0 = jnp.concatenate(halves, axis=1)
    g1 = jnp.where(own1, coarsen0(r0, 0.125) * wi1, 0.0)
    wait_g1 = send1(g1, "g", 10)

    G1, W1, V1, U1 = r["G1"], r["W1"], r["V1"], r["U1"]
    G2, W2, V2, U2, P2, Q2 = r["G2"], r["W2"], r["V2"], r["U2"], r["P2"], r["Q2"]
    G3, W3, V3, U3, P3 = r["G3"], r["W3"], r["V3"], r["U3"], r["P3"]
    run(wait_w)
    recv1w(W1)

    def spread(m0, lo, hi, l, dx, dy):
        return keep(m0, dx, dy, 0), jnp.where((l // 32) % 2 == 1, keep(lo, dx, dy, -1), keep(hi, dx, dy, 1))

    def place(m0, c, l, h):
        a = roll(m0, 32 if h == 0 else 96)
        e = roll(c, 96 if h == 0 else 32)
        return jnp.where((l >= 32) & (l < 96), a, e)

    def piece(buf, own, rows, o):
        return own[rows, :] if o == (0, 0, 0) else buf[SLOT[o], rows, :]

    def unpack2(buf, own, dst):
        rows = slice(0, 4)
        for dx in (-1, 0, 1):
            for dy in (-1, 0, 1):
                m0, c = spread(*[piece(buf, own, rows, (dx, dy, dz)) for dz in (0, -1, 1)], lane4, dx, dy)
                spread2(m0, c, dst, dx, dy)

    def spread2(m0, c, dst, dx, dy):
        for p in range(2):
            take = lane4 % 2 == p
            a = jnp.where(take, m0, roll(m0, 1 if p == 0 else -1))
            e = jnp.where(take, c, roll(c, 1 if p == 0 else -1))
            for h in range(2):
                dst[4 + 4 * dx + 2 * h + p, 8 + 4 * dy : 12 + 4 * dy, :] = place(a, e, lane4, h)

    def unpack3(get, spots, dst):
        l = lane[0:2]
        for dx, dy in spots:
            m0, c = spread(*[get((dx, dy, dz)) for dz in (0, -1, 1)], l, dx, dy)
            for h in range(2):
                dst[5 + 2 * dx + h, 12 + 2 * dy : 14 + 2 * dy, :] = place(m0, c, l, h)

    for dx in (-1, 0, 1):
        for dy in (-1, 0, 1):
            m0 = keep(SW2[...] if dx == dy == 0 else r["RW2"][FLAT.index((dx, dy, 0))], dx, dy, 0)
            lo, hi = (keep(r["RWZ"][ZSLOT[(dx, dy, dz)]], dx, dy, dz) for dz in (-1, 1))
            line = jnp.where(lane[0:1] % 16 >= 8, lo, hi)
            e = jnp.zeros((4, 128), F32)
            for y in range(4):
                e = jnp.where(row4 == y, roll(line, -32 * y), e)
            c = jnp.zeros((4, 128), F32)
            for h in range(2):
                c = jnp.where((lane4 >= 64 * h) & (lane4 < 64 * h + 8), roll(e, 48 * h), c)
                c = jnp.where((lane4 >= 64 * h + 56) & (lane4 < 64 * h + 64), roll(e, 48 * h + 48), c)
            spread2(m0, c, W2, dx, dy)

    def inverse(w):
        return jnp.where(w > 0.0, 1.0 / jnp.where(w > 0.0, w, 1.0), 0.0)

    def nsum(a, x, n, at, rows, dil):
        c = a[x : x + n, at : at + rows, :]
        t = a[x - 1 : x + n - 1, at : at + rows, :] + a[x + 1 : x + n + 1, at : at + rows, :]
        t = t + (a[x : x + n, at - 1 : at + rows - 1, :] + a[x : x + n, at + 1 : at + rows + 1, :])
        return c, t + (roll(c, dil) + roll(c, -dil))

    def rowmask(at, rows, low, high):
        y = lax.broadcasted_iota(jnp.int32, (rows, 128), 0) + at
        l = lax.broadcasted_iota(jnp.int32, (rows, 128), 1)
        m = jnp.where(y < low, my[-1], jnp.where(y >= high, my[1], 1.0))
        return m * jnp.where(l < 32, mz[-1], jnp.where(l >= 96, mz[1], 1.0))

    def xmask(a, low, high, x, n, at, rows):
        if low > x:
            a[x:low, at : at + rows, :] = a[x:low, at : at + rows, :] * mx[-1]
        if x + n > high:
            a[high : x + n, at : at + rows, :] = a[high : x + n, at : at + rows, :] * mx[1]

    A1, Q1, R2, PT, QT, Q3 = r["A1"], r["Q1"], r["R2"], r["PT"], r["QT"], r["Q3"]
    A1[3:11, 8:16, :] = g1
    for at in (4, 12):
        c, t = nsum(A1, 1, 12, at, 8, 1)
        Q1[1:13, at : at + 8, :] = S * (1.2 * c + S * t) * rowmask(at, 8, 8, 16)
    xmask(Q1, 3, 11, 1, 12, 4, 16)
    C3 = r["C3"]
    for at in (6, 10):
        c, t = nsum(Q1, 1, 12, at, 8, 1)
        res = W1[1:13, at : at + 8, :] * (A1[1:13, at : at + 8, :] - 6.0 * c + t)
        C3[:, at - 6 : at + 2, :] = jnp.sum(res.reshape(6, 2, 8, 128), axis=1)
    t = C3[:, pl.ds(0, 6, stride=2), :] + C3[:, pl.ds(1, 6, stride=2), :]
    P2[3:9, 7:13, :] = pair_z(t, 1) * 0.125 * inverse(W2[3:9, 7:13, :])
    c, t = nsum(P2, 2, 8, 6, 8, 2)
    Q2[2:10, 6:14, :] = S * (1.2 * c + S * t) * rowmask(6, 8, 8, 12)
    xmask(Q2, 4, 8, 2, 8, 6, 8)
    for at in (5, 7):
        c, t = nsum(Q2, 1, 10, at, 8, 2)
        R2[1:11, at : at + 8, :] = W2[1:11, at : at + 8, :] * (P2[1:11, at : at + 8, :] - 6.0 * c + t)
    C3[...] = jnp.sum(R2[:, 4:20, :].reshape(6, 2, 16, 128), axis=1)
    t = C3[:, pl.ds(0, 6, stride=2), :] + C3[:, pl.ds(1, 6, stride=2), :]
    b3 = pair_z(t, 2) * 0.125
    run(wait_w3)

    def piece3(o):
        if o == (0, 0, 0):
            return SW3[...]
        if abs(o[0]) == 2:
            return r["RW3X"][OFF2X.index(o)]
        if abs(o[1]) == 2:
            return r["RW3Y"][OFF2Y.index(o)]
        return r["RW3"][SLOT[o]]

    unpack3(piece3, [(a, b) for a in range(-2, 3) for b in range(-2, 3) if abs(a) < 2 or abs(b) < 2], W3)

    P3[3:9, 10:16, :] = b3 * inverse(W3[3:9, 10:16, :])
    c, t = nsum(P3, 2, 8, 9, 8, 4)
    Q3[2:10, 9:17, :] = S * (1.2 * c + S * t) * rowmask(9, 8, 12, 14)
    xmask(Q3, 5, 7, 2, 8, 9, 8)
    T4 = r["T4"]
    for at in (8, 10):
        c, t = nsum(Q3, 1, 10, at, 8, 4)
        res = W3[1:11, at : at + 8, :] * (P3[1:11, at : at + 8, :] - 6.0 * c + t)
        T4[:, at : at + 8, :] = jnp.sum(res.reshape(5, 2, 8, 128), axis=1)
    t = T4[:, pl.ds(8, 8, stride=2), :] + T4[:, pl.ds(9, 8, stride=2), :]
    patch = pair_z(t, 4) * 0.125

    lines = []
    for dx in range(5):
        v = patch[dx]
        main = zero
        for q in range(4):
            lo = 32 + 16 * q + 7
            main = jnp.where((lane >= 2 * q) & (lane < 2 * q + 2), roll(v, 2 * q - lo), main)
        edge = jnp.where(lane < 2, roll(v, 0 - 23), jnp.where(lane < 4, roll(v, 2 - 103), 0.0))
        line = pltpu.roll(main, 0, 1, stride=8, stride_axis=0) + pltpu.roll(edge, 40, 1, stride=4, stride_axis=0)
        lines.append(jnp.sum(line, axis=0, keepdims=True))
    GA, GB, GC = r["GA"], r["GB"], r["GC"]
    SA, SB, SZ = r["SA"], r["SB"], r["SZ"]
    for p in range(2):
        SA[p : p + 1, :] = lines[2 * p] + roll(lines[2 * p + 1], 64)
    SA[2:3, :] = lines[4]
    SA[3:4, :] = jnp.zeros((1, 128), F32)
    ga_at = ih * nx + ix
    to_group(21, SA, GA.at[ga_at], group_y)

    wait_w0 = [
        round_of(
            14,
            [
                ((-1, 0, 0), W0.at[pl.ds(2, 1), gsl], W0.at[pl.ds(18, 1), gsl]),
                ((1, 0, 0), W0.at[pl.ds(17, 1), gsl], W0.at[pl.ds(1, 1), gsl]),
            ],
            lambda n: W0.at[pl.ds(0, n), gsl],
        ),
        round_of(15, [((0, d, 0), r["YW"].at[i], r["RYW"].at[1 - i]) for i, d in enumerate((-1, 1))], first(r["RYW"])),
        round_of(16, [((0, 0, d), r["QW"], r["RQW"].at[1 - i]) for i, d in enumerate((-1, 1))], first(r["RQW"])),
    ]

    cp = r["CP"]
    loads[2].wait()

    @pl.loop(0, nx)
    def _(x):
        for z in range(nz):
            acc = zero
            for p in range(ny // 2):
                tile = c_ref[:, pl.ds(pl.multiple_of((x * (ny // 2) + p) * 128, 128), 128)]
                for q in range(2):
                    y = 2 * p + q
                    at = 8 * y
                    acc = jnp.where((lane >= at) & (lane < at + 8), roll(tile, at - 64 * q - 8 * z), acc)
            cp[x * nz + z] = acc

    from_group(21, GA, n_y - 1)
    GA[ga_at] = SA[...]
    sums = []
    for h in range(2):
        even, odd = zero, zero
        for p in range(3):
            m = zero
            for g in range(nx):
                m = jnp.where(row == g, GA[h * nx + g, p : p + 1, :], m)
            even = even + (m if p == 1 else pltpu.roll(m, (2 * p - 2) % 8, 0))
            if p < 2:
                odd = odd + pltpu.roll(m, (2 * p - 1) % 8, 0)
        sums.append(jnp.where(lane < 64, even, 0.0) + roll(jnp.where(lane < 64, 0.0, odd), 64))
    SB[...] = sums[0] + roll(sums[1], 64)
    to_group(22, SB, GB.at[ixx], group_x)

    recv1(g1, "g", wait_g1, G1)
    for at in (4, 12):
        c, t = nsum(G1, 1, 12, at, 8, 1)
        V1[1:13, at : at + 8, :] = S * (1.2 * c + S * t) * rowmask(at, 8, 8, 16)
    xmask(V1, 3, 11, 1, 12, 4, 16)
    c, t = nsum(V1, 3, 8, 8, 8, 1)
    r1 = W1[3:11, 8:16, :] * (G1[3:11, 8:16, :] - 6.0 * c + t)
    g2 = jnp.where(own1[0:4], coarsen1(r1, 0.125) * wi2, 0.0)

    PT[4:8, 8:12, :] = g2
    c, t = nsum(PT, 2, 8, 6, 8, 2)
    QT[2:10, 6:14, :] = S * (1.2 * c + S * t) * rowmask(6, 8, 8, 12)
    xmask(QT, 4, 8, 2, 8, 6, 8)
    c, t = nsum(QT, 2, 8, 6, 8, 2)
    res = W2[2:10, 6:14, :] * (PT[2:10, 6:14, :] - 6.0 * c + t)
    C2[...] = jnp.sum(res.reshape(4, 2, 8, 128), axis=1)
    t = C2[:, pl.ds(0, 4, stride=2), :] + C2[:, pl.ds(1, 4, stride=2), :]
    b3 = pair_z(t, 2) * 0.125
    SC = r["SC"]
    SC[0:4, :] = pack2(g2)
    l4 = lane4 % 4
    SC[4:8, :] = jnp.where(l4 < 2, jnp.where(l4 == 0, b3[0], b3[1]), jnp.where(l4 == 2, b3[2], b3[3]))
    wait_c = send_all(SC, r["RC"], 19)

    from_group(22, GB, xn - 1)
    GB[ixx] = SB[...]
    main = zero
    edges = [zero] * 5
    for k in range(xn):
        v = GB[k]
        for h in range(2):
            if xn == 8 and h == 1:
                continue
            shift = 8 * k - 16 + h * (8 * xn - 64)
            m = roll(v, shift)
            src = (lane - shift + 256) % 128
            if xn != 8:
                m = jnp.where(src // 64 == h, m, 0.0)
            main = main + jnp.where(src % 64 < 40, m, 0.0)
            for dy in range(5):
                a = 40 + 4 * dy
                edges[dy] = edges[dy] + jnp.where((src % 64 >= a) & (src % 64 < a + 4), m, 0.0)
    edge = zero
    for dy in range(5):
        edge = edge + roll(edges[dy], 4 * dy - 40)
    SZ[0] = main
    SZ[1] = edge
    to_group(23, SZ, GC.at[iz], group_z)

    run(wait_w0)
    W0[1:2, 8:24, :] = keep(W0[1:2, 8:24, :], -1, 0, 0)
    W0[18:19, 8:24, :] = keep(W0[18:19, 8:24, :], 1, 0, 0)
    W0[2:18, 7:8, :] = keep(r["RYW"][0], 0, -1, 0)
    W0[2:18, 24:25, :] = keep(r["RYW"][1], 0, 1, 0)
    for h in range(2):
        sl = slice(8 * h, 8 * h + 8)
        j = qj(lane)
        v = jnp.where(j == 3, keep(r["RQW"][0, sl, :], 0, 0, -1), jnp.where(j == 2, keep(r["RQW"][1, sl, :], 0, 0, 1), 0.0))
        r["WQ"][8 + 8 * h : 16 + 8 * h, :] = v

    run(wait_c)
    unpack2(r["RC"], SC, G2)
    c, t = nsum(G2, 2, 8, 6, 8, 2)
    V2[2:10, 6:14, :] = S * (1.2 * c + S * t) * rowmask(6, 8, 8, 12)
    xmask(V2, 4, 8, 2, 8, 6, 8)

    TB, TC, RC = r["TB"], r["TC"], r["RC"]
    for dy in (-1, 0, 1):
        acc = jnp.zeros((4, 128), F32)
        for dx in (-1, 0, 1):
            m0, lo, hi = (keep(piece(RC, SC, slice(4, 8), (dx, dy, dz)), dx, dy, dz) for dz in (0, -1, 1))
            e = jnp.where((lane4 >= 92) & (lane4 < 100), lo, jnp.where((lane4 >= 28) & (lane4 < 36), hi, 0.0))
            q = m0 + roll(e, 64)
            if dx < 0:
                q = jnp.where(l4 < 2, roll(q, -2), 0.0)
            if dx > 0:
                q = jnp.where(l4 >= 2, roll(q, 2), 0.0)
            acc = acc + q
        TB[dy + 1] = acc
    TC[0:2, :] = TB[1, 0:2, :] + TB[0, 2:4, :]
    TC[2:4, :] = TB[1, 2:4, :] + TB[2, 0:2, :]
    for i in range(4):
        v = roll(jnp.where(l4 == i, TC[...], 0.0), -i)
        v = v + roll(v, 1)
        v = v + roll(v, 2)
        G3[4 + i, 11:15, :] = v * inverse(W3[4 + i, 11:15, :])
    c, t = nsum(G3, 5, 2, 12, 2, 4)
    v3 = jnp.where(own1[0:2], S * (1.2 * c + S * t), 0.0)
    SE, SV, RE, RV = r["SE"], r["SV"], r["RE"], r["RV"]
    SV[...] = pack3(v3)
    wait_v = send_all(SV, RV, 26)

    def drain(key, slots, count, sizes):
        for n in sizes:

            @pl.when(count == n)
            def _():
                copy(slots(n), slots(n), key, right).wait_send()

    early = len(sent) - 1
    for item in sent[:early]:
        drain(*item)

    from_group(23, GC, nz - 1)
    GC[iz, 0] = SZ[0]
    GC[iz, 1] = SZ[1]
    acc = [zero] * 4
    for z in range(nz):
        v = GC[z, 0]
        if z + 1 < nz:
            v = v + jnp.where(lane % 8 >= 6, roll(GC[z + 1, 1], 6), 0.0)
        if z > 0:
            v = v + jnp.where(lane % 8 < 2, roll(GC[z - 1, 1], -2), 0.0)
        for x in range(nx):
            acc[x % 4] = acc[x % 4] + cp[x * nz + z] * v[x : x + 1, :]
    acc = (acc[0] + acc[1]) + (acc[2] + acc[3])
    tot = jnp.sum(acc, axis=1, keepdims=True)
    e4 = jnp.sum(jnp.where((lane >= 32 + 8 * row) & (lane < 40 + 8 * row), tot, 0.0), axis=0, keepdims=True)
    SE[...] = e4
    wait_e = send_all(SE, RE, 20)
    run(wait_v)

    near = [(a, b) for a in (-1, 0, 1) for b in (-1, 0, 1)]
    unpack3(lambda o: SV[...] if o == (0, 0, 0) else RV[SLOT[o]], near, V3)
    run(wait_e)
    l1 = lane[0:1]
    par = []
    for dx in (-1, 0, 1):
        v = zero
        for dy in (-1, 0, 1):
            o = (dx, dy, 0)
            own = SE[...] if o == (0, 0, 0) else keep(RE[SLOT[o], 0:1, :], *o)
            lo, hi = (keep(RE[SLOT[(dx, dy, dz)], 0:1, :], dx, dy, dz) for dz in (-1, 1))
            e = jnp.where((l1 >= 32) & (l1 < 96), own, roll(jnp.where(l1 < 64, hi, lo), 64))
            y = 4 + 2 * dy
            v = jnp.where((row == y) | (row == y + 1), e, v)
        par.append(v)
    for i in range(6):
        U3[3 + i, 8:16, :] = V3[3 + i, 8:16, :] + W3[3 + i, 8:16, :] * par[i // 2]
    c, t = nsum(U3, 4, 4, 8, 8, 4)
    E3 = r["E3"]
    E3[...] = (0.2 * c + S * (G3[4:8, 8:16, :] + t)) * inverse(W3[4:8, 8:16, :])
    F2 = r["F2"]
    F2[:, pl.ds(0, 4, stride=2), :] = E3[:, 3:7, :]
    F2[:, pl.ds(1, 4, stride=2), :] = E3[:, 3:7, :]
    for i in range(8):
        U2[2 + i, 6:14, :] = V2[2 + i, 6:14, :] + W2[2 + i, 6:14, :] * F2[i // 2]
    c, t = nsum(U2, 3, 6, 6, 8, 2)
    E2 = r["E2"]
    E2[...] = (0.2 * c + S * (G2[3:9, 6:14, :] + t)) * inverse(W2[3:9, 6:14, :])
    F1 = r["F1"]
    F1[:, pl.ds(2, 6, stride=2), :] = E2[:, 1:7, :]
    F1[:, pl.ds(3, 6, stride=2), :] = E2[:, 1:7, :]
    for i in range(12):
        U1[1 + i, 6:18, :] = V1[1 + i, 6:18, :] + W1[1 + i, 6:18, :] * F1[i // 2, 2:14, :]
    E1 = r["E1"]
    for at in (7, 9):
        c, t = nsum(U1, 2, 10, at, 8, 1)
        E1[:, at - 7 : at + 1, :] = (0.2 * c + S * (G1[2:12, at : at + 8, :] + t)) * inverse(W1[2:12, at : at + 8, :])
    o = select_dot(E1[...].reshape(160, 128), up).reshape(10, 16, 128)
    F0 = r["F0"]
    O1 = r["O1"]
    O1[...] = o
    F0[:, pl.ds(6, 10, stride=2), :] = O1[:, 0:10, :]
    F0[:, pl.ds(7, 10, stride=2), :] = O1[:, 0:10, :]
    acc = zero
    for x in range(8):
        e = E1[x + 1, 1:9, :]
        for p in range(2):
            base = 6 * (2 * x + p + 2)
            acc = jnp.where(lane == base + 3, roll(e, base + 3 - 31), acc)
            acc = jnp.where(lane == base + 2, roll(e, base + 2 - 96), acc)
    UQ = r["UQ"]
    FQ = r["FQ"]
    FQ[...] = acc
    UQ[pl.ds(8, 8, stride=2), :] = FQ[...]
    UQ[pl.ds(9, 8, stride=2), :] = FQ[...]
    UQ[8:24, :] = VQ[8:24, :] + r["WQ"][8:24, :] * UQ[8:24, :]
    for i in range(18):
        V0[1 + i, 7:25, :] = V0[1 + i, 7:25, :] + W0[1 + i, 7:25, :] * F0[(i + 1) // 2, 7:25, :]
    inject(UQ, range(2, 18), (8, 16))
    for at in (8, 16):
        c, t = sum0(V0, 2, 16, at)
        out_ref[:, at - 8 : at, :] = 0.2 * c + S * (G0[2:18, at : at + 8, :] + t)

    for item in sent[early:]:
        drain(*item)
    for key, buf, n in ((21, GA, n_y - 1), (22, GB, xn - 1), (23, GC, nz - 1)):
        copy(buf.at[pl.ds(0, n)], buf.at[pl.ds(0, n)], key, right).wait_send()


def scratch(dims):
    nx, ny, nz = dims
    xn = ny // 2
    v = {
        "B0": (1, 16, 16, 128), "A0": (16, 16, 128), "CM": (8, nx * ny * nz * 8),
        "G0": (20, 32, 128), "W0": (20, 32, 128), "V0": (20, 32, 128), "INJ": (20, 32, 128),
        "GQ": (32, 128), "VQ": (32, 128), "WQ": (32, 128), "UQ": (32, 128),
        "YS": (2, 16, 2, 128), "RY": (2, 16, 2, 128), "RXY": (4, 2, 128),
        "QS": (16, 128), "QW": (16, 128), "RQ": (6, 16, 128), "QE": (2, 1, 128), "RQE": (4, 1, 128),
        "YW": (2, 16, 1, 128), "RYW": (2, 16, 1, 128), "RQW": (2, 16, 128),
        "C0": (8, 16, 128), "C1": (4, 8, 128), "C2": (4, 8, 128),
        "SW2": (4, 128), "SW3": (2, 128), "SWZ": (1, 128), "RW2": (8, 4, 128), "RWZ": (18, 1, 128),
        "RW3": (26, 2, 128), "RW3X": (18, 2, 128), "RW3Y": (18, 2, 128), "C3": (6, 16, 128),
        "A1": (14, 24, 128), "Q1": (14, 24, 128), "R2": (12, 24, 128), "PT": (12, 24, 128), "QT": (12, 24, 128),
        "G1": (14, 24, 128), "W1": (14, 24, 128), "V1": (14, 24, 128), "U1": (14, 24, 128),
        "G2": (12, 24, 128), "W2": (12, 24, 128), "V2": (12, 24, 128), "U2": (12, 24, 128),
        "P2": (12, 24, 128), "Q2": (12, 24, 128),
        "G3": (12, 24, 128), "W3": (12, 24, 128), "V3": (12, 24, 128), "U3": (12, 24, 128), "P3": (12, 24, 128), "Q3": (12, 24, 128),
        "T4": (5, 24, 128),
        "SC": (8, 128), "RC": (26, 8, 128), "TB": (3, 4, 128), "TC": (4, 128), "SE": (1, 128), "RE": (26, 1, 128), "SV": (2, 128), "RV": (26, 2, 128),
        "SA": (4, 128), "SB": (8, 128), "SZ": (2, 8, 128),
        "GA": (2 * nx, 4, 128), "GB": (xn, 8, 128), "GC": (nz, 2, 8, 128), "CP": (nx * nz, 8, 128),
        "E3": (4, 8, 128), "F2": (4, 8, 128), "E2": (6, 8, 128), "F1": (6, 16, 128),
        "E1": (10, 16, 128), "O1": (10, 16, 128), "F0": (10, 32, 128), "FQ": (8, 128),
    }
    n = "g"
    v["S1" + n] = (8, 8, 128)
    v["YS1" + n] = (2, 4, 4, 128)
    v["ZS1" + n] = (8, 128)
    v["ZY1" + n] = (2, 4, 128)
    v["RX1" + n] = (2, 3, 8, 128)
    v["RY1" + n] = (2, 4, 4, 128)
    v["RXY1" + n] = (4, 4, 128)
    v["RZ1" + n] = (6, 8, 128)
    v["RZY1" + n] = (12, 4, 128)
    n = "w"
    v["S1" + n] = (8, 8, 128)
    v["YS1" + n] = (2, 8, 2, 128)
    v["ZS1" + n] = (8, 128)
    v["YZ1" + n] = (2, 2, 128)
    v["RX1" + n] = (2, 2, 8, 128)
    v["RY1" + n] = (2, 8, 2, 128)
    v["RXY1" + n] = (4, 2, 128)
    v["RZ1" + n] = (6, 8, 128)
    v["RYZ1" + n] = (4, 2, 128)
    return v


def solution(mesh):
    dims = tuple(mesh.shape[a] for a in ("gx", "gy", "gz"))
    sizes = scratch(dims)

    def body(*args):
        names = ["b", "w", "c", "out"] + list(sizes) + ["ssem", "rsem", "lsem"]
        kernel(dims, dict(zip(names, args)))

    def per_device(sources, stiffness, coarse_inverse):
        vmem = pl.BlockSpec(memory_space=pltpu.VMEM)
        e = pl.pallas_call(
            body,
            out_shape=jax.ShapeDtypeStruct((16, 16, 128), F32),
            in_specs=[pl.BlockSpec(memory_space=pltpu.HBM)] * 3,
            out_specs=vmem,
            scratch_shapes=[pltpu.VMEM(s, F32) for s in sizes.values()] + [pltpu.SemaphoreType.DMA((29,))] * 2 + [pltpu.SemaphoreType.DMA((3,))],
            compiler_params=pltpu.CompilerParams(collective_id=0, has_side_effects=True, vmem_limit_bytes=24 * 2**20),
            name="vcycle",
        )(*[pltpu.with_memory_space_constraint(a, pltpu.HBM) for a in (sources, stiffness, coarse_inverse)])
        return (e / stiffness)[None]

    return jax.shard_map(
        per_device,
        mesh=mesh,
        in_specs=(P(None, "gx", "gy", "gz"), P("gx", "gy", "gz"), P(("gx", "gy", "gz"), None)),
        out_specs=P(None, "gx", "gy", "gz"),
        check_vma=False,
    )
```
